32 devices in a mesh: virt: 8 (over z, x), aux: 4 (over y, core).
Axes of the slice: x: 2, y: 2, z: 4, core: 2. Of those that a mesh axis runs over, the one named last changes fastest.
Arguments:
- three_index: bfloat16 [600, 5120], P('aux', 'virt'), may hold values from -0.0625 to 0.0625
- eps_occ: float32 [20], replicated, may hold values from -1.5 to -0.5
- eps_virt: float32 [256], replicated, may hold values from 0.3 to 3
Outputs:
- virt_energy: float32 [256], P('virt')
- pair_energy: float32 [20, 20], replicated
The draws below stay inside these ranges and needn't reach their ends.
All inputs are finite; a program needn't handle non-finite values.
Results may differ from the reference program's by a relative error of at most 0.0003.
Values may be sent and summed in bfloat16 or wider, within the bound.
A program may use at most 128 MiB of HBM per device.

```python
import jax
import jax.numpy as jnp
from jax import lax

O = 20
VIRT_DEV = 32
VIRT = 256
AUX = 600


def level_of(own_key, shape, split, low, largest):
    gain = 1.0
    for axis_at, blocks in split:
        steps = jax.random.uniform(jax.random.fold_in(jax.random.fold_in(own_key, 6), axis_at), (blocks,), jnp.float32, low / len(split), largest / len(split))
        gain = gain * jnp.repeat(jnp.exp(steps), shape[axis_at] // blocks).reshape((-1,) + (1,) * (len(shape) - 1 - axis_at))
    return gain


def scatter_about(key, dims, spread, limit, split=(), kind=jnp.bfloat16):
    result = jax.random.normal(key, dims, jnp.float32) * spread
    if len(split) > 0:
        result = level_of(key, dims, split, -0.22, 0.18) * result
    return jnp.clip(result, min=-limit, max=limit).astype(kind)


def setup_inputs(seed: int = 0) -> dict:
    splits = jax.random.split(jax.random.key(seed), 4)
    three_index = scatter_about(splits[0], (AUX, VIRT * O), 0.011, 0.0625, ((0, 4), (1, 8)))
    eps_occ = jnp.clip(jax.random.uniform(splits[1], (O,), jnp.float32, -1.5, -0.5), -1.5, -0.5)
    eps_virt = jnp.clip(jax.random.uniform(splits[2], (VIRT,), jnp.float32, 0.3, 3.0), 0.3, 3.0)
    return {"three_index": three_index, "eps_occ": eps_occ, "eps_virt": eps_virt}


def reference(three_index, eps_occ, eps_virt):
    block_count = VIRT // VIRT_DEV
    widened = three_index.astype(jnp.float32).reshape(AUX, VIRT, O)

    def one_block(which):
        offset = (which * VIRT_DEV).astype(jnp.int32)
        left_rows = lax.dynamic_slice_in_dim(widened, offset, VIRT_DEV, 1)
        integrals = jnp.einsum("pai,pbj->iajb", left_rows, widened, precision=lax.Precision.HIGHEST)
        eps_own = lax.dynamic_slice_in_dim(eps_virt, offset, VIRT_DEV)
        denominator = (eps_occ[:, None, None, None] + eps_occ[None, None, :, None]
                       - eps_own[None, :, None, None] - eps_virt[None, None, None, :])
        swapped = jnp.transpose(integrals, (2, 1, 0, 3))
        energy_terms = integrals * (2.0 * integrals - swapped) / denominator
        return jnp.sum(energy_terms, axis=(0, 2, 3)), jnp.sum(energy_terms, axis=(1, 3))

    virt_parts, pair_parts = lax.map(one_block, jnp.arange(block_count, dtype=jnp.int32))
    return virt_parts.reshape(VIRT), jnp.sum(pair_parts, axis=0)
```

```python
import functools

import jax
import jax.numpy as jnp
from jax import lax
from jax.experimental import pallas as pl
from jax.experimental.pallas import tpu as pltpu
from jax.sharding import PartitionSpec as P

MESH = pl.DeviceIdType.MESH
F32 = jnp.float32
BF16 = jnp.bfloat16
EXACT = lax.Precision.HIGHEST
LANES = 128
NT = (((1,), (1,)), ((), ()))
NN = (((1,), (0,)), ((), ()))


def distances(n_aux):
    return list(range(1, n_aux + 1, 2)) + list(range(2, n_aux + 1, 2))


def pick(table, at):
    got = table[0] + jnp.int32(0)
    for k in range(1, len(table)):
        got = jnp.where(at == k, table[k] + jnp.int32(0), got)
    return got


def label_of(virt, n_virt):
    return lax.rem(virt, 2) * (n_virt // 2) + virt // 2


def virt_of(label, n_virt):
    half = n_virt // 2
    return lax.rem(label, half) * 2 + label // half


def kernel(
    n_virt, n_aux, occ,
    x_ref, occ_ref, virt_ref,
    done_ref,
    held, lhs, rhs, order, order_t, ints, sums, parts, message, slots,
    own_sem, send_sem, recv_sem, msg_send, msg_recv,
):
    rows, cols = x_ref.shape
    pitch = -(-rows // 16) * 16
    width = cols // occ
    groups = LANES // width
    supers = occ // groups
    n = n_virt * n_aux
    v = lax.axis_index("virt")
    p = lax.axis_index("aux")
    me = v * n_aux + p
    table = distances(n_aux)
    label = label_of(v, n_virt)
    other = virt_of(lax.rem(label + pick(table, p), n_virt), n_virt)
    lower = label < n_virt // 2
    solo = jnp.logical_and(p == n_aux - 1, jnp.logical_not(lower))
    extra = jnp.logical_and(p == n_aux // 2 - 1, lower)

    barrier = pltpu.get_barrier_semaphore()

    def greet(k, c):
        t = lax.rem(me + k, n)
        pl.semaphore_signal(
            barrier, inc=1,
            device_id={"virt": t // n_aux, "aux": lax.rem(t, n_aux)},
            device_id_type=MESH,
        )
        return c

    lax.fori_loop(1, n, greet, 0)
    own = pltpu.make_async_copy(x_ref, held.at[0, p], own_sem)
    own.start()
    pl.semaphore_wait(barrier, n - 1)

    pairs = n_aux // 2

    def place(k):
        return lax.rem(p // 2 + k // 2, pairs) * 2 + lax.rem(p + k, 2)

    def share_own(k):
        return pltpu.make_async_remote_copy(
            src_ref=x_ref, dst_ref=held.at[0, p],
            send_sem=send_sem.at[0, k], recv_sem=recv_sem.at[0, p],
            device_id={"virt": v, "aux": place(k)}, device_id_type=MESH,
        )

    def hand_on(k):
        q = place(k)
        return pltpu.make_async_remote_copy(
            src_ref=held.at[0, q], dst_ref=held.at[0, q],
            send_sem=send_sem.at[2, k], recv_sem=recv_sem.at[0, q],
            device_id={"virt": v, "aux": place(1)}, device_id_type=MESH,
        )

    def share_other(k):
        q = place(k)
        target = lax.rem(label + n_virt - pick(table, q), n_virt)
        copy = pltpu.make_async_remote_copy(
            src_ref=x_ref, dst_ref=held.at[1, p],
            send_sem=send_sem.at[1, k], recv_sem=recv_sem.at[1, p],
            device_id={"virt": virt_of(target, n_virt), "aux": q}, device_id_type=MESH,
        )
        wanted = jnp.logical_or(q < n_aux - 1, target < n_virt // 2)
        return copy, wanted

    for k in list(range(2, n_aux, 2)) + [1]:
        share_own(k).start()
    for k in range(n_aux):
        copy, wanted = share_other(k)
        pl.when(wanted)(copy.start)

    def arrived(side, q):
        pltpu.make_async_copy(
            held.at[side, q], held.at[side, q], recv_sem.at[side, q]
        ).wait()

    row = lax.broadcasted_iota(jnp.int32, (cols, cols), 0)
    col = lax.broadcasted_iota(jnp.int32, (cols, cols), 1)
    hit = col == lax.rem(row, width) * occ + row // width
    order[...] = jnp.where(hit, 1.0, 0.0).astype(BF16)
    hit = row == lax.rem(col, width) * occ + col // width
    order_t[...] = jnp.where(hit, 1.0, 0.0).astype(BF16)
    lhs[...] = jnp.zeros_like(lhs)
    rhs[...] = jnp.zeros_like(rhs)

    def turn(k):
        lhs[:, k * pitch:k * pitch + rows] = lax.dot_general(
            order[...], held[0, place(k)], NT, preferred_element_type=F32
        ).astype(BF16)

    own.wait()
    turn(0)
    for k in range(2, n_aux, 2):
        arrived(0, place(k))
        hand_on(k).start()
        turn(k)
    for k in range(1, n_aux, 2):
        arrived(0, place(k))
        turn(k)

    lane = lax.broadcasted_iota(jnp.int32, (1, LANES), 1)
    part = lane // width
    down = lax.broadcasted_iota(jnp.int32, (width, 1), 0)
    lane_in = lax.rem(lane, width)

    def eps_down(which):
        got = jnp.zeros((width, 1), F32)
        for k in range(width):
            got = jnp.where(down == k, virt_ref[which * width + k], got)
        return got

    def eps_across(which):
        got = jnp.zeros((1, LANES), F32)
        for k in range(width):
            got = jnp.where(lane_in == k, virt_ref[which * width + k], got)
        return got

    occ_lane = []
    for cj in range(supers):
        got = jnp.zeros((1, LANES), F32)
        for t in range(groups):
            got = jnp.where(part == t, occ_ref[cj * groups + t], got)
        occ_lane.append(got)

    tall = -(-occ // 8)
    sums[...] = jnp.zeros_like(sums)
    n_tiles = jnp.where(extra, 2, 1)
    r8 = lax.broadcasted_iota(jnp.int32, (8, LANES), 0)
    l8 = lax.broadcasted_iota(jnp.int32, (8, LANES), 1)
    free = tall * width

    def tile(t, c):
        diag = jnp.logical_or(solo, jnp.logical_and(extra, t == 0))
        source = jnp.where(diag, 0, 1)

        for k in range(n_aux):

            @pl.when(source == 1)
            def _():
                arrived(1, place(k))

            rhs[k * pitch:k * pitch + rows, :] = lax.dot_general(
                held[source, place(k)], order_t[...], NN, preferred_element_type=F32
            ).astype(BF16)
        ints[...] = lax.dot_general(lhs[...], rhs[...], NN, preferred_element_type=F32)

        base = -(eps_down(v) + eps_across(jnp.where(diag, v, other)))
        total = jnp.zeros((width, LANES), F32)
        for ci in range(supers):
            for cj in range(ci, supers):
                turned = []
                for g in range(groups):
                    block = ints[pl.ds((cj * groups + g) * width, width), pl.ds(ci * LANES, LANES)]
                    turned.append([block if r == 0 else pltpu.roll(block, r * width, 1) for r in range(groups)])
                for s in range(groups):
                    i = ci * groups + s
                    direct = ints[pl.ds(i * width, width), pl.ds(cj * LANES, LANES)]
                    swapped = turned[0][(0 - s) % groups]
                    for g in range(1, groups):
                        swapped = jnp.where(part == g, turned[g][(g - s) % groups], swapped)
                    below = base + (occ_lane[cj] + occ_ref[i])
                    if ci == cj:
                        term = direct * (2.0 * direct - swapped) / below
                    else:
                        term = 2.0 * (direct * (direct - swapped) + swapped * swapped) / below
                    total = total + term
                    short = term[0:8]
                    for m in range(8, width, 8):
                        short = short + term[m:m + 8]
                    sums[i * 8:i * 8 + 8, cj * LANES:(cj + 1) * LANES] = short

        wide = lax.broadcasted_iota(jnp.int32, (cols, LANES), 0)
        thin = lax.broadcasted_iota(jnp.int32, (cols, LANES), 1)
        fold = jnp.where(wide // width == thin, 1.0, 0.0)
        by_j = lax.dot_general(sums[...], fold, NN, precision=EXACT, preferred_element_type=F32)
        ri = lax.broadcasted_iota(jnp.int32, (tall * 8, occ * 8), 0)
        rj = lax.broadcasted_iota(jnp.int32, (tall * 8, occ * 8), 1)
        by_ij = lax.dot_general(
            jnp.where(rj // 8 == ri, 1.0, 0.0), by_j, NN,
            precision=EXACT, preferred_element_type=F32,
        )
        packed = by_ij[0:8]
        for g in range(1, tall):
            packed = packed + pltpu.roll(by_ij[g * 8:g * 8 + 8], g * width, 1)
        pads = [jnp.zeros((free, LANES), F32), total]
        if free + width < LANES:
            pads.append(jnp.zeros((LANES - free - width, LANES), F32))
        spread = jnp.concatenate(pads, 0)
        by_row = lax.dot_general(
            jnp.ones((8, LANES), F32), spread, NT, precision=EXACT, preferred_element_type=F32)
        by_col = lax.dot_general(
            jnp.ones((8, width), F32), total, NN, precision=EXACT, preferred_element_type=F32)
        folded = by_col
        for g in range(1, groups):
            folded = folded + pltpu.roll(by_col, g * width, 1)
        packed = packed * jnp.where(diag, 0.5, 1.0)
        first = jnp.where(diag, (by_row + folded) * 0.5, by_row)
        second = jnp.where(diag, 0.0, folded)
        out = jnp.where(l8 < free, packed, jnp.where(r8 == 0, first, jnp.where(r8 == 1, second, 0.0)))

        @pl.when(t == 0)
        def _():
            message[...] = out

        @pl.when(t == 1)
        def _():
            message[...] += out

        return c

    lax.fori_loop(0, n_tiles, tile, 0)

    def tell(k, c):
        t = lax.rem(me + k, n)
        pltpu.make_async_remote_copy(
            src_ref=message, dst_ref=slots.at[me],
            send_sem=msg_send, recv_sem=msg_recv,
            device_id={"virt": t // n_aux, "aux": lax.rem(t, n_aux)},
            device_id_type=MESH,
        ).start()
        return c

    lax.fori_loop(1, n, tell, 0)
    slots[me] = message[...]
    for k in list(range(2, n_aux, 2)) + [1]:
        share_own(k).wait_send()
    for k in range(2, n_aux, 2):
        hand_on(k).wait_send()
    for k in range(n_aux):
        copy, wanted = share_other(k)
        pl.when(wanted)(copy.wait_send)
    everyone = slots.at[pl.ds(0, n - 1)]
    pltpu.make_async_copy(everyone, everyone, msg_send).wait()
    pltpu.make_async_copy(everyone, everyone, msg_recv).wait()

    keep = jnp.logical_or(l8 < free, r8 < 0)

    def add(k, acc):
        sv = k // n_aux
        so = virt_of(lax.rem(label_of(sv, n_virt) + pick(table, lax.rem(k, n_aux)), n_virt), n_virt)
        row0 = jnp.where(sv == v, 1.0, 0.0)
        row1 = jnp.where(so == v, 1.0, 0.0)
        weight = jnp.where(keep, 1.0, jnp.where(r8 == 0, row0, row1))
        return acc + slots[k] * weight

    done = lax.fori_loop(0, n, add, jnp.zeros((8, LANES), F32))
    done_ref[...] = done


TILES = (
    (0, 2, 1),
    (0, 2, 0),
    (0, 1, 0),
    (1, 3, 0),
    (1, 2, 0),
    (1, 3, 1),
    (0, 3, 0),
    (2, 3, 0),
    (0, 4, 0),
    (1, 4, 0),
    (2, 4, 0),
    (0, 5, 0),
    (2, 5, 0),
    (1, 5, 0),
    (3, 4, 0),
    (3, 5, 0),
    (0, 7, 0),
    (0, 6, 0),
    (2, 6, 0),
    (2, 7, 0),
    (1, 6, 0),
    (1, 7, 0),
    (3, 6, 0),
    (3, 7, 0),
    (6, 7, 0),
    (7, 5, 1),
    (6, 4, 1),
    (7, 4, 0),
    (6, 5, 0),
    (6, 4, 0),
    (7, 5, 0),
    (4, 5, 0),
)
ROUTES = (
    ((2, 16, 12), (16,), (), (2, 34, 16), (), (), (3, 9), (3, 9), ()),
    ((4,), (0, 4), (), (), (1,), (1,), (), (), ()),
    ((), (12, 22), (12, 16, 22, 2), (12, 22), (), (), (), (18,), ()),
    ((5,), (5,), (5,), (5,), (), (), (), (), (4, 0)),
    ((10,), (6,), (10,), (10,), (), (14,), (), (24, 14), ()),
    ((26, 6), (8, 26), (26,), (), (), (), (7,), (), ()),
    ((), (), (), (), (15, 7), (15, 7), (11,), (15,), (8, 6)),
    ((), (), (), (), (), (), (13,), (7, 11), (6, 42, 8)),
    ((34, 22), (), (32, 0), (), (21,), (19, 21), (19,), (19,), (20, 24, 3)),
    ((), (), (), (), (17, 29), (), (), (), (9, 36, 24, 3)),
    ((36, 38), (), (24, 36, 1), (), (), (29,), (17, 29), (17, 29), ()),
    ((), (32,), (), (), (), (), (), (), (1, 20, 36)),
    ((9,), (), (14,), (), (27,), (), (), (), (13, 46, 11)),
    ((42, 18), (40, 18), (40, 18), (), (), (25, 31), (25,), (25,), (28, 11)),
    ((), (30, 13), (15, 30, 46), (44,), (), (), (), (), ()),
    ((28,), (44,), (44,), (28, 13), (), (23,), (27, 23), (23, 27), ()),
    ((), (34,), (34,), (), (), (), (39,), (43, 50), (55, 19, 59)),
    ((32,), (), (), (32,), (37,), (), (), (41,), (17, 55)),
    ((14,), (38,), (38,), (38,), (52, 45), (45,), (35,), (), (21, 62, 55)),
    ((), (20,), (), (), (), (), (), (), (21, 62)),
    ((), (42,), (42,), (26,), (), (35,), (58,), (), (57, 25, 23, 51)),
    ((40,), (), (), (40,), (47, 39), (33, 47), (), (47,), (27, 57)),
    ((), (46,), (), (46,), (), (), (41, 37), (), (51, 31, 61)),
    ((44, 30), (), (), (), (), (39,), (43,), (), (31, 57, 63)),
    ((35, 58), (37, 52), (), (35, 58), (54,), (50,), (), (), ()),
    ((49, 33), (), (49, 54), (49,), (), (), (57,), (), (48, 56)),
    ((), (), (45, 48), (), (62,), (62,), (), (), ()),
    ((), (), (), (39,), (53,), (53,), (53,), (53,), (52, 48, 45, 37)),
    ((41,), (58, 41), (), (), (61,), (63, 51), (), (51,), (50, 43, 60)),
    ((56,), (), (56,), (56,), (), (), (), (), (43, 60, 49)),
    ((), (54,), (33, 50, 47), (), (63, 31), (), (63,), (), ()),
    ((), (59,), (59,), (59, 55), (), (61,), (), (61,), (33, 60, 54)),
)
STEPS = (
    (0, 1, 2, 3, 14, 15, 6, 7, 8, 9, 12, 10, 13, 4, 11, 5),
    (2, 3, 0, 1, 14, 8, 15, 9, 6, 10, 7, 11, 12, 4, 13, 5),
    (4, 5, 6, 7, 2, 3, 14, 15, 12, 8, 13, 9, 10, 0, 11, 1),
    (6, 7, 4, 0, 5, 1, 8, 2, 9, 3, 14, 15, 12, 10, 13, 11),
    (0, 1, 2, 3, 4, 10, 5, 11, 6, 7, 14, 15, 12, 8, 13, 9),
    (2, 3, 0, 1, 4, 10, 5, 11, 6, 12, 7, 13, 8, 14, 9, 15),
    (4, 8, 5, 12, 9, 6, 14, 13, 0, 2, 15, 1, 3, 10, 7, 11),
    (12, 13, 8, 9, 14, 15, 4, 10, 5, 2, 11, 6, 0, 7, 1, 3),
    (0, 10, 4, 1, 11, 5, 2, 14, 3, 8, 12, 9, 15, 13, 6, 7),
    (10, 8, 11, 2, 9, 14, 3, 12, 15, 0, 13, 4, 6, 5, 7, 1),
    (4, 5, 6, 7, 0, 14, 1, 12, 15, 10, 13, 11, 2, 3, 8, 9),
    (6, 14, 2, 8, 15, 3, 12, 4, 10, 5, 9, 13, 11, 0, 1, 7),
    (0, 4, 1, 10, 5, 2, 11, 3, 8, 14, 9, 15, 12, 6, 13, 7),
    (2, 10, 3, 11, 0, 14, 1, 15, 4, 8, 12, 5, 9, 13, 6, 7),
    (4, 5, 6, 7, 2, 3, 14, 12, 15, 0, 8, 10, 1, 9, 13, 11),
    (6, 7, 4, 5, 14, 15, 2, 12, 3, 10, 13, 11, 0, 1, 8, 9),
    (14, 15, 10, 4, 12, 0, 11, 13, 8, 6, 2, 9, 7, 3, 5, 1),
    (8, 9, 0, 14, 4, 6, 15, 7, 1, 2, 12, 10, 3, 13, 5, 11),
    (6, 2, 7, 3, 4, 0, 10, 1, 11, 8, 12, 5, 9, 13, 14, 15),
    (6, 2, 7, 3, 4, 14, 5, 10, 8, 11, 15, 0, 9, 12, 1, 13),
    (6, 2, 7, 3, 12, 10, 13, 11, 0, 8, 4, 1, 14, 9, 5, 15),
    (10, 6, 11, 7, 8, 9, 2, 14, 0, 3, 15, 1, 12, 4, 13, 5),
    (12, 0, 6, 13, 1, 7, 14, 2, 15, 3, 10, 11, 4, 8, 9, 5),
    (0, 1, 6, 10, 7, 11, 12, 2, 8, 13, 4, 3, 9, 14, 5, 15),
    (0, 1, 2, 3, 6, 8, 7, 10, 9, 11, 14, 12, 4, 15, 13, 5),
    (0, 12, 1, 2, 13, 6, 3, 4, 8, 7, 5, 9, 14, 10, 11, 15),
    (4, 5, 6, 7, 10, 11, 8, 2, 9, 12, 3, 13, 14, 0, 15, 1),
    (10, 6, 11, 7, 8, 9, 12, 0, 13, 14, 1, 15, 2, 4, 3, 5),
    (8, 2, 9, 3, 14, 10, 15, 11, 0, 1, 6, 12, 7, 4, 5, 13),
    (2, 0, 3, 14, 1, 15, 6, 12, 7, 13, 4, 10, 5, 8, 11, 9),
    (4, 5, 6, 7, 2, 3, 0, 8, 12, 9, 13, 14, 10, 1, 11, 15),
    (6, 7, 4, 5, 2, 8, 14, 12, 10, 3, 9, 11, 0, 15, 13, 1),
)
PLANS = {(8, 4): (TILES, ROUTES, STEPS)}


KIDS = 4
CODE = 128


def table_kernel(
    n_virt, n_aux, occ, plan,
    x_ref, occ_ref, virt_ref,
    done_ref,
    held, lhs, rhs, order, order_t, ints, sums, message, slots,
    own_sem, send_sem, recv_sem, msg_send, msg_recv,
):
    rows, cols = x_ref.shape
    pitch = -(-rows // 16) * 16
    width = cols // occ
    groups = LANES // width
    supers = occ // groups
    n = n_virt * n_aux
    v = lax.axis_index("virt")
    p = lax.axis_index("aux")
    me = v * n_aux + p
    tiles, routes, steps = plan
    half = -(-rows // 32) * 16
    cuts = ((0, half), (half, rows - half))
    n_slots = 2 * n_aux

    def device(t):
        return {"virt": lax.div(t, n_aux), "aux": lax.rem(t, n_aux)}

    barrier = pltpu.get_barrier_semaphore()

    def greet(k, c):
        t = me + k
        t = jnp.where(t >= n, t - n, t)
        pl.semaphore_signal(barrier, inc=1, device_id=device(t), device_id_type=MESH)
        return c

    side_a = pick([t[0] for t in tiles], me)
    side_b = pick([t[1] for t in tiles], me)
    diag = pick([t[2] for t in tiles], me) == 1
    own_slot = jnp.where(side_a == v, p, jnp.where(side_b == v, n_aux + p, n_slots))
    own = pltpu.make_async_copy(x_ref, held.at[own_slot], own_sem)
    own.start()
    lax.fori_loop(1, n, greet, 0)

    def packed(codes):
        got = 0
        for c in reversed(codes):
            got = got * CODE + c + 1
        return got

    kids = [pick([packed(r[s]) for r in routes], me) for s in range(n_slots + 1)]
    todo = [pick([r[i] for r in steps], me) for i in range(2 * n_slots)]

    row = lax.broadcasted_iota(jnp.int32, (cols, cols), 0)
    col = lax.broadcasted_iota(jnp.int32, (cols, cols), 1)
    hit = col == lax.rem(row, width) * occ + row // width
    order[...] = jnp.where(hit, 1.0, 0.0).astype(BF16)
    hit = row == lax.rem(col, width) * occ + col // width
    order_t[...] = jnp.where(hit, 1.0, 0.0).astype(BF16)
    lhs[...] = jnp.zeros_like(lhs)
    rhs[...] = jnp.zeros_like(rhs)

    own.wait()
    pl.semaphore_wait(barrier, n - 1)

    def piece(slot, part):
        return held.at[slot, pl.ds(cuts[part][0], cuts[part][1])]

    def copies(slot, part, act):
        code = pick(kids, slot)
        q = jnp.where(slot == n_slots, p, lax.rem(slot, n_aux))
        for k in range(KIDS):
            this = lax.rem(code, CODE)
            code = lax.div(code, CODE)

            @pl.when(this > 0)
            def _():
                t = this - 1
                to = lax.rem(t, 2) * n_aux + q
                copy = pltpu.make_async_remote_copy(
                    src_ref=piece(slot, part), dst_ref=piece(to, part),
                    send_sem=send_sem.at[slot, part, k], recv_sem=recv_sem.at[to, part],
                    device_id=device(lax.div(t, 2)), device_id_type=MESH,
                )
                act(copy)

    for part in range(2):
        copies(own_slot, part, lambda copy: copy.start())

    def take(i, c):
        entry = pick(todo, i)
        slot = lax.div(entry, 2)
        later = lax.rem(entry, 2)
        away = slot != own_slot
        for part in range(2):

            @pl.when(jnp.logical_and(later == part, away))
            def _():
                whole = piece(slot, part)
                pltpu.make_async_copy(whole, whole, recv_sem.at[slot, part]).wait()
                copies(slot, part, lambda copy: copy.start())

        side = lax.div(slot, n_aux)
        for q in range(n_aux):
            here = jnp.logical_and(later == 1, lax.rem(slot, n_aux) == q)

            @pl.when(jnp.logical_and(here, jnp.logical_or(side == 0, diag)))
            def _():
                lhs[side, :, q * pitch:q * pitch + rows] = lax.dot_general(
                    order[...], held[slot], NT, preferred_element_type=F32
                ).astype(BF16)

            @pl.when(jnp.logical_and(here, jnp.logical_or(side == 1, diag)))
            def _():
                rhs[side, q * pitch:q * pitch + rows, :] = lax.dot_general(
                    held[slot], order_t[...], NN, preferred_element_type=F32
                ).astype(BF16)

        return c

    lax.fori_loop(0, 2 * n_slots, take, 0)

    lane = lax.broadcasted_iota(jnp.int32, (1, LANES), 1)
    part = lane // width
    down = lax.broadcasted_iota(jnp.int32, (width, 1), 0)
    lane_in = lax.rem(lane, width)

    def eps_down(which):
        got = jnp.zeros((width, 1), F32)
        for k in range(width):
            got = jnp.where(down == k, virt_ref[which * width + k], got)
        return got

    def eps_across(which):
        got = jnp.zeros((1, LANES), F32)
        for k in range(width):
            got = jnp.where(lane_in == k, virt_ref[which * width + k], got)
        return got

    occ_lane = []
    for cj in range(supers):
        got = jnp.zeros((1, LANES), F32)
        for t in range(groups):
            got = jnp.where(part == t, occ_ref[cj * groups + t], got)
        occ_lane.append(got)

    tall = -(-occ // 8)
    sums[...] = jnp.zeros_like(sums)
    n_tiles = jnp.where(diag, 2, 1)
    r8 = lax.broadcasted_iota(jnp.int32, (8, LANES), 0)
    l8 = lax.broadcasted_iota(jnp.int32, (8, LANES), 1)
    free = tall * width

    def tile(t, c):
        left = t
        right = jnp.where(diag, t, 1)
        ints[...] = lax.dot_general(lhs[left], rhs[right], NN, preferred_element_type=F32)
        block_l = jnp.where(left == 0, side_a, side_b)
        block_r = jnp.where(right == 0, side_a, side_b)
        base = -(eps_down(block_l) + eps_across(block_r))
        total = jnp.zeros((width, LANES), F32)
        for ci in range(supers):
            for cj in range(ci, supers):
                turned = []
                for g in range(groups):
                    block = ints[pl.ds((cj * groups + g) * width, width), pl.ds(ci * LANES, LANES)]
                    turned.append([block if r == 0 else pltpu.roll(block, r * width, 1) for r in range(groups)])
                for s in range(groups):
                    i = ci * groups + s
                    direct = ints[pl.ds(i * width, width), pl.ds(cj * LANES, LANES)]
                    swapped = turned[0][(0 - s) % groups]
                    for g in range(1, groups):
                        swapped = jnp.where(part == g, turned[g][(g - s) % groups], swapped)
                    below = base + (occ_lane[cj] + occ_ref[i])
                    if ci == cj:
                        term = direct * (2.0 * direct - swapped) / below
                    else:
                        term = 2.0 * (direct * (direct - swapped) + swapped * swapped) / below
                    total = total + term
                    short = term[0:8]
                    for m in range(8, width, 8):
                        short = short + term[m:m + 8]
                    sums[i * 8:i * 8 + 8, cj * LANES:(cj + 1) * LANES] = short

        wide = lax.broadcasted_iota(jnp.int32, (cols, LANES), 0)
        thin = lax.broadcasted_iota(jnp.int32, (cols, LANES), 1)
        fold = jnp.where(wide // width == thin, 1.0, 0.0)
        by_j = lax.dot_general(sums[...], fold, NN, precision=EXACT, preferred_element_type=F32)
        ri = lax.broadcasted_iota(jnp.int32, (tall * 8, occ * 8), 0)
        rj = lax.broadcasted_iota(jnp.int32, (tall * 8, occ * 8), 1)
        by_ij = lax.dot_general(
            jnp.where(rj // 8 == ri, 1.0, 0.0), by_j, NN,
            precision=EXACT, preferred_element_type=F32,
        )
        packed_ij = by_ij[0:8]
        for g in range(1, tall):
            packed_ij = packed_ij + pltpu.roll(by_ij[g * 8:g * 8 + 8], g * width, 1)
        pads = [jnp.zeros((free, LANES), F32), total]
        if free + width < LANES:
            pads.append(jnp.zeros((LANES - free - width, LANES), F32))
        spread = jnp.concatenate(pads, 0)
        by_row = lax.dot_general(
            jnp.ones((8, LANES), F32), spread, NT, precision=EXACT, preferred_element_type=F32)
        by_col = lax.dot_general(
            jnp.ones((8, width), F32), total, NN, precision=EXACT, preferred_element_type=F32)
        folded = by_col
        for g in range(1, groups):
            folded = folded + pltpu.roll(by_col, g * width, 1)
        packed_ij = packed_ij * jnp.where(diag, 0.5, 1.0)
        both = (by_row + folded) * 0.5
        first = jnp.where(diag, jnp.where(t == 0, both, 0.0), by_row)
        second = jnp.where(diag, jnp.where(t == 1, both, 0.0), folded)
        out = jnp.where(l8 < free, packed_ij, jnp.where(r8 == 0, first, jnp.where(r8 == 1, second, 0.0)))

        @pl.when(t == 0)
        def _():
            message[...] = out

        @pl.when(t == 1)
        def _():
            message[...] += out

        return c

    lax.fori_loop(0, n_tiles, tile, 0)

    def tell(k, c):
        t = me + k
        t = jnp.where(t >= n, t - n, t)
        pltpu.make_async_remote_copy(
            src_ref=message, dst_ref=slots.at[me],
            send_sem=msg_send, recv_sem=msg_recv,
            device_id=device(t), device_id_type=MESH,
        ).start()
        return c

    lax.fori_loop(1, n, tell, 0)
    slots[me] = message[...]
    for part_at in range(2):
        copies(own_slot, part_at, lambda copy: copy.wait_send())

    def flush(s, c):
        @pl.when(s != own_slot)
        def _():
            for part_at in range(2):
                copies(s, part_at, lambda copy: copy.wait_send())

        return c

    lax.fori_loop(0, n_slots, flush, 0)
    everyone = slots.at[pl.ds(0, n - 1)]
    pltpu.make_async_copy(everyone, everyone, msg_send).wait()
    pltpu.make_async_copy(everyone, everyone, msg_recv).wait()

    keep = l8 < free
    acc = None
    for k in range(n):
        a, b, _ = tiles[k]
        row0 = jnp.where(v == a, 1.0, 0.0)
        row1 = jnp.where(v == b, 1.0, 0.0)
        term = slots[k] * jnp.where(keep, 1.0, jnp.where(r8 == 0, row0, row1))
        acc = term if acc is None else acc + term
    done_ref[...] = acc


def table_call(n_virt, n_aux, occ, plan, three_index, eps_occ, eps_virt):
    rows, cols = three_index.shape
    pitch = -(-rows // 16) * 16
    n = n_virt * n_aux
    n_slots = 2 * n_aux
    vmem = pl.BlockSpec(memory_space=pltpu.VMEM)
    smem = pl.BlockSpec(memory_space=pltpu.SMEM)
    return pl.pallas_call(
        functools.partial(table_kernel, n_virt, n_aux, occ, plan),
        out_shape=jax.ShapeDtypeStruct((8, LANES), F32),
        in_specs=[pl.BlockSpec(memory_space=pltpu.HBM), smem, smem],
        out_specs=vmem,
        scratch_shapes=[
            pltpu.VMEM((n_slots + 1, rows, cols), BF16),
            pltpu.VMEM((2, cols, n_aux * pitch), BF16),
            pltpu.VMEM((2, n_aux * pitch, cols), BF16),
            pltpu.VMEM((cols, cols), BF16),
            pltpu.VMEM((cols, cols), BF16),
            pltpu.VMEM((cols, cols), F32),
            pltpu.VMEM((occ * 8, cols), F32),
            pltpu.VMEM((8, LANES), F32),
            pltpu.VMEM((n, 8, LANES), F32),
            pltpu.SemaphoreType.DMA,
            pltpu.SemaphoreType.DMA((n_slots + 1, 2, KIDS)),
            pltpu.SemaphoreType.DMA((n_slots, 2)),
            pltpu.SemaphoreType.DMA,
            pltpu.SemaphoreType.DMA,
        ],
        compiler_params=pltpu.CompilerParams(collective_id=0, has_side_effects=True),
    )(three_index, eps_occ, eps_virt)


def unpack(occ, width, done_ref, share_ref, pair_ref):
    tall = -(-occ // 8)
    free = tall * width
    done = done_ref[...]
    share = done[0:1] + done[1:2]
    share_ref[...] = share[0, free:free + width]
    blocks = [done] + [pltpu.roll(done, LANES - g * width, 1) for g in range(1, tall)]
    square = jnp.concatenate(blocks + [jnp.zeros((LANES - 8 * tall, LANES), F32)], 0)
    square = jnp.where(lax.broadcasted_iota(jnp.int32, (LANES, LANES), 1) < occ, square, 0.0)
    pair = square + square.T
    pair_ref[...] = pair[0:occ, 0:occ]


def on_device(n_virt, n_aux, three_index, eps_occ, eps_virt):
    occ = eps_occ.shape[0]
    rows, cols = three_index.shape
    width = cols // occ
    pitch = -(-rows // 16) * 16
    n = n_virt * n_aux
    vmem = pl.BlockSpec(memory_space=pltpu.VMEM)
    smem = pl.BlockSpec(memory_space=pltpu.SMEM)
    plan = PLANS.get((n_virt, n_aux))
    if plan is not None:
        done = table_call(n_virt, n_aux, occ, plan, three_index, eps_occ, eps_virt)
    else:
        done = pl.pallas_call(
            functools.partial(kernel, n_virt, n_aux, occ),
            out_shape=jax.ShapeDtypeStruct((8, LANES), F32),
            in_specs=[vmem, smem, smem],
            out_specs=vmem,
            scratch_shapes=[
                pltpu.VMEM((2, n_aux, rows, cols), BF16),
                pltpu.VMEM((cols, n_aux * pitch), BF16),
                pltpu.VMEM((n_aux * pitch, cols), BF16),
                pltpu.VMEM((cols, cols), BF16),
                pltpu.VMEM((cols, cols), BF16),
                pltpu.VMEM((cols, cols), F32),
                pltpu.VMEM((occ * 8, cols), F32),
                pltpu.VMEM((8, LANES), F32),
                pltpu.VMEM((8, LANES), F32),
                pltpu.VMEM((n, 8, LANES), F32),
                pltpu.SemaphoreType.DMA,
                pltpu.SemaphoreType.DMA((3, n_aux)),
                pltpu.SemaphoreType.DMA((2, n_aux)),
                pltpu.SemaphoreType.DMA,
                pltpu.SemaphoreType.DMA,
            ],
            compiler_params=pltpu.CompilerParams(collective_id=0, has_side_effects=True),
        )(three_index, eps_occ, eps_virt)
    return pl.pallas_call(
        functools.partial(unpack, occ, width),
        out_shape=(
            jax.ShapeDtypeStruct((width,), F32),
            jax.ShapeDtypeStruct((occ, occ), F32),
        ),
        in_specs=[vmem],
        out_specs=(vmem, vmem),
    )(done)


def solution(mesh):
    n_virt, n_aux = mesh.shape["virt"], mesh.shape["aux"]
    assert n_virt == 2 * n_aux and n_aux % 2 == 0
    in_specs = (P("aux", "virt"), P(), P())
    out_specs = (P("virt"), P())
    return jax.shard_map(
        functools.partial(on_device, n_virt, n_aux), mesh=mesh,
        in_specs=in_specs, out_specs=out_specs, check_vma=False,
    )
```

```python
import functools

import jax
import jax.numpy as jnp
from jax import lax
from jax.experimental import pallas as pl
from jax.experimental.pallas import tpu as pltpu
from jax.sharding import PartitionSpec as P

MESH = pl.DeviceIdType.MESH
F32 = jnp.float32
BF16 = jnp.bfloat16
EXACT = lax.Precision.HIGHEST
LANES = 128
NT = (((1,), (1,)), ((), ()))
NN = (((1,), (0,)), ((), ()))


def distances(n_aux):
    return list(range(1, n_aux + 1, 2)) + list(range(2, n_aux + 1, 2))


def pick(table, at):
    got = table[0] + jnp.int32(0)
    for k in range(1, len(table)):
        got = jnp.where(at == k, table[k] + jnp.int32(0), got)
    return got


def label_of(virt, n_virt):
    return lax.rem(virt, 2) * (n_virt // 2) + virt // 2


def virt_of(label, n_virt):
    half = n_virt // 2
    return lax.rem(label, half) * 2 + label // half


def kernel(
    n_virt, n_aux, occ,
    x_ref, occ_ref, virt_ref,
    done_ref,
    held, lhs, rhs, order, order_t, ints, sums, parts, message, slots,
    own_sem, send_sem, recv_sem, msg_send, msg_recv,
):
    rows, cols = x_ref.shape
    pitch = -(-rows // 16) * 16
    width = cols // occ
    groups = LANES // width
    supers = occ // groups
    n = n_virt * n_aux
    v = lax.axis_index("virt")
    p = lax.axis_index("aux")
    me = v * n_aux + p
    table = distances(n_aux)
    label = label_of(v, n_virt)
    other = virt_of(lax.rem(label + pick(table, p), n_virt), n_virt)
    lower = label < n_virt // 2
    solo = jnp.logical_and(p == n_aux - 1, jnp.logical_not(lower))
    extra = jnp.logical_and(p == n_aux // 2 - 1, lower)

    barrier = pltpu.get_barrier_semaphore()

    def greet(k, c):
        t = lax.rem(me + k, n)
        pl.semaphore_signal(
            barrier, inc=1,
            device_id={"virt": t // n_aux, "aux": lax.rem(t, n_aux)},
            device_id_type=MESH,
        )
        return c

    lax.fori_loop(1, n, greet, 0)
    own = pltpu.make_async_copy(x_ref, held.at[0, p], own_sem)
    own.start()
    pl.semaphore_wait(barrier, n - 1)

    pairs = n_aux // 2

    def place(k):
        return lax.rem(p // 2 + k // 2, pairs) * 2 + lax.rem(p + k, 2)

    def share_own(k):
        return pltpu.make_async_remote_copy(
            src_ref=x_ref, dst_ref=held.at[0, p],
            send_sem=send_sem.at[0, k], recv_sem=recv_sem.at[0, p],
            device_id={"virt": v, "aux": place(k)}, device_id_type=MESH,
        )

    def hand_on(k):
        q = place(k)
        return pltpu.make_async_remote_copy(
            src_ref=held.at[0, q], dst_ref=held.at[0, q],
            send_sem=send_sem.at[2, k], recv_sem=recv_sem.at[0, q],
            device_id={"virt": v, "aux": place(1)}, device_id_type=MESH,
        )

    def share_other(k):
        q = place(k)
        target = lax.rem(label + n_virt - pick(table, q), n_virt)
        copy = pltpu.make_async_remote_copy(
            src_ref=x_ref, dst_ref=held.at[1, p],
            send_sem=send_sem.at[1, k], recv_sem=recv_sem.at[1, p],
            device_id={"virt": virt_of(target, n_virt), "aux": q}, device_id_type=MESH,
        )
        wanted = jnp.logical_or(q < n_aux - 1, target < n_virt // 2)
        return copy, wanted

    for k in list(range(2, n_aux, 2)) + [1]:
        share_own(k).start()
    for k in range(n_aux):
        copy, wanted = share_other(k)
        pl.when(wanted)(copy.start)

    def arrived(side, q):
        pltpu.make_async_copy(
            held.at[side, q], held.at[side, q], recv_sem.at[side, q]
        ).wait()

    row = lax.broadcasted_iota(jnp.int32, (cols, cols), 0)
    col = lax.broadcasted_iota(jnp.int32, (cols, cols), 1)
    hit = col == lax.rem(row, width) * occ + row // width
    order[...] = jnp.where(hit, 1.0, 0.0).astype(BF16)
    hit = row == lax.rem(col, width) * occ + col // width
    order_t[...] = jnp.where(hit, 1.0, 0.0).astype(BF16)
    lhs[...] = jnp.zeros_like(lhs)
    rhs[...] = jnp.zeros_like(rhs)

    def turn(k):
        lhs[:, k * pitch:k * pitch + rows] = lax.dot_general(
            order[...], held[0, place(k)], NT, preferred_element_type=F32
        ).astype(BF16)

    own.wait()
    turn(0)
    for k in range(2, n_aux, 2):
        arrived(0, place(k))
        hand_on(k).start()
        turn(k)
    for k in range(1, n_aux, 2):
        arrived(0, place(k))
        turn(k)

    lane = lax.broadcasted_iota(jnp.int32, (1, LANES), 1)
    part = lane // width
    down = lax.broadcasted_iota(jnp.int32, (width, 1), 0)
    lane_in = lax.rem(lane, width)

    def eps_down(which):
        got = jnp.zeros((width, 1), F32)
        for k in range(width):
            got = jnp.where(down == k, virt_ref[which * width + k], got)
        return got

    def eps_across(which):
        got = jnp.zeros((1, LANES), F32)
        for k in range(width):
            got = jnp.where(lane_in == k, virt_ref[which * width + k], got)
        return got

    occ_lane = []
    for cj in range(supers):
        got = jnp.zeros((1, LANES), F32)
        for t in range(groups):
            got = jnp.where(part == t, occ_ref[cj * groups + t], got)
        occ_lane.append(got)

    tall = -(-occ // 8)
    sums[...] = jnp.zeros_like(sums)
    n_tiles = jnp.where(extra, 2, 1)
    r8 = lax.broadcasted_iota(jnp.int32, (8, LANES), 0)
    l8 = lax.broadcasted_iota(jnp.int32, (8, LANES), 1)
    free = tall * width

    def tile(t, c):
        diag = jnp.logical_or(solo, jnp.logical_and(extra, t == 0))
        source = jnp.where(diag, 0, 1)

        for k in range(n_aux):

            @pl.when(source == 1)
            def _():
                arrived(1, place(k))

            rhs[k * pitch:k * pitch + rows, :] = lax.dot_general(
                held[source, place(k)], order_t[...], NN, preferred_element_type=F32
            ).astype(BF16)
        ints[...] = lax.dot_general(lhs[...], rhs[...], NN, preferred_element_type=F32)

        base = -(eps_down(v) + eps_across(jnp.where(diag, v, other)))
        total = jnp.zeros((width, LANES), F32)
        for ci in range(supers):
            for cj in range(ci, supers):
                turned = []
                for g in range(groups):
                    block = ints[pl.ds((cj * groups + g) * width, width), pl.ds(ci * LANES, LANES)]
                    turned.append([block if r == 0 else pltpu.roll(block, r * width, 1) for r in range(groups)])
                for s in range(groups):
                    i = ci * groups + s
                    direct = ints[pl.ds(i * width, width), pl.ds(cj * LANES, LANES)]
                    swapped = turned[0][(0 - s) % groups]
                    for g in range(1, groups):
                        swapped = jnp.where(part == g, turned[g][(g - s) % groups], swapped)
                    below = base + (occ_lane[cj] + occ_ref[i])
                    if ci == cj:
                        term = direct * (2.0 * direct - swapped) / below
                    else:
                        term = 2.0 * (direct * (direct - swapped) + swapped * swapped) / below
                    total = total + term
                    short = term[0:8]
                    for m in range(8, width, 8):
                        short = short + term[m:m + 8]
                    sums[i * 8:i * 8 + 8, cj * LANES:(cj + 1) * LANES] = short

        wide = lax.broadcasted_iota(jnp.int32, (cols, LANES), 0)
        thin = lax.broadcasted_iota(jnp.int32, (cols, LANES), 1)
        fold = jnp.where(wide // width == thin, 1.0, 0.0)
        by_j = lax.dot_general(sums[...], fold, NN, precision=EXACT, preferred_element_type=F32)
        ri = lax.broadcasted_iota(jnp.int32, (tall * 8, occ * 8), 0)
        rj = lax.broadcasted_iota(jnp.int32, (tall * 8, occ * 8), 1)
        by_ij = lax.dot_general(
            jnp.where(rj // 8 == ri, 1.0, 0.0), by_j, NN,
            precision=EXACT, preferred_element_type=F32,
        )
        packed = by_ij[0:8]
        for g in range(1, tall):
            packed = packed + pltpu.roll(by_ij[g * 8:g * 8 + 8], g * width, 1)
        pads = [jnp.zeros((free, LANES), F32), total]
        if free + width < LANES:
            pads.append(jnp.zeros((LANES - free - width, LANES), F32))
        spread = jnp.concatenate(pads, 0)
        by_row = lax.dot_general(
            jnp.ones((8, LANES), F32), spread, NT, precision=EXACT, preferred_element_type=F32)
        by_col = lax.dot_general(
            jnp.ones((8, width), F32), total, NN, precision=EXACT, preferred_element_type=F32)
        folded = by_col
        for g in range(1, groups):
            folded = folded + pltpu.roll(by_col, g * width, 1)
        packed = packed * jnp.where(diag, 0.5, 1.0)
        first = jnp.where(diag, (by_row + folded) * 0.5, by_row)
        second = jnp.where(diag, 0.0, folded)
        out = jnp.where(l8 < free, packed, jnp.where(r8 == 0, first, jnp.where(r8 == 1, second, 0.0)))

        @pl.when(t == 0)
        def _():
            message[...] = out

        @pl.when(t == 1)
        def _():
            message[...] += out

        return c

    lax.fori_loop(0, n_tiles, tile, 0)

    def tell(k, c):
        t = lax.rem(me + k, n)
        pltpu.make_async_remote_copy(
            src_ref=message, dst_ref=slots.at[me],
            send_sem=msg_send, recv_sem=msg_recv,
            device_id={"virt": t // n_aux, "aux": lax.rem(t, n_aux)},
            device_id_type=MESH,
        ).start()
        return c

    lax.fori_loop(1, n, tell, 0)
    slots[me] = message[...]
    for k in list(range(2, n_aux, 2)) + [1]:
        share_own(k).wait_send()
    for k in range(2, n_aux, 2):
        hand_on(k).wait_send()
    for k in range(n_aux):
        copy, wanted = share_other(k)
        pl.when(wanted)(copy.wait_send)
    everyone = slots.at[pl.ds(0, n - 1)]
    pltpu.make_async_copy(everyone, everyone, msg_send).wait()
    pltpu.make_async_copy(everyone, everyone, msg_recv).wait()

    keep = jnp.logical_or(l8 < free, r8 < 0)

    def add(k, acc):
        sv = k // n_aux
        so = virt_of(lax.rem(label_of(sv, n_virt) + pick(table, lax.rem(k, n_aux)), n_virt), n_virt)
        row0 = jnp.where(sv == v, 1.0, 0.0)
        row1 = jnp.where(so == v, 1.0, 0.0)
        weight = jnp.where(keep, 1.0, jnp.where(r8 == 0, row0, row1))
        return acc + slots[k] * weight

    done = lax.fori_loop(0, n, add, jnp.zeros((8, LANES), F32))
    done_ref[...] = done


TILES = (
    (0, 2, 1),
    (0, 2, 0),
    (0, 1, 0),
    (1, 2, 0),
    (1, 3, 0),
    (0, 3, 0),
    (1, 3, 1),
    (2, 3, 0),
    (0, 4, 0),
    (0, 5, 0),
    (2, 4, 0),
    (2, 5, 0),
    (1, 4, 0),
    (3, 4, 0),
    (1, 5, 0),
    (3, 5, 0),
    (0, 6, 0),
    (0, 7, 0),
    (2, 6, 0),
    (2, 7, 0),
    (1, 6, 0),
    (1, 7, 0),
    (3, 6, 0),
    (3, 7, 0),
    (6, 7, 0),
    (6, 4, 0),
    (7, 4, 0),
    (6, 4, 1),
    (6, 5, 0),
    (7, 5, 0),
    (4, 5, 0),
    (7, 5, 1),
)
ROUTES = (
    ((2, 10, 34), (10, 4), (2,), (16, 10), (3,), (), (), (3,), ()),
    ((4, 18), (0, 16), (), (), (14,), (1,), (1,), (), ()),
    ((), (), (10, 18), (34,), (), (), (), (), ()),
    ((), (), (5,), (5,), (), (14,), (3, 14, 22), (1, 14), (0, 4)),
    ((5, 24, 12), (5, 40, 24), (), (24,), (), (11,), (), (11,), ()),
    ((), (), (0,), (), (9, 13), (), (), (), (8, 12)),
    ((28, 6), (6, 28), (6, 28), (28, 8), (15,), (15,), (15, 11), (15,), ()),
    ((), (), (), (), (), (), (), (), (12, 6)),
    ((), (18, 34), (32,), (2, 18), (21,), (), (25,), (), (1, 36, 22)),
    ((16,), (), (16,), (), (23,), (), (), (), (20, 3)),
    ((), (22, 38, 7), (7, 38), (7,), (), (), (17,), (25,), ()),
    ((20, 7), (), (), (20, 36), (), (), (31, 19), (19,), ()),
    ((42,), (), (8, 42), (), (17, 27), (), (27,), (27,), (11, 26, 44, 30)),
    ((), (30, 9), (), (9,), (), (25,), (), (), ()),
    ((), (), (24,), (42,), (), (23, 31), (), (31,), (13, 30)),
    ((), (44, 13), (26, 44, 9), (26, 46, 13), (29,), (), (), (), ()),
    ((), (), (34,), (), (37, 45), (37, 41), (), (48, 41), (25, 51)),
    ((32,), (32,), (), (32,), (), (39,), (), (), (53, 27, 51, 17)),
    ((38,), (), (), (38,), (), (54, 45), (), (33, 45), (21, 55)),
    ((), (36,), (36,), (), (), (), (), (35,), (53, 21, 55)),
    ((), (42,), (), (), (), (), (), (), (19, 59, 31)),
    ((40,), (), (40,), (40,), (47, 35), (35, 47), (58, 35), (), (59, 29, 57, 19)),
    ((46,), (46,), (46,), (), (), (), (37, 41), (), (23, 61, 29)),
    ((), (), (), (44,), (), (62,), (), (39,), (63, 23, 29)),
    ((50, 56, 54), (56,), (), (), (), (52,), (), (), ()),
    ((33,), (33, 48), (48, 56, 33), (), (55, 60), (), (), (17,), ()),
    ((39,), (), (49,), (), (), (55, 60, 21), (60,), (51, 60), (50, 54)),
    ((), (), (45,), (37, 56), (53,), (), (51, 53), (), ()),
    ((41,), (), (), (50,), (), (), (59,), (), (58, 62, 43)),
    ((49,), (43, 49), (), (43, 49), (57, 63), (61,), (), (57,), ()),
    ((), (), (), (), (), (63,), (63,), (59,), (52, 62, 39, 47)),
    ((52,), (), (43,), (47, 52, 58), (61,), (), (57,), (61,), ()),
)
STEPS = (
    (0, 1, 2, 3, 6, 8, 7, 9, 10, 12, 4, 11, 14, 13, 5, 15),
    (2, 3, 0, 1, 8, 10, 9, 12, 11, 13, 4, 6, 14, 5, 7, 15),
    (4, 5, 6, 7, 8, 12, 9, 14, 10, 13, 11, 2, 15, 3, 0, 1),
    (4, 12, 6, 13, 5, 14, 7, 15, 2, 10, 3, 11, 0, 8, 1, 9),
    (0, 1, 2, 3, 8, 6, 10, 9, 7, 14, 11, 15, 4, 12, 5, 13),
    (0, 8, 4, 1, 9, 5, 2, 3, 10, 6, 12, 14, 7, 13, 11, 15),
    (4, 5, 6, 7, 2, 12, 3, 13, 0, 14, 1, 15, 8, 10, 9, 11),
    (12, 13, 4, 14, 5, 15, 6, 8, 10, 7, 11, 9, 0, 2, 1, 3),
    (2, 3, 4, 12, 5, 6, 8, 13, 7, 10, 9, 11, 14, 0, 15, 1),
    (4, 8, 2, 5, 9, 3, 6, 14, 7, 12, 0, 10, 15, 1, 11, 13),
    (4, 5, 6, 7, 2, 12, 3, 13, 14, 15, 0, 1, 10, 11, 8, 9),
    (6, 7, 12, 2, 14, 0, 3, 15, 1, 13, 4, 8, 5, 9, 10, 11),
    (0, 8, 1, 9, 4, 10, 2, 5, 11, 3, 12, 14, 6, 13, 15, 7),
    (2, 3, 0, 1, 6, 7, 8, 4, 10, 9, 11, 12, 14, 5, 13, 15),
    (4, 5, 6, 10, 7, 11, 2, 14, 0, 15, 8, 1, 12, 9, 3, 13),
    (6, 7, 4, 5, 2, 3, 12, 10, 8, 11, 14, 9, 0, 15, 1, 13),
    (10, 11, 8, 9, 0, 14, 2, 12, 6, 15, 3, 13, 7, 4, 1, 5),
    (0, 2, 10, 6, 3, 11, 7, 8, 1, 14, 12, 15, 4, 13, 5, 9),
    (6, 14, 0, 7, 15, 1, 10, 11, 2, 8, 4, 3, 12, 5, 9, 13),
    (6, 0, 7, 1, 14, 2, 15, 4, 3, 12, 10, 8, 5, 13, 11, 9),
    (2, 10, 3, 11, 8, 0, 1, 6, 12, 4, 14, 9, 7, 13, 5, 15),
    (10, 11, 8, 12, 9, 2, 0, 13, 3, 1, 14, 6, 4, 15, 7, 5),
    (0, 6, 1, 4, 7, 2, 12, 3, 13, 14, 15, 8, 10, 9, 5, 11),
    (6, 14, 7, 15, 0, 1, 4, 10, 2, 11, 12, 3, 8, 13, 5, 9),
    (0, 1, 2, 3, 10, 11, 4, 8, 5, 9, 14, 6, 12, 15, 7, 13),
    (2, 3, 0, 1, 4, 5, 8, 14, 9, 15, 10, 6, 12, 11, 7, 13),
    (14, 4, 10, 15, 5, 11, 6, 12, 0, 2, 13, 1, 7, 8, 3, 9),
    (6, 7, 4, 5, 10, 0, 12, 11, 1, 13, 14, 8, 15, 9, 2, 3),
    (0, 6, 1, 7, 8, 2, 4, 10, 9, 5, 11, 3, 12, 14, 13, 15),
    (2, 3, 0, 1, 10, 8, 11, 6, 9, 7, 14, 4, 12, 5, 15, 13),
    (12, 14, 13, 6, 10, 2, 15, 3, 11, 8, 7, 4, 9, 0, 5, 1),
    (6, 7, 4, 5, 14, 0, 1, 12, 15, 13, 8, 10, 9, 11, 2, 3),
)
PARTNERS = (
    (1, 2, 4, 8, 3, 5, 17),
    (0, 3, 5, 9, 2, 7, 8),
    (3, 0, 6, 10, 1, 4, 5, 9, 17),
    (2, 1, 7, 11, 0, 6, 10),
    (5, 6, 0, 12, 2, 13, 15, 20),
    (4, 7, 1, 13, 0, 2, 6, 12),
    (7, 4, 2, 14, 3, 5, 15),
    (6, 5, 3, 15, 1),
    (9, 10, 12, 0, 16, 1, 11, 17, 18, 25),
    (8, 11, 13, 1, 17, 2, 10, 20, 21),
    (11, 8, 14, 2, 18, 3, 9, 12, 19, 26),
    (10, 9, 15, 3, 19, 8, 14, 18, 22, 23),
    (13, 14, 8, 4, 20, 5, 10, 15, 16, 21, 22),
    (12, 15, 9, 5, 21, 4, 17),
    (15, 12, 10, 6, 22, 11, 21, 23),
    (14, 13, 11, 7, 23, 4, 6, 12, 20, 22),
    (17, 18, 20, 8, 24, 12, 22, 25),
    (16, 19, 21, 9, 25, 0, 2, 8, 13, 26),
    (19, 16, 22, 10, 26, 8, 11, 27),
    (18, 17, 23, 11, 27, 10, 26, 30),
    (21, 22, 16, 12, 28, 4, 9, 15, 29),
    (20, 23, 17, 13, 29, 9, 12, 14, 28, 31),
    (23, 20, 18, 14, 30, 11, 12, 15, 16, 27),
    (22, 21, 19, 15, 31, 11, 14, 30),
    (25, 26, 28, 16, 27, 29),
    (24, 27, 29, 17, 8, 16, 26, 28, 30),
    (27, 24, 30, 18, 10, 17, 19, 25, 31),
    (26, 25, 31, 19, 18, 22, 24, 28),
    (29, 30, 24, 20, 21, 25, 27, 31),
    (28, 31, 25, 21, 20, 24, 30),
    (31, 28, 26, 22, 19, 23, 25, 29),
    (30, 29, 27, 23, 21, 26, 28),
)
NEAR = (4, 4, 4, 4, 4, 4, 4, 4, 5, 5, 5, 5, 5, 5, 5, 5, 5, 5, 5, 5, 5, 5, 5, 5, 4, 4, 4, 4, 4, 4, 4, 4)
NEWS = (
    (8, 8, 12),
    (4, 9, 11),
    (5, 7, 14),
    (2, 8, 12),
    (4, 10, 12),
    (5, 9, 15),
    (8, 12, 15),
    (0, 4, 6),
    (2, 6, 12),
    (2, 6, 7),
    (8, 11, 13),
    (3, 9, 14),
    (3, 5, 11),
    (6, 10, 11),
    (2, 3, 10),
    (6, 6, 12),
    (1, 3, 4),
    (0, 0, 7),
    (4, 7, 10),
    (0, 5, 7),
    (0, 0, 4),
    (1, 2, 12),
    (1, 7, 11),
    (3, 8, 10),
    (5, 7, 10),
    (5, 9, 15),
    (4, 8, 13),
    (4, 10, 11),
    (1, 4, 12),
    (5, 9, 11),
    (0, 5, 9),
    (6, 10, 10),
)
PLANS = {(8, 4): (TILES, ROUTES, STEPS, PARTNERS, NEAR, NEWS)}


KIDS = 4
CODE = 128


def table_kernel(
    n_virt, n_aux, occ, plan,
    x_ref, occ_hbm, virt_hbm,
    done_ref,
    held, lhs, rhs, order, order_t, ints, sums, message, slots, occ_ref, virt_ref,
    own_sem, eps_sem, send_sem, recv_sem, msg_send, msg_recv, news_sem,
):
    rows, cols = x_ref.shape
    pitch = -(-rows // 16) * 16
    width = cols // occ
    groups = LANES // width
    supers = occ // groups
    n = n_virt * n_aux
    v = lax.axis_index("virt")
    p = lax.axis_index("aux")
    me = v * n_aux + p
    tiles, routes, steps, partners, n_near, news = plan
    rounds = len(news[0]) + 1
    half = -(-rows // 32) * 16
    cuts = ((0, half), (half, rows - half))
    n_slots = 2 * n_aux

    def device(t):
        return {"virt": lax.div(t, n_aux), "aux": lax.rem(t, n_aux)}

    barrier = pltpu.get_barrier_semaphore()

    side_a = pick([t[0] for t in tiles], me)
    side_b = pick([t[1] for t in tiles], me)
    diag = pick([t[2] for t in tiles], me) == 1
    own_slot = jnp.where(side_a == v, p, jnp.where(side_b == v, n_aux + p, n_slots))
    own = pltpu.make_async_copy(x_ref, held.at[own_slot], own_sem)
    own.start()
    eps = (
        pltpu.make_async_copy(occ_hbm, occ_ref, eps_sem.at[0]),
        pltpu.make_async_copy(virt_hbm, virt_ref, eps_sem.at[1]),
    )
    for copy in eps:
        copy.start()

    def packed(codes):
        got = 0
        for c in reversed(codes):
            got = got * CODE + c + 1
        return got

    most = max(len(r) for r in partners)
    folk = [
        pick([packed(r[at:at + KIDS]) for r in partners], me) for at in range(0, most, KIDS)
    ]
    n_folk = pick([len(r) for r in partners], me)
    near = pick(n_near, me)

    def signal(sem, amount, limit):
        code = None
        for k in range(amount):
            code = folk[k // KIDS] if k % KIDS == 0 else lax.div(code, CODE)

            @pl.when(k < limit)
            def _():
                t = lax.rem(code, CODE) - 1
                pl.semaphore_signal(sem, inc=1, device_id=device(t), device_id_type=MESH)

    signal(barrier, most, n_folk)

    kids = [pick([packed(r[s]) for r in routes], me) for s in range(n_slots + 1)]
    spread_at = [pick([r[k] for r in news], me) for k in range(rounds - 1)]
    todo = [pick([r[i] for r in steps], me) for i in range(2 * n_slots)]

    row = lax.broadcasted_iota(jnp.int32, (cols, cols), 0)
    col = lax.broadcasted_iota(jnp.int32, (cols, cols), 1)
    hit = col == lax.rem(row, width) * occ + row // width
    order[...] = jnp.where(hit, 1.0, 0.0).astype(BF16)
    hit = row == lax.rem(col, width) * occ + col // width
    order_t[...] = jnp.where(hit, 1.0, 0.0).astype(BF16)
    own.wait()
    pl.semaphore_wait(barrier, n_folk)

    def piece(slot, part):
        return held.at[slot, pl.ds(cuts[part][0], cuts[part][1])]

    def copies(slot, part, act):
        code = pick(kids, slot)
        q = jnp.where(slot == n_slots, p, lax.rem(slot, n_aux))
        for k in range(KIDS):
            this = lax.rem(code, CODE)
            code = lax.div(code, CODE)

            @pl.when(this > 0)
            def _():
                t = this - 1
                to = lax.rem(t, 2) * n_aux + q
                copy = pltpu.make_async_remote_copy(
                    src_ref=piece(slot, part), dst_ref=piece(to, part),
                    send_sem=send_sem.at[slot, part, k], recv_sem=recv_sem.at[to, part],
                    device_id=device(lax.div(t, 2)), device_id_type=MESH,
                )
                act(copy)

    for part in range(2):
        copies(own_slot, part, lambda copy: copy.start())
    close = max(n_near)
    signal(news_sem.at[0], close, near)
    lhs[...] = jnp.zeros_like(lhs)
    rhs[...] = jnp.zeros_like(rhs)
    for copy in eps:
        copy.wait()

    def take(i, c):
        for r in range(1, rounds):

            @pl.when(i == spread_at[r - 1])
            def _():
                pl.semaphore_wait(news_sem.at[r - 1], near)
                signal(news_sem.at[r], close, near)

        entry = pick(todo, i)
        slot = lax.div(entry, 2)
        later = lax.rem(entry, 2)
        away = slot != own_slot
        for part in range(2):

            @pl.when(jnp.logical_and(later == part, away))
            def _():
                whole = piece(slot, part)
                pltpu.make_async_copy(whole, whole, recv_sem.at[slot, part]).wait()
                copies(slot, part, lambda copy: copy.start())

        side = lax.div(slot, n_aux)
        for q in range(n_aux):
            here = jnp.logical_and(later == 1, lax.rem(slot, n_aux) == q)

            @pl.when(jnp.logical_and(here, jnp.logical_or(side == 0, diag)))
            def _():
                lhs[side, :, q * pitch:q * pitch + rows] = lax.dot_general(
                    order[...], held[slot], NT, preferred_element_type=F32
                ).astype(BF16)

            @pl.when(jnp.logical_and(here, jnp.logical_or(side == 1, diag)))
            def _():
                rhs[side, q * pitch:q * pitch + rows, :] = lax.dot_general(
                    held[slot], order_t[...], NN, preferred_element_type=F32
                ).astype(BF16)

        return c

    lax.fori_loop(0, 2 * n_slots, take, 0)

    lane = lax.broadcasted_iota(jnp.int32, (1, LANES), 1)
    part = lane // width
    down = lax.broadcasted_iota(jnp.int32, (width, 1), 0)
    lane_in = lax.rem(lane, width)

    def eps_down(which):
        got = jnp.zeros((width, 1), F32)
        for k in range(width):
            got = jnp.where(down == k, virt_ref[which * width + k], got)
        return got

    def eps_across(which):
        got = jnp.zeros((1, LANES), F32)
        for k in range(width):
            got = jnp.where(lane_in == k, virt_ref[which * width + k], got)
        return got

    occ_lane = []
    for cj in range(supers):
        got = jnp.zeros((1, LANES), F32)
        for t in range(groups):
            got = jnp.where(part == t, occ_ref[cj * groups + t], got)
        occ_lane.append(got)

    tall = -(-occ // 8)
    sums[...] = jnp.zeros_like(sums)
    n_tiles = jnp.where(diag, 2, 1)
    r8 = lax.broadcasted_iota(jnp.int32, (8, LANES), 0)
    l8 = lax.broadcasted_iota(jnp.int32, (8, LANES), 1)
    free = tall * width

    def tile(t, c):
        left = t
        right = jnp.where(diag, t, 1)
        ints[...] = lax.dot_general(lhs[left], rhs[right], NN, preferred_element_type=F32)
        block_l = jnp.where(left == 0, side_a, side_b)
        block_r = jnp.where(right == 0, side_a, side_b)
        base = -(eps_down(block_l) + eps_across(block_r))
        total = jnp.zeros((width, LANES), F32)
        for ci in range(supers):
            for cj in range(ci, supers):
                turned = []
                for g in range(groups):
                    block = ints[pl.ds((cj * groups + g) * width, width), pl.ds(ci * LANES, LANES)]
                    turned.append([block if r == 0 else pltpu.roll(block, r * width, 1) for r in range(groups)])
                for s in range(groups):
                    i = ci * groups + s
                    direct = ints[pl.ds(i * width, width), pl.ds(cj * LANES, LANES)]
                    swapped = turned[0][(0 - s) % groups]
                    for g in range(1, groups):
                        swapped = jnp.where(part == g, turned[g][(g - s) % groups], swapped)
                    below = base + (occ_lane[cj] + occ_ref[i])
                    if ci == cj:
                        term = direct * (2.0 * direct - swapped) / below
                    else:
                        term = 2.0 * (direct * (direct - swapped) + swapped * swapped) / below
                    total = total + term
                    short = term[0:8]
                    for m in range(8, width, 8):
                        short = short + term[m:m + 8]
                    sums[i * 8:i * 8 + 8, cj * LANES:(cj + 1) * LANES] = short

        wide = lax.broadcasted_iota(jnp.int32, (cols, LANES), 0)
        thin = lax.broadcasted_iota(jnp.int32, (cols, LANES), 1)
        fold = jnp.where(wide // width == thin, 1.0, 0.0)
        by_j = lax.dot_general(sums[...], fold, NN, precision=EXACT, preferred_element_type=F32)
        ri = lax.broadcasted_iota(jnp.int32, (tall * 8, occ * 8), 0)
        rj = lax.broadcasted_iota(jnp.int32, (tall * 8, occ * 8), 1)
        by_ij = lax.dot_general(
            jnp.where(rj // 8 == ri, 1.0, 0.0), by_j, NN,
            precision=EXACT, preferred_element_type=F32,
        )
        packed_ij = by_ij[0:8]
        for g in range(1, tall):
            packed_ij = packed_ij + pltpu.roll(by_ij[g * 8:g * 8 + 8], g * width, 1)
        pads = [jnp.zeros((free, LANES), F32), total]
        if free + width < LANES:
            pads.append(jnp.zeros((LANES - free - width, LANES), F32))
        spread = jnp.concatenate(pads, 0)
        by_row = lax.dot_general(
            jnp.ones((8, LANES), F32), spread, NT, precision=EXACT, preferred_element_type=F32)
        by_col = lax.dot_general(
            jnp.ones((8, width), F32), total, NN, precision=EXACT, preferred_element_type=F32)
        folded = by_col
        for g in range(1, groups):
            folded = folded + pltpu.roll(by_col, g * width, 1)
        packed_ij = packed_ij * jnp.where(diag, 0.5, 1.0)
        both = (by_row + folded) * 0.5
        first = jnp.where(diag, jnp.where(t == 0, both, 0.0), by_row)
        second = jnp.where(diag, jnp.where(t == 1, both, 0.0), folded)
        out = jnp.where(l8 < free, packed_ij, jnp.where(r8 == 0, first, jnp.where(r8 == 1, second, 0.0)))

        @pl.when(t == 0)
        def _():
            message[...] = out

        @pl.when(t == 1)
        def _():
            message[...] += out

        return c

    lax.fori_loop(0, n_tiles, tile, 0)
    pl.semaphore_wait(news_sem.at[rounds - 1], near)

    def tell(k, c):
        t = me + k
        t = jnp.where(t >= n, t - n, t)
        pltpu.make_async_remote_copy(
            src_ref=message, dst_ref=slots.at[me],
            send_sem=msg_send, recv_sem=msg_recv,
            device_id=device(t), device_id_type=MESH,
        ).start()
        return c

    lax.fori_loop(1, n, tell, 0)
    slots[me] = message[...]
    for part_at in range(2):
        copies(own_slot, part_at, lambda copy: copy.wait_send())

    def flush(s, c):
        @pl.when(s != own_slot)
        def _():
            for part_at in range(2):
                copies(s, part_at, lambda copy: copy.wait_send())

        return c

    lax.fori_loop(0, n_slots, flush, 0)
    everyone = slots.at[pl.ds(0, n - 1)]
    pltpu.make_async_copy(everyone, everyone, msg_send).wait()
    pltpu.make_async_copy(everyone, everyone, msg_recv).wait()

    keep = l8 < free
    acc = None
    for k in range(n):
        a, b, _ = tiles[k]
        row0 = jnp.where(v == a, 1.0, 0.0)
        row1 = jnp.where(v == b, 1.0, 0.0)
        term = slots[k] * jnp.where(keep, 1.0, jnp.where(r8 == 0, row0, row1))
        acc = term if acc is None else acc + term
    done_ref[...] = acc


def table_call(n_virt, n_aux, occ, plan, three_index, eps_occ, eps_virt):
    rows, cols = three_index.shape
    pitch = -(-rows // 16) * 16
    n = n_virt * n_aux
    n_slots = 2 * n_aux
    vmem = pl.BlockSpec(memory_space=pltpu.VMEM)
    hbm = pl.BlockSpec(memory_space=pltpu.HBM)
    return pl.pallas_call(
        functools.partial(table_kernel, n_virt, n_aux, occ, plan),
        out_shape=jax.ShapeDtypeStruct((8, LANES), F32),
        in_specs=[hbm, hbm, hbm],
        out_specs=vmem,
        scratch_shapes=[
            pltpu.VMEM((n_slots + 1, rows, cols), BF16),
            pltpu.VMEM((2, cols, n_aux * pitch), BF16),
            pltpu.VMEM((2, n_aux * pitch, cols), BF16),
            pltpu.VMEM((cols, cols), BF16),
            pltpu.VMEM((cols, cols), BF16),
            pltpu.VMEM((cols, cols), F32),
            pltpu.VMEM((occ * 8, cols), F32),
            pltpu.VMEM((8, LANES), F32),
            pltpu.VMEM((n, 8, LANES), F32),
            pltpu.SMEM(eps_occ.shape, F32),
            pltpu.SMEM(eps_virt.shape, F32),
            pltpu.SemaphoreType.DMA,
            pltpu.SemaphoreType.DMA((2,)),
            pltpu.SemaphoreType.DMA((n_slots + 1, 2, KIDS)),
            pltpu.SemaphoreType.DMA((n_slots, 2)),
            pltpu.SemaphoreType.DMA,
            pltpu.SemaphoreType.DMA,
            pltpu.SemaphoreType.REGULAR((len(plan[5][0]) + 1,)),
        ],
        compiler_params=pltpu.CompilerParams(collective_id=0, has_side_effects=True),
    )(three_index, eps_occ, eps_virt)


def unpack(occ, width, done_ref, share_ref, pair_ref):
    tall = -(-occ // 8)
    free = tall * width
    done = done_ref[...]
    share = done[0:1] + done[1:2]
    share_ref[...] = share[0, free:free + width]
    blocks = [done] + [pltpu.roll(done, LANES - g * width, 1) for g in range(1, tall)]
    square = jnp.concatenate(blocks + [jnp.zeros((LANES - 8 * tall, LANES), F32)], 0)
    square = jnp.where(lax.broadcasted_iota(jnp.int32, (LANES, LANES), 1) < occ, square, 0.0)
    pair = square + square.T
    pair_ref[...] = pair[0:occ, 0:occ]


def on_device(n_virt, n_aux, three_index, eps_occ, eps_virt):
    occ = eps_occ.shape[0]
    rows, cols = three_index.shape
    width = cols // occ
    pitch = -(-rows // 16) * 16
    n = n_virt * n_aux
    vmem = pl.BlockSpec(memory_space=pltpu.VMEM)
    smem = pl.BlockSpec(memory_space=pltpu.SMEM)
    plan = PLANS.get((n_virt, n_aux))
    if plan is not None:
        done = table_call(n_virt, n_aux, occ, plan, three_index, eps_occ, eps_virt)
    else:
        done = pl.pallas_call(
            functools.partial(kernel, n_virt, n_aux, occ),
            out_shape=jax.ShapeDtypeStruct((8, LANES), F32),
            in_specs=[vmem, smem, smem],
            out_specs=vmem,
            scratch_shapes=[
                pltpu.VMEM((2, n_aux, rows, cols), BF16),
                pltpu.VMEM((cols, n_aux * pitch), BF16),
                pltpu.VMEM((n_aux * pitch, cols), BF16),
                pltpu.VMEM((cols, cols), BF16),
                pltpu.VMEM((cols, cols), BF16),
                pltpu.VMEM((cols, cols), F32),
                pltpu.VMEM((occ * 8, cols), F32),
                pltpu.VMEM((8, LANES), F32),
                pltpu.VMEM((8, LANES), F32),
                pltpu.VMEM((n, 8, LANES), F32),
                pltpu.SemaphoreType.DMA,
                pltpu.SemaphoreType.DMA((3, n_aux)),
                pltpu.SemaphoreType.DMA((2, n_aux)),
                pltpu.SemaphoreType.DMA,
                pltpu.SemaphoreType.DMA,
            ],
            compiler_params=pltpu.CompilerParams(collective_id=0, has_side_effects=True),
        )(three_index, eps_occ, eps_virt)
    return pl.pallas_call(
        functools.partial(unpack, occ, width),
        out_shape=(
            jax.ShapeDtypeStruct((width,), F32),
            jax.ShapeDtypeStruct((occ, occ), F32),
        ),
        in_specs=[vmem],
        out_specs=(vmem, vmem),
    )(done)


def solution(mesh):
    n_virt, n_aux = mesh.shape["virt"], mesh.shape["aux"]
    assert n_virt == 2 * n_aux and n_aux % 2 == 0
    in_specs = (P("aux", "virt"), P(), P())
    out_specs = (P("virt"), P())
    return jax.shard_map(
        functools.partial(on_device, n_virt, n_aux), mesh=mesh,
        in_specs=in_specs, out_specs=out_specs, check_vma=False,
    )
```

```python
import functools

import jax
import jax.numpy as jnp
from jax import lax
from jax.experimental import pallas as pl
from jax.experimental.pallas import tpu as pltpu
from jax.sharding import PartitionSpec as P

MESH = pl.DeviceIdType.MESH
F32 = jnp.float32
BF16 = jnp.bfloat16
EXACT = lax.Precision.HIGHEST
LANES = 128
NT = (((1,), (1,)), ((), ()))
NN = (((1,), (0,)), ((), ()))


def distances(n_aux):
    return list(range(1, n_aux + 1, 2)) + list(range(2, n_aux + 1, 2))


def pick(table, at):
    got = table[0] + jnp.int32(0)
    for k in range(1, len(table)):
        got = jnp.where(at == k, table[k] + jnp.int32(0), got)
    return got


def label_of(virt, n_virt):
    return lax.rem(virt, 2) * (n_virt // 2) + virt // 2


def virt_of(label, n_virt):
    half = n_virt // 2
    return lax.rem(label, half) * 2 + label // half


def kernel(
    n_virt, n_aux, occ,
    x_ref, occ_ref, virt_ref,
    done_ref,
    held, lhs, rhs, order, order_t, ints, sums, parts, message, slots,
    own_sem, send_sem, recv_sem, msg_send, msg_recv,
):
    rows, cols = x_ref.shape
    pitch = -(-rows // 16) * 16
    width = cols // occ
    groups = LANES // width
    supers = occ // groups
    n = n_virt * n_aux
    v = lax.axis_index("virt")
    p = lax.axis_index("aux")
    me = v * n_aux + p
    table = distances(n_aux)
    label = label_of(v, n_virt)
    other = virt_of(lax.rem(label + pick(table, p), n_virt), n_virt)
    lower = label < n_virt // 2
    solo = jnp.logical_and(p == n_aux - 1, jnp.logical_not(lower))
    extra = jnp.logical_and(p == n_aux // 2 - 1, lower)

    barrier = pltpu.get_barrier_semaphore()

    def greet(k, c):
        t = lax.rem(me + k, n)
        pl.semaphore_signal(
            barrier, inc=1,
            device_id={"virt": t // n_aux, "aux": lax.rem(t, n_aux)},
            device_id_type=MESH,
        )
        return c

    lax.fori_loop(1, n, greet, 0)
    own = pltpu.make_async_copy(x_ref, held.at[0, p], own_sem)
    own.start()
    pl.semaphore_wait(barrier, n - 1)

    pairs = n_aux // 2

    def place(k):
        return lax.rem(p // 2 + k // 2, pairs) * 2 + lax.rem(p + k, 2)

    def share_own(k):
        return pltpu.make_async_remote_copy(
            src_ref=x_ref, dst_ref=held.at[0, p],
            send_sem=send_sem.at[0, k], recv_sem=recv_sem.at[0, p],
            device_id={"virt": v, "aux": place(k)}, device_id_type=MESH,
        )

    def hand_on(k):
        q = place(k)
        return pltpu.make_async_remote_copy(
            src_ref=held.at[0, q], dst_ref=held.at[0, q],
            send_sem=send_sem.at[2, k], recv_sem=recv_sem.at[0, q],
            device_id={"virt": v, "aux": place(1)}, device_id_type=MESH,
        )

    def share_other(k):
        q = place(k)
        target = lax.rem(label + n_virt - pick(table, q), n_virt)
        copy = pltpu.make_async_remote_copy(
            src_ref=x_ref, dst_ref=held.at[1, p],
            send_sem=send_sem.at[1, k], recv_sem=recv_sem.at[1, p],
            device_id={"virt": virt_of(target, n_virt), "aux": q}, device_id_type=MESH,
        )
        wanted = jnp.logical_or(q < n_aux - 1, target < n_virt // 2)
        return copy, wanted

    for k in list(range(2, n_aux, 2)) + [1]:
        share_own(k).start()
    for k in range(n_aux):
        copy, wanted = share_other(k)
        pl.when(wanted)(copy.start)

    def arrived(side, q):
        pltpu.make_async_copy(
            held.at[side, q], held.at[side, q], recv_sem.at[side, q]
        ).wait()

    row = lax.broadcasted_iota(jnp.int32, (cols, cols), 0)
    col = lax.broadcasted_iota(jnp.int32, (cols, cols), 1)
    hit = col == lax.rem(row, width) * occ + row // width
    order[...] = jnp.where(hit, 1.0, 0.0).astype(BF16)
    hit = row == lax.rem(col, width) * occ + col // width
    order_t[...] = jnp.where(hit, 1.0, 0.0).astype(BF16)
    lhs[...] = jnp.zeros_like(lhs)
    rhs[...] = jnp.zeros_like(rhs)

    def turn(k):
        lhs[:, k * pitch:k * pitch + rows] = lax.dot_general(
            order[...], held[0, place(k)], NT, preferred_element_type=F32
        ).astype(BF16)

    own.wait()
    turn(0)
    for k in range(2, n_aux, 2):
        arrived(0, place(k))
        hand_on(k).start()
        turn(k)
    for k in range(1, n_aux, 2):
        arrived(0, place(k))
        turn(k)

    lane = lax.broadcasted_iota(jnp.int32, (1, LANES), 1)
    part = lane // width
    down = lax.broadcasted_iota(jnp.int32, (width, 1), 0)
    lane_in = lax.rem(lane, width)

    def eps_down(which):
        got = jnp.zeros((width, 1), F32)
        for k in range(width):
            got = jnp.where(down == k, virt_ref[which * width + k], got)
        return got

    def eps_across(which):
        got = jnp.zeros((1, LANES), F32)
        for k in range(width):
            got = jnp.where(lane_in == k, virt_ref[which * width + k], got)
        return got

    occ_lane = []
    for cj in range(supers):
        got = jnp.zeros((1, LANES), F32)
        for t in range(groups):
            got = jnp.where(part == t, occ_ref[cj * groups + t], got)
        occ_lane.append(got)

    tall = -(-occ // 8)
    sums[...] = jnp.zeros_like(sums)
    n_tiles = jnp.where(extra, 2, 1)
    r8 = lax.broadcasted_iota(jnp.int32, (8, LANES), 0)
    l8 = lax.broadcasted_iota(jnp.int32, (8, LANES), 1)
    free = tall * width

    def tile(t, c):
        diag = jnp.logical_or(solo, jnp.logical_and(extra, t == 0))
        source = jnp.where(diag, 0, 1)

        for k in range(n_aux):

            @pl.when(source == 1)
            def _():
                arrived(1, place(k))

            rhs[k * pitch:k * pitch + rows, :] = lax.dot_general(
                held[source, place(k)], order_t[...], NN, preferred_element_type=F32
            ).astype(BF16)
        ints[...] = lax.dot_general(lhs[...], rhs[...], NN, preferred_element_type=F32)

        base = -(eps_down(v) + eps_across(jnp.where(diag, v, other)))
        total = jnp.zeros((width, LANES), F32)
        for ci in range(supers):
            for cj in range(ci, supers):
                turned = []
                for g in range(groups):
                    block = ints[pl.ds((cj * groups + g) * width, width), pl.ds(ci * LANES, LANES)]
                    turned.append([block if r == 0 else pltpu.roll(block, r * width, 1) for r in range(groups)])
                for s in range(groups):
                    i = ci * groups + s
                    direct = ints[pl.ds(i * width, width), pl.ds(cj * LANES, LANES)]
                    swapped = turned[0][(0 - s) % groups]
                    for g in range(1, groups):
                        swapped = jnp.where(part == g, turned[g][(g - s) % groups], swapped)
                    below = base + (occ_lane[cj] + occ_ref[i])
                    if ci == cj:
                        term = direct * (2.0 * direct - swapped) / below
                    else:
                        term = 2.0 * (direct * (direct - swapped) + swapped * swapped) / below
                    total = total + term
                    short = term[0:8]
                    for m in range(8, width, 8):
                        short = short + term[m:m + 8]
                    sums[i * 8:i * 8 + 8, cj * LANES:(cj + 1) * LANES] = short

        wide = lax.broadcasted_iota(jnp.int32, (cols, LANES), 0)
        thin = lax.broadcasted_iota(jnp.int32, (cols, LANES), 1)
        fold = jnp.where(wide // width == thin, 1.0, 0.0)
        by_j = lax.dot_general(sums[...], fold, NN, precision=EXACT, preferred_element_type=F32)
        ri = lax.broadcasted_iota(jnp.int32, (tall * 8, occ * 8), 0)
        rj = lax.broadcasted_iota(jnp.int32, (tall * 8, occ * 8), 1)
        by_ij = lax.dot_general(
            jnp.where(rj // 8 == ri, 1.0, 0.0), by_j, NN,
            precision=EXACT, preferred_element_type=F32,
        )
        packed = by_ij[0:8]
        for g in range(1, tall):
            packed = packed + pltpu.roll(by_ij[g * 8:g * 8 + 8], g * width, 1)
        pads = [jnp.zeros((free, LANES), F32), total]
        if free + width < LANES:
            pads.append(jnp.zeros((LANES - free - width, LANES), F32))
        spread = jnp.concatenate(pads, 0)
        by_row = lax.dot_general(
            jnp.ones((8, LANES), F32), spread, NT, precision=EXACT, preferred_element_type=F32)
        by_col = lax.dot_general(
            jnp.ones((8, width), F32), total, NN, precision=EXACT, preferred_element_type=F32)
        folded = by_col
        for g in range(1, groups):
            folded = folded + pltpu.roll(by_col, g * width, 1)
        packed = packed * jnp.where(diag, 0.5, 1.0)
        first = jnp.where(diag, (by_row + folded) * 0.5, by_row)
        second = jnp.where(diag, 0.0, folded)
        out = jnp.where(l8 < free, packed, jnp.where(r8 == 0, first, jnp.where(r8 == 1, second, 0.0)))

        @pl.when(t == 0)
        def _():
            message[...] = out

        @pl.when(t == 1)
        def _():
            message[...] += out

        return c

    lax.fori_loop(0, n_tiles, tile, 0)

    def tell(k, c):
        t = lax.rem(me + k, n)
        pltpu.make_async_remote_copy(
            src_ref=message, dst_ref=slots.at[me],
            send_sem=msg_send, recv_sem=msg_recv,
            device_id={"virt": t // n_aux, "aux": lax.rem(t, n_aux)},
            device_id_type=MESH,
        ).start()
        return c

    lax.fori_loop(1, n, tell, 0)
    slots[me] = message[...]
    for k in list(range(2, n_aux, 2)) + [1]:
        share_own(k).wait_send()
    for k in range(2, n_aux, 2):
        hand_on(k).wait_send()
    for k in range(n_aux):
        copy, wanted = share_other(k)
        pl.when(wanted)(copy.wait_send)
    everyone = slots.at[pl.ds(0, n - 1)]
    pltpu.make_async_copy(everyone, everyone, msg_send).wait()
    pltpu.make_async_copy(everyone, everyone, msg_recv).wait()

    keep = jnp.logical_or(l8 < free, r8 < 0)

    def add(k, acc):
        sv = k // n_aux
        so = virt_of(lax.rem(label_of(sv, n_virt) + pick(table, lax.rem(k, n_aux)), n_virt), n_virt)
        row0 = jnp.where(sv == v, 1.0, 0.0)
        row1 = jnp.where(so == v, 1.0, 0.0)
        weight = jnp.where(keep, 1.0, jnp.where(r8 == 0, row0, row1))
        return acc + slots[k] * weight

    done = lax.fori_loop(0, n, add, jnp.zeros((8, LANES), F32))
    done_ref[...] = done


TILES = (
    (0, 2, 1),
    (0, 2, 0),
    (0, 1, 0),
    (1, 2, 0),
    (1, 3, 0),
    (0, 3, 0),
    (1, 3, 1),
    (2, 3, 0),
    (0, 4, 0),
    (0, 5, 0),
    (2, 4, 0),
    (2, 5, 0),
    (1, 4, 0),
    (3, 4, 0),
    (1, 5, 0),
    (3, 5, 0),
    (0, 6, 0),
    (0, 7, 0),
    (2, 6, 0),
    (2, 7, 0),
    (1, 6, 0),
    (1, 7, 0),
    (3, 6, 0),
    (3, 7, 0),
    (6, 7, 0),
    (6, 4, 0),
    (7, 4, 0),
    (6, 4, 1),
    (6, 5, 0),
    (7, 5, 0),
    (4, 5, 0),
    (7, 5, 1),
)
ROUTES = (
    ((2, 10, 34), (10, 4), (2,), (16, 10), (3,), (), (), (3,), ()),
    ((4, 18), (0, 16), (), (), (14,), (1,), (1,), (), ()),
    ((), (), (10, 18), (34,), (), (), (), (), ()),
    ((), (), (5,), (5,), (), (14,), (3, 14, 22), (1, 14), (0, 4)),
    ((5, 24, 12), (5, 40, 24), (), (24,), (), (11,), (), (11,), ()),
    ((), (), (0,), (), (9, 13), (), (), (), (8, 12)),
    ((28, 6), (6, 28), (6, 28), (28, 8), (15,), (15,), (15, 11), (15,), ()),
    ((), (), (), (), (), (), (), (), (12, 6)),
    ((), (18, 34), (32,), (2, 18), (21,), (), (25,), (), (1, 36, 22)),
    ((16,), (), (16,), (), (23,), (), (), (), (20, 3)),
    ((), (22, 38, 7), (7, 38), (7,), (), (), (17,), (25,), ()),
    ((20, 7), (), (), (20, 36), (), (), (31, 19), (19,), ()),
    ((42,), (), (8, 42), (), (17, 27), (), (27,), (27,), (11, 26, 44, 30)),
    ((), (30, 9), (), (9,), (), (25,), (), (), ()),
    ((), (), (24,), (42,), (), (23, 31), (), (31,), (13, 30)),
    ((), (44, 13), (26, 44, 9), (26, 46, 13), (29,), (), (), (), ()),
    ((), (), (34,), (), (37, 45), (37, 41), (), (48, 41), (25, 51)),
    ((32,), (32,), (), (32,), (), (39,), (), (), (53, 27, 51, 17)),
    ((38,), (), (), (38,), (), (54, 45), (), (33, 45), (21, 55)),
    ((), (36,), (36,), (), (), (), (), (35,), (53, 21, 55)),
    ((), (42,), (), (), (), (), (), (), (19, 59, 31)),
    ((40,), (), (40,), (40,), (47, 35), (35, 47), (58, 35), (), (59, 29, 57, 19)),
    ((46,), (46,), (46,), (), (), (), (37, 41), (), (23, 61, 29)),
    ((), (), (), (44,), (), (62,), (), (39,), (63, 23, 29)),
    ((50, 56, 54), (56,), (), (), (), (52,), (), (), ()),
    ((33,), (33, 48), (48, 56, 33), (), (55, 60), (), (), (17,), ()),
    ((39,), (), (49,), (), (), (55, 60, 21), (60,), (51, 60), (50, 54)),
    ((), (), (45,), (37, 56), (53,), (), (51, 53), (), ()),
    ((41,), (), (), (50,), (), (), (59,), (), (58, 62, 43)),
    ((49,), (43, 49), (), (43, 49), (57, 63), (61,), (), (57,), ()),
    ((), (), (), (), (), (63,), (63,), (59,), (52, 62, 39, 47)),
    ((52,), (), (43,), (47, 52, 58), (61,), (), (57,), (61,), ()),
)
STEPS = (
    (0, 17, 2, 19, 6, 8, 23, 25, 10, 12, 4, 27, 14, 29, 21, 31),
    (2, 3, 0, 1, 8, 10, 25, 12, 27, 13, 4, 6, 14, 21, 7, 31),
    (4, 5, 6, 7, 8, 12, 9, 14, 10, 29, 11, 2, 31, 19, 0, 17),
    (4, 12, 6, 13, 21, 14, 7, 31, 2, 10, 3, 27, 0, 8, 1, 25),
    (0, 1, 2, 3, 8, 6, 10, 25, 7, 14, 27, 31, 4, 12, 5, 29),
    (0, 8, 4, 1, 25, 5, 2, 3, 10, 6, 12, 14, 7, 29, 27, 31),
    (4, 21, 6, 23, 2, 12, 19, 29, 0, 14, 17, 31, 8, 10, 25, 27),
    (12, 13, 4, 14, 21, 15, 6, 8, 10, 23, 11, 9, 0, 2, 17, 19),
    (2, 3, 4, 12, 5, 6, 8, 29, 7, 10, 9, 27, 14, 0, 31, 17),
    (4, 8, 2, 5, 9, 3, 6, 14, 7, 12, 0, 10, 31, 17, 27, 29),
    (4, 5, 6, 7, 2, 12, 3, 29, 14, 31, 0, 1, 10, 27, 8, 25),
    (6, 7, 12, 2, 14, 0, 3, 31, 1, 13, 4, 8, 21, 25, 10, 27),
    (0, 8, 1, 25, 4, 10, 2, 5, 11, 19, 12, 14, 6, 29, 15, 23),
    (2, 3, 0, 1, 6, 7, 8, 4, 10, 25, 27, 12, 14, 5, 29, 31),
    (4, 5, 6, 10, 7, 11, 2, 14, 0, 31, 8, 1, 12, 25, 19, 29),
    (6, 7, 4, 5, 2, 3, 12, 10, 8, 27, 14, 9, 0, 31, 17, 29),
    (10, 11, 8, 9, 0, 14, 2, 12, 6, 15, 19, 13, 23, 4, 17, 21),
    (0, 2, 10, 6, 3, 27, 7, 8, 1, 14, 12, 31, 4, 13, 21, 25),
    (6, 14, 0, 7, 31, 1, 10, 11, 2, 8, 4, 19, 12, 5, 25, 29),
    (6, 0, 7, 1, 14, 2, 31, 4, 3, 12, 10, 8, 5, 29, 27, 25),
    (2, 10, 3, 27, 8, 0, 1, 6, 12, 4, 14, 25, 7, 13, 21, 31),
    (10, 11, 8, 12, 9, 2, 0, 13, 19, 17, 14, 6, 4, 15, 23, 21),
    (0, 6, 1, 4, 7, 2, 12, 3, 13, 14, 31, 8, 10, 25, 21, 27),
    (6, 14, 7, 31, 0, 1, 4, 10, 2, 11, 12, 19, 8, 13, 21, 25),
    (0, 1, 2, 3, 10, 27, 4, 8, 5, 25, 14, 6, 12, 15, 23, 29),
    (2, 3, 0, 1, 4, 5, 8, 14, 25, 15, 10, 6, 12, 27, 23, 29),
    (14, 4, 10, 15, 5, 11, 6, 12, 0, 2, 29, 1, 23, 8, 19, 25),
    (6, 23, 4, 21, 10, 0, 12, 27, 17, 29, 14, 8, 31, 25, 2, 19),
    (0, 6, 1, 7, 8, 2, 4, 10, 25, 5, 11, 19, 12, 14, 29, 31),
    (2, 3, 0, 1, 10, 8, 27, 6, 25, 7, 14, 4, 12, 5, 31, 29),
    (12, 14, 13, 6, 10, 2, 15, 3, 27, 8, 23, 4, 9, 0, 21, 17),
    (6, 23, 4, 21, 14, 0, 17, 12, 31, 29, 8, 10, 25, 27, 2, 19),
)
PARTNERS = (
    (1, 2, 4, 8, 3, 5, 17),
    (0, 3, 5, 9, 2, 7, 8),
    (3, 0, 6, 10, 1, 4, 5, 9, 17),
    (2, 1, 7, 11, 0, 6, 10),
    (5, 6, 0, 12, 2, 13, 15, 20),
    (4, 7, 1, 13, 0, 2, 6, 12),
    (7, 4, 2, 14, 3, 5, 15),
    (6, 5, 3, 15, 1),
    (9, 10, 12, 0, 16, 1, 11, 17, 18, 25),
    (8, 11, 13, 1, 17, 2, 10, 20, 21),
    (11, 8, 14, 2, 18, 3, 9, 12, 19, 26),
    (10, 9, 15, 3, 19, 8, 14, 18, 22, 23),
    (13, 14, 8, 4, 20, 5, 10, 15, 16, 21, 22),
    (12, 15, 9, 5, 21, 4, 17),
    (15, 12, 10, 6, 22, 11, 21, 23),
    (14, 13, 11, 7, 23, 4, 6, 12, 20, 22),
    (17, 18, 20, 8, 24, 12, 22, 25),
    (16, 19, 21, 9, 25, 0, 2, 8, 13, 26),
    (19, 16, 22, 10, 26, 8, 11, 27),
    (18, 17, 23, 11, 27, 10, 26, 30),
    (21, 22, 16, 12, 28, 4, 9, 15, 29),
    (20, 23, 17, 13, 29, 9, 12, 14, 28, 31),
    (23, 20, 18, 14, 30, 11, 12, 15, 16, 27),
    (22, 21, 19, 15, 31, 11, 14, 30),
    (25, 26, 28, 16, 27, 29),
    (24, 27, 29, 17, 8, 16, 26, 28, 30),
    (27, 24, 30, 18, 10, 17, 19, 25, 31),
    (26, 25, 31, 19, 18, 22, 24, 28),
    (29, 30, 24, 20, 21, 25, 27, 31),
    (28, 31, 25, 21, 20, 24, 30),
    (31, 28, 26, 22, 19, 23, 25, 29),
    (30, 29, 27, 23, 21, 26, 28),
)
NEAR = (4, 4, 4, 4, 4, 4, 4, 4, 5, 5, 5, 5, 5, 5, 5, 5, 5, 5, 5, 5, 5, 5, 5, 5, 4, 4, 4, 4, 4, 4, 4, 4)
NEWS = (
    (8, 8, 12),
    (4, 9, 11),
    (5, 7, 14),
    (2, 8, 12),
    (4, 10, 12),
    (5, 9, 15),
    (8, 12, 15),
    (0, 4, 6),
    (2, 6, 12),
    (2, 6, 7),
    (8, 11, 13),
    (3, 9, 14),
    (3, 5, 11),
    (6, 10, 11),
    (2, 3, 10),
    (6, 6, 12),
    (1, 3, 4),
    (0, 0, 7),
    (4, 7, 10),
    (0, 5, 7),
    (0, 0, 4),
    (1, 2, 12),
    (1, 7, 11),
    (3, 8, 10),
    (5, 7, 10),
    (5, 9, 15),
    (4, 8, 13),
    (4, 10, 11),
    (1, 4, 12),
    (5, 9, 11),
    (0, 5, 9),
    (6, 10, 10),
)
PLANS = {(8, 4): (TILES, ROUTES, STEPS, PARTNERS, NEAR, NEWS)}


KIDS = 4
CODE = 128


def table_kernel(
    n_virt, n_aux, occ, plan,
    x_ref, occ_hbm, virt_hbm,
    done_ref,
    held, lhs, rhs, order, order_t, ints, over, sums, message, slots, occ_ref, virt_ref,
    own_sem, eps_sem, send_sem, recv_sem, msg_send, msg_recv, news_sem,
):
    rows, cols = x_ref.shape
    deep = lhs.shape[2]
    width = cols // occ
    groups = LANES // width
    supers = occ // groups
    n = n_virt * n_aux
    v = lax.axis_index("virt")
    p = lax.axis_index("aux")
    me = v * n_aux + p
    tiles, routes, steps, partners, n_near, news = plan
    rounds = len(news[0]) + 1
    half = -(-rows // 32) * 16
    cuts = ((0, half), (half, rows - half))
    n_slots = 2 * n_aux

    def device(t):
        return {"virt": lax.div(t, n_aux), "aux": lax.rem(t, n_aux)}

    barrier = pltpu.get_barrier_semaphore()

    side_a = pick([t[0] for t in tiles], me)
    side_b = pick([t[1] for t in tiles], me)
    diag = pick([t[2] for t in tiles], me) == 1
    own_slot = jnp.where(side_a == v, p, jnp.where(side_b == v, n_aux + p, n_slots))
    own = pltpu.make_async_copy(x_ref, held.at[own_slot], own_sem)
    own.start()
    eps = (
        pltpu.make_async_copy(occ_hbm, occ_ref, eps_sem.at[0]),
        pltpu.make_async_copy(virt_hbm, virt_ref, eps_sem.at[1]),
    )
    for copy in eps:
        copy.start()

    def packed(codes):
        got = 0
        for c in reversed(codes):
            got = got * CODE + c + 1
        return got

    most = max(len(r) for r in partners)
    folk = [
        pick([packed(r[at:at + KIDS]) for r in partners], me) for at in range(0, most, KIDS)
    ]
    n_folk = pick([len(r) for r in partners], me)
    near = pick(n_near, me)

    def signal(sem, amount, limit):
        code = None
        for k in range(amount):
            code = folk[k // KIDS] if k % KIDS == 0 else lax.div(code, CODE)

            @pl.when(k < limit)
            def _():
                t = lax.rem(code, CODE) - 1
                pl.semaphore_signal(sem, inc=1, device_id=device(t), device_id_type=MESH)

    signal(barrier, most, n_folk)

    kids = [pick([packed(r[s]) for r in routes], me) for s in range(n_slots + 1)]
    spread_at = [pick([r[k] for r in news], me) for k in range(rounds - 1)]
    todo = [pick([r[i] for r in steps], me) for i in range(2 * n_slots)]

    row = lax.broadcasted_iota(jnp.int32, (cols, cols), 0)
    col = lax.broadcasted_iota(jnp.int32, (cols, cols), 1)
    hit = col == lax.rem(row, width) * occ + row // width
    order[...] = jnp.where(hit, 1.0, 0.0).astype(BF16)
    hit = row == lax.rem(col, width) * occ + col // width
    order_t[...] = jnp.where(hit, 1.0, 0.0).astype(BF16)
    own.wait()
    pl.semaphore_wait(barrier, n_folk)

    def piece(slot, part):
        return held.at[slot, pl.ds(cuts[part][0], cuts[part][1])]

    def copies(slot, part, act):
        code = pick(kids, slot)
        q = jnp.where(slot == n_slots, p, lax.rem(slot, n_aux))
        for k in range(KIDS):
            this = lax.rem(code, CODE)
            code = lax.div(code, CODE)

            @pl.when(this > 0)
            def _():
                t = this - 1
                to = lax.rem(t, 2) * n_aux + q
                copy = pltpu.make_async_remote_copy(
                    src_ref=piece(slot, part), dst_ref=piece(to, part),
                    send_sem=send_sem.at[slot, part, k], recv_sem=recv_sem.at[to, part],
                    device_id=device(lax.div(t, 2)), device_id_type=MESH,
                )
                act(copy)

    for part in range(2):
        copies(own_slot, part, lambda copy: copy.start())
    close = max(n_near)
    signal(news_sem.at[0], close, near)
    whole_rows = rows // 16 * 16
    whole_lanes = rows // LANES * LANES
    lhs[:, :, whole_lanes:] = jnp.zeros((n_slots, cols, deep - whole_lanes), BF16)
    rhs[:, whole_rows:, :] = jnp.zeros((n_slots, deep - whole_rows, cols), BF16)
    for copy in eps:
        copy.wait()

    lane = lax.broadcasted_iota(jnp.int32, (1, LANES), 1)
    part = lane // width
    down = lax.broadcasted_iota(jnp.int32, (width, 1), 0)
    lane_in = lax.rem(lane, width)
    n_tiles = jnp.where(diag, 2, 1)

    def eps_down(which):
        got = jnp.zeros((width, 1), F32)
        for k in range(width):
            got = jnp.where(down == k, virt_ref[which * width + k], got)
        return got

    def eps_across(which):
        got = jnp.zeros((1, LANES), F32)
        for k in range(width):
            got = jnp.where(lane_in == k, virt_ref[which * width + k], got)
        return got

    occ_lane = []
    for cj in range(supers):
        got = jnp.zeros((1, LANES), F32)
        for t in range(groups):
            got = jnp.where(part == t, occ_ref[cj * groups + t], got)
        occ_lane.append(got)

    def prepare(t, c):
        block_l = jnp.where(t == 0, side_a, side_b)
        block_r = jnp.where(jnp.logical_and(diag, t == 0), side_a, side_b)
        base = -(eps_down(block_l) + eps_across(block_r))
        ints[t] = jnp.zeros((cols, cols), F32)
        for i in range(occ):
            for cj in range(i // groups, supers):
                below = base + (occ_lane[cj] + occ_ref[i])
                over[t, i * width:(i + 1) * width, cj * LANES:(cj + 1) * LANES] = (
                    (1.0 if cj == i // groups else 2.0) / below
                )
        return c

    lax.fori_loop(0, n_tiles, prepare, 0)

    def take(i, c):
        for r in range(1, rounds):

            @pl.when(i == spread_at[r - 1])
            def _():
                pl.semaphore_wait(news_sem.at[r - 1], near)
                signal(news_sem.at[r], close, near)

        entry = pick(todo, i)
        slot = lax.rem(lax.div(entry, 2), n_slots)
        meets = lax.div(entry, 4 * n_aux) == 1
        later = lax.rem(entry, 2)
        away = slot != own_slot
        for part in range(2):

            @pl.when(jnp.logical_and(later == part, away))
            def _():
                whole = piece(slot, part)
                pltpu.make_async_copy(whole, whole, recv_sem.at[slot, part]).wait()
                copies(slot, part, lambda copy: copy.start())

        side = lax.div(slot, n_aux)
        mine = jnp.where(diag, side, 0)
        left = jnp.where(diag, slot, lax.rem(slot, n_aux))
        right = jnp.where(diag, slot, n_aux + lax.rem(slot, n_aux))

        @pl.when(jnp.logical_and(later == 1, jnp.logical_or(side == 0, diag)))
        def _():
            lhs[slot, :, 0:rows] = lax.dot_general(
                order[...], held[slot], NT, preferred_element_type=F32
            ).astype(BF16)

        @pl.when(jnp.logical_and(later == 1, jnp.logical_or(side == 1, diag)))
        def _():
            rhs[slot, 0:rows, :] = lax.dot_general(
                held[slot], order_t[...], NN, preferred_element_type=F32
            ).astype(BF16)

        @pl.when(meets)
        def _():
            ints[mine] += lax.dot_general(lhs[left], rhs[right], NN, preferred_element_type=F32)

        return c

    lax.fori_loop(0, 2 * n_slots, take, 0)

    tall = -(-occ // 4)
    sums[...] = jnp.zeros_like(sums)
    r8 = lax.broadcasted_iota(jnp.int32, (8, LANES), 0)
    l8 = lax.broadcasted_iota(jnp.int32, (8, LANES), 1)
    wide = lax.broadcasted_iota(jnp.int32, (cols, LANES), 0)
    thin = lax.broadcasted_iota(jnp.int32, (cols, LANES), 1)
    fold = jnp.where(wide // width == thin, 1.0, 0.0).astype(BF16)
    ri = lax.broadcasted_iota(jnp.int32, (tall * 8, occ * 8), 0)
    rj = lax.broadcasted_iota(jnp.int32, (tall * 8, occ * 8), 1)
    gather = jnp.logical_and(lax.rem(ri, 8) < 4, rj // 8 == ri // 8 * 4 + lax.rem(ri, 8))
    gather = jnp.where(gather, 1.0, 0.0).astype(BF16)
    ones = jnp.ones((8, LANES), BF16)
    free = tall * occ

    def split(x):
        high = x.astype(BF16)
        return high, (x - high.astype(F32)).astype(BF16)

    def tile(t, c):
        total = jnp.zeros((width, LANES), F32)
        for ci in range(supers):
            for cj in range(ci, supers):
                turned = []
                for g in range(groups):
                    block = ints[t, pl.ds((cj * groups + g) * width, width), pl.ds(ci * LANES, LANES)]
                    turned.append([block if r == 0 else pltpu.roll(block, r * width, 1) for r in range(groups)])
                for s in range(groups):
                    i = ci * groups + s
                    direct = ints[t, pl.ds(i * width, width), pl.ds(cj * LANES, LANES)]
                    inverse = over[t, pl.ds(i * width, width), pl.ds(cj * LANES, LANES)]
                    swapped = turned[0][(0 - s) % groups]
                    for g in range(1, groups):
                        swapped = jnp.where(part == g, turned[g][(g - s) % groups], swapped)
                    if ci == cj:
                        term = direct * (2.0 * direct - swapped) * inverse
                    else:
                        term = (direct * (direct - swapped) + swapped * swapped) * inverse
                    total = total + term
                    short = term[0:8]
                    for m in range(8, width, 8):
                        short = short + term[m:m + 8]
                    sums[i * 8:i * 8 + 8, cj * LANES:(cj + 1) * LANES] = short

        rows_of = [
            lax.dot_general(gather, x, NN, preferred_element_type=F32) for x in split(sums[...])
        ]
        pairs_of = [
            lax.dot_general(x, fold, NN, preferred_element_type=F32)
            for x in split(rows_of[0] + rows_of[1])
        ]
        by_ij = pairs_of[0] + pairs_of[1]
        packed_ij = by_ij[0:8]
        for g in range(1, tall):
            packed_ij = packed_ij + pltpu.roll(by_ij[g * 8:g * 8 + 8], g * occ, 1)
        spread = jnp.concatenate([jnp.zeros((LANES - width, LANES), F32), total], 0)
        by_row = [
            lax.dot_general(ones, x, NT, preferred_element_type=F32) for x in split(spread)
        ]
        by_row = by_row[0] + by_row[1]
        by_col = [
            lax.dot_general(ones[:, :width], x, NN, preferred_element_type=F32) for x in split(total)
        ]
        by_col = by_col[0] + by_col[1]
        folded = by_col
        for g in range(1, groups):
            folded = folded + pltpu.roll(by_col, g * width, 1)
        packed_ij = packed_ij * jnp.where(diag, 0.5, 1.0)
        both = (by_row + folded) * 0.5
        first = jnp.where(diag, jnp.where(t == 0, both, 0.0), by_row)
        second = jnp.where(diag, jnp.where(t == 1, both, 0.0), folded)
        near_turn = free - (LANES - width)
        far_turn = near_turn - width // 2
        shares = jnp.where(r8 == 3, pltpu.roll(second, far_turn % LANES, 1), 0.0)
        shares = jnp.where(r8 == 2, pltpu.roll(second, near_turn % LANES, 1), shares)
        shares = jnp.where(r8 == 1, pltpu.roll(first, far_turn % LANES, 1), shares)
        shares = jnp.where(r8 == 0, pltpu.roll(first, near_turn % LANES, 1), shares)
        shares = jnp.where(l8 < free + width // 2, shares, 0.0)
        out = jnp.where(l8 < free, packed_ij, shares)[0:4]

        @pl.when(t == 0)
        def _():
            message[...] = out

        @pl.when(t == 1)
        def _():
            message[...] += out

        return c

    lax.fori_loop(0, n_tiles, tile, 0)
    pl.semaphore_wait(news_sem.at[rounds - 1], near)

    def tell(k, c):
        t = me + k
        t = jnp.where(t >= n, t - n, t)
        pltpu.make_async_remote_copy(
            src_ref=message, dst_ref=slots.at[me],
            send_sem=msg_send, recv_sem=msg_recv,
            device_id=device(t), device_id_type=MESH,
        ).start()
        return c

    lax.fori_loop(1, n, tell, 0)
    slots[me] = message[...]
    for part_at in range(2):
        copies(own_slot, part_at, lambda copy: copy.wait_send())

    def flush(s, c):
        @pl.when(s != own_slot)
        def _():
            for part_at in range(2):
                copies(s, part_at, lambda copy: copy.wait_send())

        return c

    lax.fori_loop(0, n_slots, flush, 0)
    everyone = slots.at[pl.ds(0, n - 1)]
    pltpu.make_async_copy(everyone, everyone, msg_send).wait()
    pltpu.make_async_copy(everyone, everyone, msg_recv).wait()

    keep = l8[0:4] < free
    upper = r8[0:4] < 2
    acc = None
    for k in range(n):
        a, b, _ = tiles[k]
        row0 = jnp.where(v == a, 1.0, 0.0)
        row1 = jnp.where(v == b, 1.0, 0.0)
        term = slots[k] * jnp.where(keep, 1.0, jnp.where(upper, row0, row1))
        acc = term if acc is None else acc + term
    done_ref[...] = acc


def table_unpack(occ, width, done_ref, share_ref, pair_ref):
    tall = -(-occ // 4)
    free = tall * occ
    done = done_ref[...]
    share = done[0:2] + done[2:4]
    share_ref[...] = jnp.concatenate(
        [share[0, free:free + width // 2], share[1, free:free + width // 2]], 0
    )
    blocks = [done] + [pltpu.roll(done, LANES - g * occ, 1) for g in range(1, tall)]
    square = jnp.concatenate(blocks + [jnp.zeros((LANES - 4 * tall, LANES), F32)], 0)
    square = jnp.where(lax.broadcasted_iota(jnp.int32, (LANES, LANES), 1) < occ, square, 0.0)
    pair = square + square.T
    pair_ref[...] = pair[0:occ, 0:occ]


def table_call(n_virt, n_aux, occ, plan, three_index, eps_occ, eps_virt):
    rows, cols = three_index.shape
    width = cols // occ
    deep = -(-rows // LANES) * LANES
    n = n_virt * n_aux
    n_slots = 2 * n_aux
    vmem = pl.BlockSpec(memory_space=pltpu.VMEM)
    hbm = pl.BlockSpec(memory_space=pltpu.HBM)
    done = pl.pallas_call(
        functools.partial(table_kernel, n_virt, n_aux, occ, plan),
        out_shape=pltpu.VMEM((4, LANES), F32),
        in_specs=[hbm, hbm, hbm],
        out_specs=vmem,
        scratch_shapes=[
            pltpu.VMEM((n_slots + 1, rows, cols), BF16),
            pltpu.VMEM((n_slots, cols, deep), BF16),
            pltpu.VMEM((n_slots, deep, cols), BF16),
            pltpu.VMEM((cols, cols), BF16),
            pltpu.VMEM((cols, cols), BF16),
            pltpu.VMEM((2, cols, cols), F32),
            pltpu.VMEM((2, cols, cols), F32),
            pltpu.VMEM((occ * 8, cols), F32),
            pltpu.VMEM((4, LANES), F32),
            pltpu.VMEM((n, 4, LANES), F32),
            pltpu.SMEM(eps_occ.shape, F32),
            pltpu.SMEM(eps_virt.shape, F32),
            pltpu.SemaphoreType.DMA,
            pltpu.SemaphoreType.DMA((2,)),
            pltpu.SemaphoreType.DMA((n_slots + 1, 2, KIDS)),
            pltpu.SemaphoreType.DMA((n_slots, 2)),
            pltpu.SemaphoreType.DMA,
            pltpu.SemaphoreType.DMA,
            pltpu.SemaphoreType.REGULAR((len(plan[5][0]) + 1,)),
        ],
        compiler_params=pltpu.CompilerParams(collective_id=0, has_side_effects=True),
    )(three_index, eps_occ, eps_virt)
    return pl.pallas_call(
        functools.partial(table_unpack, occ, width),
        out_shape=(
            jax.ShapeDtypeStruct((width,), F32),
            jax.ShapeDtypeStruct((occ, occ), F32),
        ),
        in_specs=[vmem],
        out_specs=(vmem, vmem),
    )(pltpu.with_memory_space_constraint(done, pltpu.VMEM))


def unpack(occ, width, done_ref, share_ref, pair_ref):
    tall = -(-occ // 8)
    free = tall * width
    done = done_ref[...]
    share = done[0:1] + done[1:2]
    share_ref[...] = share[0, free:free + width]
    blocks = [done] + [pltpu.roll(done, LANES - g * width, 1) for g in range(1, tall)]
    square = jnp.concatenate(blocks + [jnp.zeros((LANES - 8 * tall, LANES), F32)], 0)
    square = jnp.where(lax.broadcasted_iota(jnp.int32, (LANES, LANES), 1) < occ, square, 0.0)
    pair = square + square.T
    pair_ref[...] = pair[0:occ, 0:occ]


def on_device(n_virt, n_aux, three_index, eps_occ, eps_virt):
    occ = eps_occ.shape[0]
    rows, cols = three_index.shape
    width = cols // occ
    pitch = -(-rows // 16) * 16
    n = n_virt * n_aux
    vmem = pl.BlockSpec(memory_space=pltpu.VMEM)
    smem = pl.BlockSpec(memory_space=pltpu.SMEM)
    plan = PLANS.get((n_virt, n_aux))
    if plan is not None:
        return table_call(n_virt, n_aux, occ, plan, three_index, eps_occ, eps_virt)
    done = pl.pallas_call(
        functools.partial(kernel, n_virt, n_aux, occ),
        out_shape=jax.ShapeDtypeStruct((8, LANES), F32),
        in_specs=[vmem, smem, smem],
        out_specs=vmem,
        scratch_shapes=[
            pltpu.VMEM((2, n_aux, rows, cols), BF16),
            pltpu.VMEM((cols, n_aux * pitch), BF16),
            pltpu.VMEM((n_aux * pitch, cols), BF16),
            pltpu.VMEM((cols, cols), BF16),
            pltpu.VMEM((cols, cols), BF16),
            pltpu.VMEM((cols, cols), F32),
            pltpu.VMEM((occ * 8, cols), F32),
            pltpu.VMEM((8, LANES), F32),
            pltpu.VMEM((8, LANES), F32),
            pltpu.VMEM((n, 8, LANES), F32),
            pltpu.SemaphoreType.DMA,
            pltpu.SemaphoreType.DMA((3, n_aux)),
            pltpu.SemaphoreType.DMA((2, n_aux)),
            pltpu.SemaphoreType.DMA,
            pltpu.SemaphoreType.DMA,
        ],
        compiler_params=pltpu.CompilerParams(collective_id=0, has_side_effects=True),
    )(three_index, eps_occ, eps_virt)
    return pl.pallas_call(
        functools.partial(unpack, occ, width),
        out_shape=(
            jax.ShapeDtypeStruct((width,), F32),
            jax.ShapeDtypeStruct((occ, occ), F32),
        ),
        in_specs=[vmem],
        out_specs=(vmem, vmem),
    )(done)


def solution(mesh):
    n_virt, n_aux = mesh.shape["virt"], mesh.shape["aux"]
    assert n_virt == 2 * n_aux and n_aux % 2 == 0
    in_specs = (P("aux", "virt"), P(), P())
    out_specs = (P("virt"), P())
    return jax.shard_map(
        functools.partial(on_device, n_virt, n_aux), mesh=mesh,
        in_specs=in_specs, out_specs=out_specs, check_vma=False,
    )
```

```python
import functools

import jax
import jax.numpy as jnp
from jax import lax
from jax.experimental import pallas as pl
from jax.experimental.pallas import tpu as pltpu
from jax.sharding import PartitionSpec as P

MESH = pl.DeviceIdType.MESH
F32 = jnp.float32
BF16 = jnp.bfloat16
EXACT = lax.Precision.HIGHEST
LANES = 128
NT = (((1,), (1,)), ((), ()))
NN = (((1,), (0,)), ((), ()))


def distances(n_aux):
    return list(range(1, n_aux + 1, 2)) + list(range(2, n_aux + 1, 2))


def pick(table, at):
    got = table[0] + jnp.int32(0)
    for k in range(1, len(table)):
        got = jnp.where(at == k, table[k] + jnp.int32(0), got)
    return got


def label_of(virt, n_virt):
    return lax.rem(virt, 2) * (n_virt // 2) + virt // 2


def virt_of(label, n_virt):
    half = n_virt // 2
    return lax.rem(label, half) * 2 + label // half


def kernel(
    n_virt, n_aux, occ,
    x_ref, occ_ref, virt_ref,
    done_ref,
    held, lhs, rhs, order, order_t, ints, sums, parts, message, slots,
    own_sem, send_sem, recv_sem, msg_send, msg_recv,
):
    rows, cols = x_ref.shape
    pitch = -(-rows // 16) * 16
    width = cols // occ
    groups = LANES // width
    supers = occ // groups
    n = n_virt * n_aux
    v = lax.axis_index("virt")
    p = lax.axis_index("aux")
    me = v * n_aux + p
    table = distances(n_aux)
    label = label_of(v, n_virt)
    other = virt_of(lax.rem(label + pick(table, p), n_virt), n_virt)
    lower = label < n_virt // 2
    solo = jnp.logical_and(p == n_aux - 1, jnp.logical_not(lower))
    extra = jnp.logical_and(p == n_aux // 2 - 1, lower)

    barrier = pltpu.get_barrier_semaphore()

    def greet(k, c):
        t = lax.rem(me + k, n)
        pl.semaphore_signal(
            barrier, inc=1,
            device_id={"virt": t // n_aux, "aux": lax.rem(t, n_aux)},
            device_id_type=MESH,
        )
        return c

    lax.fori_loop(1, n, greet, 0)
    own = pltpu.make_async_copy(x_ref, held.at[0, p], own_sem)
    own.start()
    pl.semaphore_wait(barrier, n - 1)

    pairs = n_aux // 2

    def place(k):
        return lax.rem(p // 2 + k // 2, pairs) * 2 + lax.rem(p + k, 2)

    def share_own(k):
        return pltpu.make_async_remote_copy(
            src_ref=x_ref, dst_ref=held.at[0, p],
            send_sem=send_sem.at[0, k], recv_sem=recv_sem.at[0, p],
            device_id={"virt": v, "aux": place(k)}, device_id_type=MESH,
        )

    def hand_on(k):
        q = place(k)
        return pltpu.make_async_remote_copy(
            src_ref=held.at[0, q], dst_ref=held.at[0, q],
            send_sem=send_sem.at[2, k], recv_sem=recv_sem.at[0, q],
            device_id={"virt": v, "aux": place(1)}, device_id_type=MESH,
        )

    def share_other(k):
        q = place(k)
        target = lax.rem(label + n_virt - pick(table, q), n_virt)
        copy = pltpu.make_async_remote_copy(
            src_ref=x_ref, dst_ref=held.at[1, p],
            send_sem=send_sem.at[1, k], recv_sem=recv_sem.at[1, p],
            device_id={"virt": virt_of(target, n_virt), "aux": q}, device_id_type=MESH,
        )
        wanted = jnp.logical_or(q < n_aux - 1, target < n_virt // 2)
        return copy, wanted

    for k in list(range(2, n_aux, 2)) + [1]:
        share_own(k).start()
    for k in range(n_aux):
        copy, wanted = share_other(k)
        pl.when(wanted)(copy.start)

    def arrived(side, q):
        pltpu.make_async_copy(
            held.at[side, q], held.at[side, q], recv_sem.at[side, q]
        ).wait()

    row = lax.broadcasted_iota(jnp.int32, (cols, cols), 0)
    col = lax.broadcasted_iota(jnp.int32, (cols, cols), 1)
    hit = col == lax.rem(row, width) * occ + row // width
    order[...] = jnp.where(hit, 1.0, 0.0).astype(BF16)
    hit = row == lax.rem(col, width) * occ + col // width
    order_t[...] = jnp.where(hit, 1.0, 0.0).astype(BF16)
    lhs[...] = jnp.zeros_like(lhs)
    rhs[...] = jnp.zeros_like(rhs)

    def turn(k):
        lhs[:, k * pitch:k * pitch + rows] = lax.dot_general(
            order[...], held[0, place(k)], NT, preferred_element_type=F32
        ).astype(BF16)

    own.wait()
    turn(0)
    for k in range(2, n_aux, 2):
        arrived(0, place(k))
        hand_on(k).start()
        turn(k)
    for k in range(1, n_aux, 2):
        arrived(0, place(k))
        turn(k)

    lane = lax.broadcasted_iota(jnp.int32, (1, LANES), 1)
    part = lane // width
    down = lax.broadcasted_iota(jnp.int32, (width, 1), 0)
    lane_in = lax.rem(lane, width)

    def eps_down(which):
        got = jnp.zeros((width, 1), F32)
        for k in range(width):
            got = jnp.where(down == k, virt_ref[which * width + k], got)
        return got

    def eps_across(which):
        got = jnp.zeros((1, LANES), F32)
        for k in range(width):
            got = jnp.where(lane_in == k, virt_ref[which * width + k], got)
        return got

    occ_lane = []
    for cj in range(supers):
        got = jnp.zeros((1, LANES), F32)
        for t in range(groups):
            got = jnp.where(part == t, occ_ref[cj * groups + t], got)
        occ_lane.append(got)

    tall = -(-occ // 8)
    sums[...] = jnp.zeros_like(sums)
    n_tiles = jnp.where(extra, 2, 1)
    r8 = lax.broadcasted_iota(jnp.int32, (8, LANES), 0)
    l8 = lax.broadcasted_iota(jnp.int32, (8, LANES), 1)
    free = tall * width

    def tile(t, c):
        diag = jnp.logical_or(solo, jnp.logical_and(extra, t == 0))
        source = jnp.where(diag, 0, 1)

        for k in range(n_aux):

            @pl.when(source == 1)
            def _():
                arrived(1, place(k))

            rhs[k * pitch:k * pitch + rows, :] = lax.dot_general(
                held[source, place(k)], order_t[...], NN, preferred_element_type=F32
            ).astype(BF16)
        ints[...] = lax.dot_general(lhs[...], rhs[...], NN, preferred_element_type=F32)

        base = -(eps_down(v) + eps_across(jnp.where(diag, v, other)))
        total = jnp.zeros((width, LANES), F32)
        for ci in range(supers):
            for cj in range(ci, supers):
                turned = []
                for g in range(groups):
                    block = ints[pl.ds((cj * groups + g) * width, width), pl.ds(ci * LANES, LANES)]
                    turned.append([block if r == 0 else pltpu.roll(block, r * width, 1) for r in range(groups)])
                for s in range(groups):
                    i = ci * groups + s
                    direct = ints[pl.ds(i * width, width), pl.ds(cj * LANES, LANES)]
                    swapped = turned[0][(0 - s) % groups]
                    for g in range(1, groups):
                        swapped = jnp.where(part == g, turned[g][(g - s) % groups], swapped)
                    below = base + (occ_lane[cj] + occ_ref[i])
                    if ci == cj:
                        term = direct * (2.0 * direct - swapped) / below
                    else:
                        term = 2.0 * (direct * (direct - swapped) + swapped * swapped) / below
                    total = total + term
                    short = term[0:8]
                    for m in range(8, width, 8):
                        short = short + term[m:m + 8]
                    sums[i * 8:i * 8 + 8, cj * LANES:(cj + 1) * LANES] = short

        wide = lax.broadcasted_iota(jnp.int32, (cols, LANES), 0)
        thin = lax.broadcasted_iota(jnp.int32, (cols, LANES), 1)
        fold = jnp.where(wide // width == thin, 1.0, 0.0)
        by_j = lax.dot_general(sums[...], fold, NN, precision=EXACT, preferred_element_type=F32)
        ri = lax.broadcasted_iota(jnp.int32, (tall * 8, occ * 8), 0)
        rj = lax.broadcasted_iota(jnp.int32, (tall * 8, occ * 8), 1)
        by_ij = lax.dot_general(
            jnp.where(rj // 8 == ri, 1.0, 0.0), by_j, NN,
            precision=EXACT, preferred_element_type=F32,
        )
        packed = by_ij[0:8]
        for g in range(1, tall):
            packed = packed + pltpu.roll(by_ij[g * 8:g * 8 + 8], g * width, 1)
        pads = [jnp.zeros((free, LANES), F32), total]
        if free + width < LANES:
            pads.append(jnp.zeros((LANES - free - width, LANES), F32))
        spread = jnp.concatenate(pads, 0)
        by_row = lax.dot_general(
            jnp.ones((8, LANES), F32), spread, NT, precision=EXACT, preferred_element_type=F32)
        by_col = lax.dot_general(
            jnp.ones((8, width), F32), total, NN, precision=EXACT, preferred_element_type=F32)
        folded = by_col
        for g in range(1, groups):
            folded = folded + pltpu.roll(by_col, g * width, 1)
        packed = packed * jnp.where(diag, 0.5, 1.0)
        first = jnp.where(diag, (by_row + folded) * 0.5, by_row)
        second = jnp.where(diag, 0.0, folded)
        out = jnp.where(l8 < free, packed, jnp.where(r8 == 0, first, jnp.where(r8 == 1, second, 0.0)))

        @pl.when(t == 0)
        def _():
            message[...] = out

        @pl.when(t == 1)
        def _():
            message[...] += out

        return c

    lax.fori_loop(0, n_tiles, tile, 0)

    def tell(k, c):
        t = lax.rem(me + k, n)
        pltpu.make_async_remote_copy(
            src_ref=message, dst_ref=slots.at[me],
            send_sem=msg_send, recv_sem=msg_recv,
            device_id={"virt": t // n_aux, "aux": lax.rem(t, n_aux)},
            device_id_type=MESH,
        ).start()
        return c

    lax.fori_loop(1, n, tell, 0)
    slots[me] = message[...]
    for k in list(range(2, n_aux, 2)) + [1]:
        share_own(k).wait_send()
    for k in range(2, n_aux, 2):
        hand_on(k).wait_send()
    for k in range(n_aux):
        copy, wanted = share_other(k)
        pl.when(wanted)(copy.wait_send)
    everyone = slots.at[pl.ds(0, n - 1)]
    pltpu.make_async_copy(everyone, everyone, msg_send).wait()
    pltpu.make_async_copy(everyone, everyone, msg_recv).wait()

    keep = jnp.logical_or(l8 < free, r8 < 0)

    def add(k, acc):
        sv = k // n_aux
        so = virt_of(lax.rem(label_of(sv, n_virt) + pick(table, lax.rem(k, n_aux)), n_virt), n_virt)
        row0 = jnp.where(sv == v, 1.0, 0.0)
        row1 = jnp.where(so == v, 1.0, 0.0)
        weight = jnp.where(keep, 1.0, jnp.where(r8 == 0, row0, row1))
        return acc + slots[k] * weight

    done = lax.fori_loop(0, n, add, jnp.zeros((8, LANES), F32))
    done_ref[...] = done


TILES = (
    (1, 2, 0),
    (0, 1, 0),
    (0, 2, 0),
    (0, 2, 1),
    (2, 3, 0),
    (1, 3, 0),
    (1, 3, 1),
    (0, 3, 0),
    (0, 4, 0),
    (0, 5, 0),
    (2, 4, 0),
    (2, 5, 0),
    (1, 4, 0),
    (1, 5, 0),
    (3, 4, 0),
    (3, 5, 0),
    (0, 6, 0),
    (0, 7, 0),
    (2, 6, 0),
    (2, 7, 0),
    (1, 6, 0),
    (1, 7, 0),
    (3, 6, 0),
    (3, 7, 0),
    (6, 4, 0),
    (6, 7, 0),
    (7, 4, 0),
    (6, 4, 1),
    (6, 5, 0),
    (7, 5, 1),
    (4, 5, 0),
    (7, 5, 0),
)
ROUTES = (
    ((3,), (), (3,), (3,), (8,), (), (8,), (), (2, 14)),
    ((6, 32), (4, 18), (18,), (), (), (0,), (), (), ()),
    ((), (6, 14), (6, 14, 32), (), (), (), (), (7,), ()),
    ((4,), (), (2,), (4, 14, 18), (5,), (5,), (5, 1), (1, 8), ()),
    ((), (1,), (), (), (11,), (), (), (11,), (0, 10, 24)),
    ((12,), (3, 12, 42), (), (0, 24), (13,), (9,), (9,), (), ()),
    ((), (), (0, 24), (40,), (), (15,), (15, 11), (9, 15), ()),
    ((), (), (), (), (), (), (), (), (10, 12)),
    ((), (), (), (), (21, 25), (25,), (), (25,), (1, 22)),
    ((), (16, 34), (16,), (16, 34, 2), (23,), (), (), (), (8, 38, 7)),
    ((7,), (22,), (7, 22), (5,), (), (29,), (17,), (17, 29), ()),
    ((20, 36), (), (36,), (20, 38), (), (), (19,), (), ()),
    ((26, 42), (), (26, 10), (26,), (29,), (), (), (), (9, 30, 46)),
    ((), (), (42,), (), (19, 31), (19, 31), (), (19,), (11, 30)),
    ((), (44,), (30, 44), (44,), (), (), (25,), (), ()),
    ((28, 15), (28, 13), (13,), (13, 28), (), (23,), (23, 27), (23, 27), ()),
    ((16, 34, 18), (), (34,), (), (37, 41), (37, 41), (), (), (17, 49)),
    ((), (32,), (), (32,), (39,), (51,), (), (), (17, 53, 21)),
    ((38,), (20,), (38,), (), (), (45,), (), (45,), (21, 55, 29)),
    ((), (36,), (), (36,), (), (), (), (), (21, 53, 55)),
    ((), (), (), (42,), (45,), (), (), (), (27, 59)),
    ((40,), (24, 40, 26), (40,), (), (35, 47), (35, 47), (), (35,), (27, 59, 57)),
    ((), (46,), (46,), (46,), (), (), (41,), (41,), (31, 63)),
    ((44,), (), (), (), (62,), (39,), (39,), (39,), (31, 57, 63)),
    ((50,), (), (33, 50), (), (55, 60), (), (), (), ()),
    ((33, 56, 54), (33, 48, 54, 56), (56,), (48, 33, 56), (52,), (), (), (), ()),
    ((), (), (35,), (), (), (49, 55, 60), (), (60,), (45, 54)),
    ((), (), (48, 37), (37, 50), (53,), (), (53, 60, 49), (49,), ()),
    ((), (), (), (), (), (), (), (59,), (58,)),
    ((51, 43), (43, 62), (43, 51), (51, 43), (57, 61), (63,), (57,), (), ()),
    ((), (), (), (), (63,), (), (), (), (52, 62)),
    ((), (52,), (47, 58), (47, 52, 58), (), (61,), (61, 59), (61,), ()),
)
STEPS = (
    (4, 0, 8, 2, 5, 1, 25, 3, 12, 6, 29, 10, 7, 14, 31, 27),
    (2, 3, 0, 1, 10, 4, 12, 8, 5, 27, 29, 25, 14, 6, 15, 23),
    (4, 5, 6, 7, 2, 12, 3, 29, 14, 31, 0, 10, 1, 8, 25, 27),
    (6, 23, 4, 21, 12, 2, 29, 19, 0, 14, 10, 17, 8, 31, 25, 27),
    (8, 2, 10, 14, 9, 11, 15, 0, 19, 12, 17, 13, 6, 4, 23, 21),
    (2, 3, 0, 1, 6, 7, 10, 8, 27, 4, 14, 25, 12, 5, 31, 29),
    (4, 21, 6, 23, 14, 2, 31, 12, 19, 29, 0, 10, 17, 8, 27, 25),
    (6, 14, 4, 0, 15, 23, 12, 5, 1, 29, 2, 8, 3, 10, 25, 27),
    (2, 10, 8, 3, 6, 9, 27, 14, 7, 12, 4, 31, 0, 5, 29, 17),
    (2, 3, 6, 10, 7, 8, 4, 27, 5, 9, 0, 14, 12, 31, 17, 29),
    (4, 5, 6, 7, 0, 14, 12, 1, 31, 10, 29, 8, 11, 25, 2, 19),
    (6, 7, 4, 5, 0, 1, 14, 12, 31, 29, 8, 10, 2, 3, 27, 25),
    (4, 0, 5, 1, 6, 10, 2, 7, 8, 25, 3, 27, 12, 14, 29, 31),
    (10, 8, 4, 0, 11, 5, 9, 14, 17, 12, 6, 2, 15, 23, 19, 29),
    (4, 5, 6, 7, 2, 0, 12, 14, 3, 1, 29, 31, 10, 8, 27, 25),
    (6, 7, 4, 5, 2, 14, 0, 12, 3, 31, 1, 29, 10, 8, 27, 25),
    (10, 11, 8, 4, 0, 9, 14, 2, 5, 17, 19, 15, 12, 6, 29, 23),
    (10, 2, 4, 11, 0, 8, 19, 5, 9, 6, 12, 17, 14, 7, 31, 29),
    (14, 2, 6, 3, 15, 10, 23, 4, 27, 5, 12, 8, 0, 9, 17, 29),
    (2, 6, 3, 14, 7, 31, 12, 4, 13, 21, 10, 0, 8, 27, 1, 25),
    (2, 10, 11, 6, 19, 8, 0, 12, 4, 9, 7, 13, 21, 14, 17, 31),
    (10, 11, 2, 8, 9, 19, 14, 0, 4, 15, 6, 12, 5, 17, 29, 23),
    (4, 5, 12, 0, 6, 29, 14, 1, 7, 2, 31, 3, 10, 27, 8, 25),
    (14, 15, 4, 0, 12, 5, 29, 10, 1, 6, 11, 8, 23, 25, 2, 19),
    (0, 1, 2, 3, 6, 8, 7, 4, 25, 5, 12, 10, 14, 27, 29, 31),
    (2, 3, 0, 1, 6, 8, 7, 25, 4, 14, 31, 5, 10, 27, 12, 29),
    (14, 6, 4, 10, 12, 7, 5, 11, 29, 31, 2, 19, 8, 0, 9, 17),
    (6, 23, 4, 21, 12, 2, 10, 14, 29, 19, 31, 8, 0, 27, 17, 25),
    (2, 3, 14, 8, 0, 10, 1, 25, 27, 6, 15, 12, 23, 4, 13, 21),
    (2, 19, 0, 17, 10, 6, 8, 23, 14, 25, 4, 27, 21, 12, 31, 29),
    (12, 14, 13, 4, 6, 10, 0, 8, 15, 21, 2, 9, 17, 3, 23, 27),
    (6, 7, 4, 5, 2, 12, 3, 14, 29, 10, 31, 8, 0, 27, 9, 17),
)
PARTNERS = (
    (1, 2, 4, 8, 3, 5, 6, 7),
    (0, 3, 5, 9, 2, 16),
    (3, 0, 6, 10, 1, 7, 16),
    (2, 1, 7, 11, 0, 4, 9, 10),
    (5, 6, 0, 12, 3, 9),
    (4, 7, 1, 13, 0, 6, 12, 21),
    (7, 4, 2, 14, 0, 5, 12, 15, 20),
    (6, 5, 3, 15, 0, 2),
    (9, 10, 12, 0, 16, 11, 17),
    (8, 11, 13, 1, 17, 3, 4, 16, 19),
    (11, 8, 14, 2, 18, 3, 17, 19),
    (10, 9, 15, 3, 19, 8, 18),
    (13, 14, 8, 4, 20, 5, 6, 15, 21, 23),
    (12, 15, 9, 5, 21, 20),
    (15, 12, 10, 6, 22, 18),
    (14, 13, 11, 7, 23, 6, 12, 22),
    (17, 18, 20, 8, 24, 1, 2, 9, 25),
    (16, 19, 21, 9, 25, 8, 10, 26),
    (19, 16, 22, 10, 26, 11, 14, 27),
    (18, 17, 23, 11, 27, 9, 10, 26),
    (21, 22, 16, 12, 28, 6, 13, 29),
    (20, 23, 17, 13, 29, 5, 12, 28),
    (23, 20, 18, 14, 30, 15, 26, 31),
    (22, 21, 19, 15, 31, 12, 28),
    (25, 26, 28, 16, 27, 30),
    (24, 27, 29, 17, 16, 26, 28),
    (27, 24, 30, 18, 17, 19, 22, 25, 31),
    (26, 25, 31, 19, 18, 24, 30),
    (29, 30, 24, 20, 21, 23, 25),
    (28, 31, 25, 21, 20, 30),
    (31, 28, 26, 22, 24, 27, 29),
    (30, 29, 27, 23, 22, 26),
)
NEAR = (4, 4, 4, 4, 4, 4, 4, 4, 5, 5, 5, 5, 5, 5, 5, 5, 5, 5, 5, 5, 5, 5, 5, 5, 4, 4, 4, 4, 4, 4, 4, 4)
NEWS = (
    (3, 8, 14),
    (5, 10, 13),
    (7, 11, 14),
    (7, 12, 15),
    (1, 6, 10),
    (7, 9, 15),
    (7, 10, 15),
    (3, 9, 14),
    (3, 6, 13),
    (2, 5, 9),
    (7, 10, 14),
    (6, 7, 9),
    (2, 4, 10),
    (2, 8, 14),
    (4, 6, 12),
    (8, 13, 15),
    (2, 6, 12),
    (0, 4, 12),
    (1, 7, 14),
    (2, 6, 10),
    (0, 2, 10),
    (2, 6, 11),
    (2, 5, 11),
    (3, 9, 14),
    (6, 10, 12),
    (7, 10, 13),
    (2, 8, 12),
    (6, 10, 14),
    (2, 7, 11),
    (7, 12, 14),
    (0, 2, 8),
    (7, 9, 11),
)
PLANS = {(8, 4): (TILES, ROUTES, STEPS, PARTNERS, NEAR, NEWS)}


TN = (((0,), (0,)), ((), ()))
KIDS = 4
CODE = 128


def table_kernel(
    n_virt, n_aux, occ, plan,
    x_ref, occ_hbm, virt_hbm,
    done_ref,
    raw, held, order, ints, over, sums, message, slots, occ_ref, virt_ref,
    own_sem, eps_sem, send_sem, recv_sem, msg_send, msg_recv, news_sem,
):
    rows, cols = x_ref.shape
    deep = held.shape[1]
    width = cols // occ
    groups = LANES // width
    supers = occ // groups
    n = n_virt * n_aux
    v = lax.axis_index("virt")
    p = lax.axis_index("aux")
    me = v * n_aux + p
    tiles, routes, steps, partners, n_near, news = plan
    rounds = len(news[0]) + 1
    half = -(-rows // 32) * 16
    cuts = ((0, half), (half, -(-rows // 8) * 8 - half))
    n_slots = 2 * n_aux

    def device(t):
        return {"virt": lax.div(t, n_aux), "aux": lax.rem(t, n_aux)}

    barrier = pltpu.get_barrier_semaphore()

    side_a = pick([t[0] for t in tiles], me)
    side_b = pick([t[1] for t in tiles], me)
    diag = pick([t[2] for t in tiles], me) == 1
    own_slot = jnp.where(side_a == v, p, jnp.where(side_b == v, n_aux + p, n_slots))
    own = pltpu.make_async_copy(x_ref, raw, own_sem)
    own.start()
    eps = (
        pltpu.make_async_copy(occ_hbm, occ_ref, eps_sem.at[0]),
        pltpu.make_async_copy(virt_hbm, virt_ref, eps_sem.at[1]),
    )
    for copy in eps:
        copy.start()

    def packed(codes):
        got = 0
        for c in reversed(codes):
            got = got * CODE + c + 1
        return got

    most = max(len(r) for r in partners)
    folk = [
        pick([packed(r[at:at + KIDS]) for r in partners], me) for at in range(0, most, KIDS)
    ]
    n_folk = pick([len(r) for r in partners], me)
    near = pick(n_near, me)

    def signal(sem, amount, limit):
        code = None
        for k in range(amount):
            code = folk[k // KIDS] if k % KIDS == 0 else lax.div(code, CODE)

            @pl.when(k < limit)
            def _():
                t = lax.rem(code, CODE) - 1
                pl.semaphore_signal(sem, inc=1, device_id=device(t), device_id_type=MESH)

    if deep > rows:
        held[:, rows:, :] = jnp.zeros((n_slots + 1, deep - rows, cols), BF16)
    signal(barrier, most, n_folk)

    kids = [pick([packed(r[s]) for r in routes], me) for s in range(n_slots + 1)]
    spread_at = [pick([r[k] for r in news], me) for k in range(rounds - 1)]
    todo = [pick([r[i] for r in steps], me) for i in range(2 * n_slots)]

    row = lax.broadcasted_iota(jnp.int32, (cols, cols), 0)
    col = lax.broadcasted_iota(jnp.int32, (cols, cols), 1)
    hit = row == lax.rem(col, width) * occ + col // width
    order[...] = jnp.where(hit, 1.0, 0.0).astype(BF16)
    own.wait()
    held[own_slot, 0:rows, :] = lax.dot_general(
        raw[...], order[...], NN, preferred_element_type=F32
    ).astype(BF16)
    pl.semaphore_wait(barrier, n_folk)

    def piece(slot, part):
        return held.at[slot, pl.ds(cuts[part][0], cuts[part][1])]

    def copies(slot, part, act):
        code = pick(kids, slot)
        q = jnp.where(slot == n_slots, p, lax.rem(slot, n_aux))
        for k in range(KIDS):
            this = lax.rem(code, CODE)
            code = lax.div(code, CODE)

            @pl.when(this > 0)
            def _():
                t = this - 1
                to = lax.rem(t, 2) * n_aux + q
                copy = pltpu.make_async_remote_copy(
                    src_ref=piece(slot, part), dst_ref=piece(to, part),
                    send_sem=send_sem.at[slot, part, k], recv_sem=recv_sem.at[to, part],
                    device_id=device(lax.div(t, 2)), device_id_type=MESH,
                )
                act(copy)

    for part in range(2):
        copies(own_slot, part, lambda copy: copy.start())
    close = max(n_near)
    signal(news_sem.at[0], close, near)
    for copy in eps:
        copy.wait()

    lane = lax.broadcasted_iota(jnp.int32, (1, LANES), 1)
    part = lane // width
    down = lax.broadcasted_iota(jnp.int32, (width, 1), 0)
    lane_in = lax.rem(lane, width)
    n_tiles = jnp.where(diag, 2, 1)

    def eps_down(which):
        got = jnp.zeros((width, 1), F32)
        for k in range(width):
            got = jnp.where(down == k, virt_ref[which * width + k], got)
        return got

    def eps_across(which):
        got = jnp.zeros((1, LANES), F32)
        for k in range(width):
            got = jnp.where(lane_in == k, virt_ref[which * width + k], got)
        return got

    occ_lane = []
    for cj in range(supers):
        got = jnp.zeros((1, LANES), F32)
        for t in range(groups):
            got = jnp.where(part == t, occ_ref[cj * groups + t], got)
        occ_lane.append(got)

    def prepare(t, c):
        block_l = jnp.where(t == 0, side_a, side_b)
        block_r = jnp.where(jnp.logical_and(diag, t == 0), side_a, side_b)
        base = -(eps_down(block_l) + eps_across(block_r))
        ints[t] = jnp.zeros((cols, cols), F32)
        for i in range(occ):
            for cj in range(i // groups, supers):
                below = base + (occ_lane[cj] + occ_ref[i])
                over[t, i * width:(i + 1) * width, cj * LANES:(cj + 1) * LANES] = (
                    (1.0 if cj == i // groups else 2.0) / below
                )
        return c

    lax.fori_loop(0, n_tiles, prepare, 0)

    def take(i, c):
        for r in range(1, rounds):

            @pl.when(i == spread_at[r - 1])
            def _():
                pl.semaphore_wait(news_sem.at[r - 1], near)
                signal(news_sem.at[r], close, near)

        entry = pick(todo, i)
        slot = lax.rem(lax.div(entry, 2), n_slots)
        meets = lax.div(entry, 4 * n_aux) == 1
        later = lax.rem(entry, 2)
        away = slot != own_slot
        for part in range(2):

            @pl.when(jnp.logical_and(later == part, away))
            def _():
                whole = piece(slot, part)
                pltpu.make_async_copy(whole, whole, recv_sem.at[slot, part]).wait()
                copies(slot, part, lambda copy: copy.start())

        side = lax.div(slot, n_aux)
        mine = jnp.where(diag, side, 0)
        left = jnp.where(diag, slot, lax.rem(slot, n_aux))
        right = jnp.where(diag, slot, n_aux + lax.rem(slot, n_aux))

        @pl.when(meets)
        def _():
            ints[mine] += lax.dot_general(held[left], held[right], TN, preferred_element_type=F32)

        return c

    lax.fori_loop(0, 2 * n_slots, take, 0)

    tall = -(-occ // 4)
    sums[...] = jnp.zeros_like(sums)
    r8 = lax.broadcasted_iota(jnp.int32, (8, LANES), 0)
    l8 = lax.broadcasted_iota(jnp.int32, (8, LANES), 1)
    wide = lax.broadcasted_iota(jnp.int32, (cols, LANES), 0)
    thin = lax.broadcasted_iota(jnp.int32, (cols, LANES), 1)
    fold = jnp.where(wide // width == thin, 1.0, 0.0).astype(BF16)
    ri = lax.broadcasted_iota(jnp.int32, (tall * 8, occ * 8), 0)
    rj = lax.broadcasted_iota(jnp.int32, (tall * 8, occ * 8), 1)
    gather = jnp.logical_and(lax.rem(ri, 8) < 4, rj // 8 == ri // 8 * 4 + lax.rem(ri, 8))
    gather = jnp.where(gather, 1.0, 0.0).astype(BF16)
    ones = jnp.ones((8, LANES), BF16)
    free = tall * occ

    def split(x):
        high = x.astype(BF16)
        return high, (x - high.astype(F32)).astype(BF16)

    def tile(t, c):
        total = jnp.zeros((width, LANES), F32)
        for ci in range(supers):
            for cj in range(ci, supers):
                block = [
                    ints[t, pl.ds((cj * groups + g) * width, width), pl.ds(ci * LANES, LANES)]
                    for g in range(groups)
                ]
                turned = []
                for r in range(groups):
                    mixed = block[r]
                    for g in range(1, groups):
                        mixed = jnp.where(part == g, block[(g + r) % groups], mixed)
                    turned.append(mixed if r == 0 else pltpu.roll(mixed, r * width, 1))
                for s in range(groups):
                    i = ci * groups + s
                    direct = ints[t, pl.ds(i * width, width), pl.ds(cj * LANES, LANES)]
                    inverse = over[t, pl.ds(i * width, width), pl.ds(cj * LANES, LANES)]
                    swapped = turned[(0 - s) % groups]
                    for g in range(1, groups):
                        swapped = jnp.where(part == g, turned[(g - s) % groups], swapped)
                    if ci == cj:
                        term = direct * (2.0 * direct - swapped) * inverse
                    else:
                        term = (direct * (direct - swapped) + swapped * swapped) * inverse
                    total = total + term
                    short = term[0:8]
                    for m in range(8, width, 8):
                        short = short + term[m:m + 8]
                    sums[i * 8:i * 8 + 8, cj * LANES:(cj + 1) * LANES] = short

        rows_of = [
            lax.dot_general(gather, x, NN, preferred_element_type=F32) for x in split(sums[...])
        ]
        pairs_of = [
            lax.dot_general(x, fold, NN, preferred_element_type=F32)
            for x in split(rows_of[0] + rows_of[1])
        ]
        by_ij = pairs_of[0] + pairs_of[1]
        packed_ij = by_ij[0:8]
        for g in range(1, tall):
            packed_ij = packed_ij + pltpu.roll(by_ij[g * 8:g * 8 + 8], g * occ, 1)
        spread = jnp.concatenate([jnp.zeros((LANES - width, LANES), F32), total], 0)
        by_row = [
            lax.dot_general(ones, x, NT, preferred_element_type=F32) for x in split(spread)
        ]
        by_row = by_row[0] + by_row[1]
        by_col = [
            lax.dot_general(ones[:, :width], x, NN, preferred_element_type=F32) for x in split(total)
        ]
        by_col = by_col[0] + by_col[1]
        folded = by_col
        for g in range(1, groups):
            folded = folded + pltpu.roll(by_col, g * width, 1)
        packed_ij = packed_ij * jnp.where(diag, 0.5, 1.0)
        both = (by_row + folded) * 0.5
        first = jnp.where(diag, jnp.where(t == 0, both, 0.0), by_row)
        second = jnp.where(diag, jnp.where(t == 1, both, 0.0), folded)
        near_turn = free - (LANES - width)
        far_turn = near_turn - width // 2
        shares = jnp.where(r8 == 3, pltpu.roll(second, far_turn % LANES, 1), 0.0)
        shares = jnp.where(r8 == 2, pltpu.roll(second, near_turn % LANES, 1), shares)
        shares = jnp.where(r8 == 1, pltpu.roll(first, far_turn % LANES, 1), shares)
        shares = jnp.where(r8 == 0, pltpu.roll(first, near_turn % LANES, 1), shares)
        shares = jnp.where(l8 < free + width // 2, shares, 0.0)
        out = jnp.where(l8 < free, packed_ij, shares)[0:4]

        @pl.when(t == 0)
        def _():
            message[...] = out

        @pl.when(t == 1)
        def _():
            message[...] += out

        return c

    lax.fori_loop(0, n_tiles, tile, 0)
    pl.semaphore_wait(news_sem.at[rounds - 1], near)

    def tell(k, c):
        t = me + k
        t = jnp.where(t >= n, t - n, t)
        pltpu.make_async_remote_copy(
            src_ref=message, dst_ref=slots.at[me],
            send_sem=msg_send, recv_sem=msg_recv,
            device_id=device(t), device_id_type=MESH,
        ).start()
        return c

    lax.fori_loop(1, n, tell, 0)
    slots[me] = message[...]
    for part_at in range(2):
        copies(own_slot, part_at, lambda copy: copy.wait_send())

    def flush(s, c):
        @pl.when(s != own_slot)
        def _():
            for part_at in range(2):
                copies(s, part_at, lambda copy: copy.wait_send())

        return c

    lax.fori_loop(0, n_slots, flush, 0)
    everyone = slots.at[pl.ds(0, n - 1)]
    pltpu.make_async_copy(everyone, everyone, msg_send).wait()
    pltpu.make_async_copy(everyone, everyone, msg_recv).wait()

    keep = l8[0:4] < free
    upper = r8[0:4] < 2
    acc = None
    for k in range(n):
        a, b, _ = tiles[k]
        row0 = jnp.where(v == a, 1.0, 0.0)
        row1 = jnp.where(v == b, 1.0, 0.0)
        term = slots[k] * jnp.where(keep, 1.0, jnp.where(upper, row0, row1))
        acc = term if acc is None else acc + term
    done_ref[...] = acc


def table_unpack(occ, width, done_ref, share_ref, pair_ref):
    tall = -(-occ // 4)
    free = tall * occ
    done = done_ref[...]
    share = done[0:2] + done[2:4]
    share_ref[...] = jnp.concatenate(
        [share[0, free:free + width // 2], share[1, free:free + width // 2]], 0
    )
    blocks = [done] + [pltpu.roll(done, LANES - g * occ, 1) for g in range(1, tall)]
    square = jnp.concatenate(blocks + [jnp.zeros((LANES - 4 * tall, LANES), F32)], 0)
    square = jnp.where(lax.broadcasted_iota(jnp.int32, (LANES, LANES), 1) < occ, square, 0.0)
    pair = square + square.T
    pair_ref[...] = pair[0:occ, 0:occ]


def table_call(n_virt, n_aux, occ, plan, three_index, eps_occ, eps_virt):
    rows, cols = three_index.shape
    width = cols // occ
    deep = -(-rows // 16) * 16
    n = n_virt * n_aux
    n_slots = 2 * n_aux
    vmem = pl.BlockSpec(memory_space=pltpu.VMEM)
    hbm = pl.BlockSpec(memory_space=pltpu.HBM)
    done = pl.pallas_call(
        functools.partial(table_kernel, n_virt, n_aux, occ, plan),
        out_shape=pltpu.VMEM((4, LANES), F32),
        in_specs=[hbm, hbm, hbm],
        out_specs=vmem,
        scratch_shapes=[
            pltpu.VMEM((rows, cols), BF16),
            pltpu.VMEM((n_slots + 1, deep, cols), BF16),
            pltpu.VMEM((cols, cols), BF16),
            pltpu.VMEM((2, cols, cols), F32),
            pltpu.VMEM((2, cols, cols), F32),
            pltpu.VMEM((occ * 8, cols), F32),
            pltpu.VMEM((4, LANES), F32),
            pltpu.VMEM((n, 4, LANES), F32),
            pltpu.SMEM(eps_occ.shape, F32),
            pltpu.SMEM(eps_virt.shape, F32),
            pltpu.SemaphoreType.DMA,
            pltpu.SemaphoreType.DMA((2,)),
            pltpu.SemaphoreType.DMA((n_slots + 1, 2, KIDS)),
            pltpu.SemaphoreType.DMA((n_slots, 2)),
            pltpu.SemaphoreType.DMA,
            pltpu.SemaphoreType.DMA,
            pltpu.SemaphoreType.REGULAR((len(plan[5][0]) + 1,)),
        ],
        compiler_params=pltpu.CompilerParams(collective_id=0, has_side_effects=True),
    )(three_index, eps_occ, eps_virt)
    return pl.pallas_call(
        functools.partial(table_unpack, occ, width),
        out_shape=(
            jax.ShapeDtypeStruct((width,), F32),
            jax.ShapeDtypeStruct((occ, occ), F32),
        ),
        in_specs=[vmem],
        out_specs=(vmem, vmem),
    )(pltpu.with_memory_space_constraint(done, pltpu.VMEM))


def unpack(occ, width, done_ref, share_ref, pair_ref):
    tall = -(-occ // 8)
    free = tall * width
    done = done_ref[...]
    share = done[0:1] + done[1:2]
    share_ref[...] = share[0, free:free + width]
    blocks = [done] + [pltpu.roll(done, LANES - g * width, 1) for g in range(1, tall)]
    square = jnp.concatenate(blocks + [jnp.zeros((LANES - 8 * tall, LANES), F32)], 0)
    square = jnp.where(lax.broadcasted_iota(jnp.int32, (LANES, LANES), 1) < occ, square, 0.0)
    pair = square + square.T
    pair_ref[...] = pair[0:occ, 0:occ]


def on_device(n_virt, n_aux, three_index, eps_occ, eps_virt):
    occ = eps_occ.shape[0]
    rows, cols = three_index.shape
    width = cols // occ
    pitch = -(-rows // 16) * 16
    n = n_virt * n_aux
    vmem = pl.BlockSpec(memory_space=pltpu.VMEM)
    smem = pl.BlockSpec(memory_space=pltpu.SMEM)
    plan = PLANS.get((n_virt, n_aux))
    if plan is not None:
        return table_call(n_virt, n_aux, occ, plan, three_index, eps_occ, eps_virt)
    done = pl.pallas_call(
        functools.partial(kernel, n_virt, n_aux, occ),
        out_shape=jax.ShapeDtypeStruct((8, LANES), F32),
        in_specs=[vmem, smem, smem],
        out_specs=vmem,
        scratch_shapes=[
            pltpu.VMEM((2, n_aux, rows, cols), BF16),
            pltpu.VMEM((cols, n_aux * pitch), BF16),
            pltpu.VMEM((n_aux * pitch, cols), BF16),
            pltpu.VMEM((cols, cols), BF16),
            pltpu.VMEM((cols, cols), BF16),
            pltpu.VMEM((cols, cols), F32),
            pltpu.VMEM((occ * 8, cols), F32),
            pltpu.VMEM((8, LANES), F32),
            pltpu.VMEM((8, LANES), F32),
            pltpu.VMEM((n, 8, LANES), F32),
            pltpu.SemaphoreType.DMA,
            pltpu.SemaphoreType.DMA((3, n_aux)),
            pltpu.SemaphoreType.DMA((2, n_aux)),
            pltpu.SemaphoreType.DMA,
            pltpu.SemaphoreType.DMA,
        ],
        compiler_params=pltpu.CompilerParams(collective_id=0, has_side_effects=True),
    )(three_index, eps_occ, eps_virt)
    return pl.pallas_call(
        functools.partial(unpack, occ, width),
        out_shape=(
            jax.ShapeDtypeStruct((width,), F32),
            jax.ShapeDtypeStruct((occ, occ), F32),
        ),
        in_specs=[vmem],
        out_specs=(vmem, vmem),
    )(done)


def solution(mesh):
    n_virt, n_aux = mesh.shape["virt"], mesh.shape["aux"]
    assert n_virt == 2 * n_aux and n_aux % 2 == 0
    in_specs = (P("aux", "virt"), P(), P())
    out_specs = (P("virt"), P())
    return jax.shard_map(
        functools.partial(on_device, n_virt, n_aux), mesh=mesh,
        in_specs=in_specs, out_specs=out_specs, check_vma=False,
    )
```

```python
import functools

import jax
import jax.numpy as jnp
from jax import lax
from jax.experimental import pallas as pl
from jax.experimental.pallas import tpu as pltpu
from jax.sharding import PartitionSpec as P

MESH = pl.DeviceIdType.MESH
F32 = jnp.float32
BF16 = jnp.bfloat16
EXACT = lax.Precision.HIGHEST
LANES = 128
NT = (((1,), (1,)), ((), ()))
NN = (((1,), (0,)), ((), ()))


def distances(n_aux):
    return list(range(1, n_aux + 1, 2)) + list(range(2, n_aux + 1, 2))


def pick(table, at):
    got = table[0] + jnp.int32(0)
    for k in range(1, len(table)):
        got = jnp.where(at == k, table[k] + jnp.int32(0), got)
    return got


def label_of(virt, n_virt):
    return lax.rem(virt, 2) * (n_virt // 2) + virt // 2


def virt_of(label, n_virt):
    half = n_virt // 2
    return lax.rem(label, half) * 2 + label // half


def kernel(
    n_virt, n_aux, occ,
    x_ref, occ_ref, virt_ref,
    done_ref,
    held, lhs, rhs, order, order_t, ints, sums, parts, message, slots,
    own_sem, send_sem, recv_sem, msg_send, msg_recv,
):
    rows, cols = x_ref.shape
    pitch = -(-rows // 16) * 16
    width = cols // occ
    groups = LANES // width
    supers = occ // groups
    n = n_virt * n_aux
    v = lax.axis_index("virt")
    p = lax.axis_index("aux")
    me = v * n_aux + p
    table = distances(n_aux)
    label = label_of(v, n_virt)
    other = virt_of(lax.rem(label + pick(table, p), n_virt), n_virt)
    lower = label < n_virt // 2
    solo = jnp.logical_and(p == n_aux - 1, jnp.logical_not(lower))
    extra = jnp.logical_and(p == n_aux // 2 - 1, lower)

    barrier = pltpu.get_barrier_semaphore()

    def greet(k, c):
        t = lax.rem(me + k, n)
        pl.semaphore_signal(
            barrier, inc=1,
            device_id={"virt": t // n_aux, "aux": lax.rem(t, n_aux)},
            device_id_type=MESH,
        )
        return c

    lax.fori_loop(1, n, greet, 0)
    own = pltpu.make_async_copy(x_ref, held.at[0, p], own_sem)
    own.start()
    pl.semaphore_wait(barrier, n - 1)

    pairs = n_aux // 2

    def place(k):
        return lax.rem(p // 2 + k // 2, pairs) * 2 + lax.rem(p + k, 2)

    def share_own(k):
        return pltpu.make_async_remote_copy(
            src_ref=x_ref, dst_ref=held.at[0, p],
            send_sem=send_sem.at[0, k], recv_sem=recv_sem.at[0, p],
            device_id={"virt": v, "aux": place(k)}, device_id_type=MESH,
        )

    def hand_on(k):
        q = place(k)
        return pltpu.make_async_remote_copy(
            src_ref=held.at[0, q], dst_ref=held.at[0, q],
            send_sem=send_sem.at[2, k], recv_sem=recv_sem.at[0, q],
            device_id={"virt": v, "aux": place(1)}, device_id_type=MESH,
        )

    def share_other(k):
        q = place(k)
        target = lax.rem(label + n_virt - pick(table, q), n_virt)
        copy = pltpu.make_async_remote_copy(
            src_ref=x_ref, dst_ref=held.at[1, p],
            send_sem=send_sem.at[1, k], recv_sem=recv_sem.at[1, p],
            device_id={"virt": virt_of(target, n_virt), "aux": q}, device_id_type=MESH,
        )
        wanted = jnp.logical_or(q < n_aux - 1, target < n_virt // 2)
        return copy, wanted

    for k in list(range(2, n_aux, 2)) + [1]:
        share_own(k).start()
    for k in range(n_aux):
        copy, wanted = share_other(k)
        pl.when(wanted)(copy.start)

    def arrived(side, q):
        pltpu.make_async_copy(
            held.at[side, q], held.at[side, q], recv_sem.at[side, q]
        ).wait()

    row = lax.broadcasted_iota(jnp.int32, (cols, cols), 0)
    col = lax.broadcasted_iota(jnp.int32, (cols, cols), 1)
    hit = col == lax.rem(row, width) * occ + row // width
    order[...] = jnp.where(hit, 1.0, 0.0).astype(BF16)
    hit = row == lax.rem(col, width) * occ + col // width
    order_t[...] = jnp.where(hit, 1.0, 0.0).astype(BF16)
    lhs[...] = jnp.zeros_like(lhs)
    rhs[...] = jnp.zeros_like(rhs)

    def turn(k):
        lhs[:, k * pitch:k * pitch + rows] = lax.dot_general(
            order[...], held[0, place(k)], NT, preferred_element_type=F32
        ).astype(BF16)

    own.wait()
    turn(0)
    for k in range(2, n_aux, 2):
        arrived(0, place(k))
        hand_on(k).start()
        turn(k)
    for k in range(1, n_aux, 2):
        arrived(0, place(k))
        turn(k)

    lane = lax.broadcasted_iota(jnp.int32, (1, LANES), 1)
    part = lane // width
    down = lax.broadcasted_iota(jnp.int32, (width, 1), 0)
    lane_in = lax.rem(lane, width)

    def eps_down(which):
        got = jnp.zeros((width, 1), F32)
        for k in range(width):
            got = jnp.where(down == k, virt_ref[which * width + k], got)
        return got

    def eps_across(which):
        got = jnp.zeros((1, LANES), F32)
        for k in range(width):
            got = jnp.where(lane_in == k, virt_ref[which * width + k], got)
        return got

    occ_lane = []
    for cj in range(supers):
        got = jnp.zeros((1, LANES), F32)
        for t in range(groups):
            got = jnp.where(part == t, occ_ref[cj * groups + t], got)
        occ_lane.append(got)

    tall = -(-occ // 8)
    sums[...] = jnp.zeros_like(sums)
    n_tiles = jnp.where(extra, 2, 1)
    r8 = lax.broadcasted_iota(jnp.int32, (8, LANES), 0)
    l8 = lax.broadcasted_iota(jnp.int32, (8, LANES), 1)
    free = tall * width

    def tile(t, c):
        diag = jnp.logical_or(solo, jnp.logical_and(extra, t == 0))
        source = jnp.where(diag, 0, 1)

        for k in range(n_aux):

            @pl.when(source == 1)
            def _():
                arrived(1, place(k))

            rhs[k * pitch:k * pitch + rows, :] = lax.dot_general(
                held[source, place(k)], order_t[...], NN, preferred_element_type=F32
            ).astype(BF16)
        ints[...] = lax.dot_general(lhs[...], rhs[...], NN, preferred_element_type=F32)

        base = -(eps_down(v) + eps_across(jnp.where(diag, v, other)))
        total = jnp.zeros((width, LANES), F32)
        for ci in range(supers):
            for cj in range(ci, supers):
                turned = []
                for g in range(groups):
                    block = ints[pl.ds((cj * groups + g) * width, width), pl.ds(ci * LANES, LANES)]
                    turned.append([block if r == 0 else pltpu.roll(block, r * width, 1) for r in range(groups)])
                for s in range(groups):
                    i = ci * groups + s
                    direct = ints[pl.ds(i * width, width), pl.ds(cj * LANES, LANES)]
                    swapped = turned[0][(0 - s) % groups]
                    for g in range(1, groups):
                        swapped = jnp.where(part == g, turned[g][(g - s) % groups], swapped)
                    below = base + (occ_lane[cj] + occ_ref[i])
                    if ci == cj:
                        term = direct * (2.0 * direct - swapped) / below
                    else:
                        term = 2.0 * (direct * (direct - swapped) + swapped * swapped) / below
                    total = total + term
                    short = term[0:8]
                    for m in range(8, width, 8):
                        short = short + term[m:m + 8]
                    sums[i * 8:i * 8 + 8, cj * LANES:(cj + 1) * LANES] = short

        wide = lax.broadcasted_iota(jnp.int32, (cols, LANES), 0)
        thin = lax.broadcasted_iota(jnp.int32, (cols, LANES), 1)
        fold = jnp.where(wide // width == thin, 1.0, 0.0)
        by_j = lax.dot_general(sums[...], fold, NN, precision=EXACT, preferred_element_type=F32)
        ri = lax.broadcasted_iota(jnp.int32, (tall * 8, occ * 8), 0)
        rj = lax.broadcasted_iota(jnp.int32, (tall * 8, occ * 8), 1)
        by_ij = lax.dot_general(
            jnp.where(rj // 8 == ri, 1.0, 0.0), by_j, NN,
            precision=EXACT, preferred_element_type=F32,
        )
        packed = by_ij[0:8]
        for g in range(1, tall):
            packed = packed + pltpu.roll(by_ij[g * 8:g * 8 + 8], g * width, 1)
        pads = [jnp.zeros((free, LANES), F32), total]
        if free + width < LANES:
            pads.append(jnp.zeros((LANES - free - width, LANES), F32))
        spread = jnp.concatenate(pads, 0)
        by_row = lax.dot_general(
            jnp.ones((8, LANES), F32), spread, NT, precision=EXACT, preferred_element_type=F32)
        by_col = lax.dot_general(
            jnp.ones((8, width), F32), total, NN, precision=EXACT, preferred_element_type=F32)
        folded = by_col
        for g in range(1, groups):
            folded = folded + pltpu.roll(by_col, g * width, 1)
        packed = packed * jnp.where(diag, 0.5, 1.0)
        first = jnp.where(diag, (by_row + folded) * 0.5, by_row)
        second = jnp.where(diag, 0.0, folded)
        out = jnp.where(l8 < free, packed, jnp.where(r8 == 0, first, jnp.where(r8 == 1, second, 0.0)))

        @pl.when(t == 0)
        def _():
            message[...] = out

        @pl.when(t == 1)
        def _():
            message[...] += out

        return c

    lax.fori_loop(0, n_tiles, tile, 0)

    def tell(k, c):
        t = lax.rem(me + k, n)
        pltpu.make_async_remote_copy(
            src_ref=message, dst_ref=slots.at[me],
            send_sem=msg_send, recv_sem=msg_recv,
            device_id={"virt": t // n_aux, "aux": lax.rem(t, n_aux)},
            device_id_type=MESH,
        ).start()
        return c

    lax.fori_loop(1, n, tell, 0)
    slots[me] = message[...]
    for k in list(range(2, n_aux, 2)) + [1]:
        share_own(k).wait_send()
    for k in range(2, n_aux, 2):
        hand_on(k).wait_send()
    for k in range(n_aux):
        copy, wanted = share_other(k)
        pl.when(wanted)(copy.wait_send)
    everyone = slots.at[pl.ds(0, n - 1)]
    pltpu.make_async_copy(everyone, everyone, msg_send).wait()
    pltpu.make_async_copy(everyone, everyone, msg_recv).wait()

    keep = jnp.logical_or(l8 < free, r8 < 0)

    def add(k, acc):
        sv = k // n_aux
        so = virt_of(lax.rem(label_of(sv, n_virt) + pick(table, lax.rem(k, n_aux)), n_virt), n_virt)
        row0 = jnp.where(sv == v, 1.0, 0.0)
        row1 = jnp.where(so == v, 1.0, 0.0)
        weight = jnp.where(keep, 1.0, jnp.where(r8 == 0, row0, row1))
        return acc + slots[k] * weight

    done = lax.fori_loop(0, n, add, jnp.zeros((8, LANES), F32))
    done_ref[...] = done


TILES = (
    (0, 2, 0),
    (0, 1, 0),
    (0, 2, 1),
    (1, 2, 0),
    (2, 3, 0),
    (1, 3, 1),
    (1, 3, 0),
    (0, 3, 0),
    (0, 4, 0),
    (0, 5, 0),
    (2, 4, 0),
    (2, 5, 0),
    (1, 4, 0),
    (1, 5, 0),
    (3, 4, 0),
    (3, 5, 0),
    (0, 6, 0),
    (0, 7, 0),
    (2, 6, 0),
    (2, 7, 0),
    (1, 6, 0),
    (1, 7, 0),
    (3, 6, 0),
    (3, 7, 0),
    (6, 4, 0),
    (6, 7, 0),
    (7, 4, 0),
    (6, 4, 1),
    (6, 5, 0),
    (7, 5, 1),
    (4, 5, 0),
    (7, 5, 0),
)
ROUTES = (
    ((2,), (), (18,), (2,), (8, 7), (7, 8), (), (8,), ()),
    ((4, 16), (0, 4, 16), (0,), (), (), (), (), (), ()),
    ((14,), (14,), (2, 14, 34), (0, 14), (), (), (7,), (1,), ()),
    ((), (), (), (), (5,), (), (1, 8), (), (4, 18)),
    ((), (), (), (), (11, 13), (11,), (11,), (), (10, 40)),
    ((3, 12), (3, 12, 26), (3, 26), (3, 26), (15,), (), (), (9,), ()),
    ((6,), (6,), (6, 10), (10,), (), (), (15,), (15,), ()),
    ((), (), (), (), (), (), (9,), (11,), (6, 12, 24)),
    ((18, 32), (18, 32), (), (), (21, 25), (), (), (25,), (1, 20)),
    ((), (), (16,), (16, 34), (23,), (23,), (), (), (1, 22, 38)),
    ((22, 38), (), (22, 36), (7, 38), (29,), (), (29, 17), (17, 29), ()),
    ((36,), (5,), (5,), (5, 20), (), (), (), (19,), ()),
    ((), (), (), (42,), (), (), (), (), (9, 44)),
    ((24,), (24, 42), (24, 40), (), (19, 31), (31,), (19,), (), (9, 28)),
    ((30,), (30, 46), (13, 30, 44), (13,), (), (21, 25, 60), (25,), (), ()),
    ((), (13, 15), (), (28, 44), (), (), (23,), (23, 27), ()),
    ((34,), (34,), (), (), (37, 41), (37, 45), (), (), (17, 53)),
    ((), (), (32,), (32,), (), (39,), (), (), (29, 49)),
    ((), (), (38,), (), (45, 54), (), (), (33, 45), (21, 53, 60)),
    ((), (36, 20), (), (36,), (), (), (35,), (35,), (21, 53)),
    ((42,), (), (42,), (), (), (), (), (), (27, 57)),
    ((26,), (40,), (), (40,), (35,), (35, 47), (), (), (19, 57, 27)),
    ((46,), (), (46,), (46,), (), (), (41,), (), (27, 61, 31)),
    ((28,), (44,), (), (), (39,), (62,), (39, 43), (39, 43), (31, 61)),
    ((33, 50, 56), (33,), (50, 56), (50, 56), (), (53, 17), (), (), ()),
    ((), (48, 54, 56), (33,), (), (), (52,), (), (), ()),
    ((), (), (), (), (55,), (55,), (55,), (55, 60, 49), (48, 54)),
    ((), (), (45, 37), (37, 48), (60, 49), (), (49,), (), ()),
    ((), (41,), (), (41,), (59, 63), (59, 61), (), (), (51, 58)),
    ((62, 43), (43, 51), (51,), (51,), (), (), (57,), (57,), ()),
    ((), (), (), (), (), (63,), (63, 59), (63, 59), (52, 58, 62)),
    ((47, 52), (), (47,), (47, 52, 58), (61,), (), (), (), ()),
)
STEPS = (
    (0, 1, 2, 3, 4, 10, 8, 6, 5, 27, 7, 25, 14, 31, 12, 29),
    (2, 3, 0, 1, 10, 4, 27, 5, 8, 25, 6, 12, 7, 29, 14, 31),
    (4, 21, 6, 23, 2, 14, 19, 0, 31, 17, 12, 29, 10, 8, 27, 25),
    (6, 4, 14, 7, 5, 31, 2, 10, 12, 3, 8, 29, 0, 27, 1, 25),
    (10, 8, 11, 9, 12, 2, 13, 0, 19, 14, 17, 15, 6, 4, 23, 21),
    (2, 19, 0, 17, 4, 21, 10, 6, 8, 23, 27, 25, 12, 14, 29, 31),
    (4, 5, 6, 7, 2, 12, 3, 29, 0, 14, 1, 31, 8, 10, 25, 27),
    (4, 5, 12, 6, 29, 7, 14, 2, 31, 8, 3, 10, 0, 1, 25, 27),
    (2, 3, 8, 0, 6, 1, 25, 14, 7, 4, 12, 10, 5, 31, 27, 29),
    (2, 6, 10, 3, 0, 7, 4, 1, 8, 5, 27, 12, 25, 14, 31, 29),
    (4, 5, 6, 7, 14, 0, 12, 31, 1, 29, 2, 8, 3, 10, 25, 27),
    (6, 7, 4, 5, 2, 0, 3, 14, 1, 10, 31, 8, 12, 27, 25, 29),
    (6, 2, 7, 3, 8, 4, 5, 9, 10, 14, 27, 0, 17, 12, 31, 29),
    (2, 8, 12, 3, 10, 9, 4, 14, 5, 27, 6, 29, 15, 0, 23, 17),
    (4, 5, 6, 7, 2, 10, 3, 14, 27, 12, 31, 0, 29, 8, 1, 25),
    (6, 7, 4, 5, 14, 2, 31, 12, 8, 3, 10, 9, 29, 0, 27, 17),
    (8, 9, 10, 2, 4, 11, 14, 19, 15, 5, 12, 6, 0, 29, 17, 23),
    (4, 10, 11, 2, 5, 8, 6, 14, 19, 9, 15, 23, 12, 0, 29, 17),
    (14, 4, 15, 2, 3, 5, 12, 8, 9, 6, 0, 10, 29, 23, 27, 17),
    (2, 3, 4, 14, 15, 6, 5, 12, 29, 23, 10, 8, 0, 27, 9, 17),
    (0, 8, 1, 10, 25, 2, 11, 6, 12, 14, 19, 4, 7, 5, 29, 31),
    (10, 11, 8, 14, 0, 9, 15, 2, 12, 17, 6, 19, 13, 23, 4, 21),
    (6, 4, 0, 7, 12, 5, 14, 1, 31, 2, 29, 10, 8, 3, 27, 25),
    (14, 15, 6, 12, 4, 0, 13, 10, 23, 2, 8, 21, 11, 1, 25, 19),
    (0, 1, 2, 3, 10, 6, 4, 27, 7, 5, 14, 12, 31, 8, 25, 29),
    (2, 3, 0, 1, 10, 8, 6, 4, 27, 25, 14, 7, 5, 12, 31, 29),
    (14, 12, 6, 4, 8, 15, 23, 5, 9, 29, 0, 10, 17, 2, 11, 19),
    (6, 23, 4, 21, 2, 14, 12, 8, 19, 31, 25, 29, 10, 0, 17, 27),
    (10, 8, 2, 0, 11, 9, 19, 17, 6, 4, 14, 12, 7, 31, 5, 29),
    (2, 19, 0, 17, 6, 4, 10, 8, 23, 21, 27, 25, 14, 12, 31, 29),
    (14, 12, 15, 13, 4, 10, 6, 11, 2, 8, 21, 0, 23, 9, 17, 19),
    (6, 7, 4, 5, 0, 14, 1, 12, 31, 29, 8, 10, 2, 25, 11, 19),
)
PARTNERS = (
    (1, 2, 4, 8, 3, 9),
    (0, 3, 5, 9, 2, 8),
    (3, 0, 6, 10, 1, 7, 11, 17),
    (2, 1, 7, 11, 0, 4, 6, 9, 10),
    (5, 6, 0, 12, 3, 7, 13, 20),
    (4, 7, 1, 13, 6),
    (7, 4, 2, 14, 3, 5, 15),
    (6, 5, 3, 15, 2, 4, 12),
    (9, 10, 12, 0, 16, 1, 24),
    (8, 11, 13, 1, 17, 0, 3, 19, 21),
    (11, 8, 14, 2, 18, 3, 19),
    (10, 9, 15, 3, 19, 2, 18),
    (13, 14, 8, 4, 20, 7, 21, 22),
    (12, 15, 9, 5, 21, 4, 14, 20, 22),
    (15, 12, 10, 6, 22, 13, 17, 23, 30),
    (14, 13, 11, 7, 23, 6, 22),
    (17, 18, 20, 8, 24, 22, 25, 26),
    (16, 19, 21, 9, 25, 2, 14, 24),
    (19, 16, 22, 10, 26, 11, 27, 30),
    (18, 17, 23, 11, 27, 9, 10, 26),
    (21, 22, 16, 12, 28, 4, 13),
    (20, 23, 17, 13, 29, 9, 12, 28),
    (23, 20, 18, 14, 30, 12, 13, 15, 16, 27),
    (22, 21, 19, 15, 31, 14, 30),
    (25, 26, 28, 16, 8, 17, 27),
    (24, 27, 29, 17, 16, 26, 28),
    (27, 24, 30, 18, 16, 19, 25, 31),
    (26, 25, 31, 19, 18, 22, 24, 30),
    (29, 30, 24, 20, 21, 25, 31),
    (28, 31, 25, 21, 30),
    (31, 28, 26, 22, 14, 18, 23, 27, 29),
    (30, 29, 27, 23, 26, 28),
)
NEAR = (4, 4, 4, 4, 4, 4, 4, 4, 5, 5, 5, 5, 5, 5, 5, 5, 5, 5, 5, 5, 5, 5, 5, 5, 4, 4, 4, 4, 4, 4, 4, 4)
NEWS = (
    (7, 12, 14),
    (8, 12, 15),
    (7, 11, 14),
    (2, 8, 14),
    (2, 6, 9),
    (6, 11, 15),
    (8, 12, 15),
    (3, 8, 13),
    (3, 8, 14),
    (3, 7, 13),
    (7, 11, 15),
    (5, 8, 11),
    (0, 4, 9),
    (2, 7, 13),
    (5, 8, 12),
    (5, 10, 12),
    (2, 7, 13),
    (0, 4, 11),
    (4, 8, 13),
    (2, 6, 11),
    (0, 3, 8),
    (2, 7, 13),
    (2, 8, 13),
    (2, 11, 15),
    (7, 10, 12),
    (6, 11, 15),
    (4, 9, 14),
    (5, 10, 14),
    (4, 8, 13),
    (6, 11, 15),
    (2, 7, 11),
    (5, 9, 13),
)
PLANS = {(8, 4): (TILES, ROUTES, STEPS, PARTNERS, NEAR, NEWS)}


TN = (((0,), (0,)), ((), ()))
KIDS = 4
CODE = 128


def table_kernel(
    n_virt, n_aux, occ, plan,
    x_ref, occ_hbm, virt_hbm,
    done_ref,
    raw, held, order, ints, over, sums, message, slots, occ_ref, virt_ref,
    own_sem, eps_sem, send_sem, recv_sem, msg_send, msg_recv, news_sem,
):
    rows, cols = x_ref.shape
    deep = held.shape[1]
    width = cols // occ
    groups = LANES // width
    supers = occ // groups
    n = n_virt * n_aux
    v = lax.axis_index("virt")
    p = lax.axis_index("aux")
    me = v * n_aux + p
    tiles, routes, steps, partners, n_near, news = plan
    rounds = len(news[0]) + 1
    half = -(-rows // 32) * 16
    cuts = ((0, half), (half, -(-rows // 8) * 8 - half))
    n_slots = 2 * n_aux

    def device(t):
        return {"virt": lax.div(t, n_aux), "aux": lax.rem(t, n_aux)}

    barrier = pltpu.get_barrier_semaphore()

    side_a = pick([t[0] for t in tiles], me)
    side_b = pick([t[1] for t in tiles], me)
    diag = pick([t[2] for t in tiles], me) == 1
    own_slot = jnp.where(side_a == v, p, jnp.where(side_b == v, n_aux + p, n_slots))
    owns = []
    for d, (a, b, _) in enumerate(tiles):
        q = d % n_aux
        owns.append(q if a == d // n_aux else n_aux + q if b == d // n_aux else n_slots)
    own = pltpu.make_async_copy(x_ref, raw, own_sem)
    own.start()
    eps = (
        pltpu.make_async_copy(occ_hbm, occ_ref, eps_sem.at[0]),
        pltpu.make_async_copy(virt_hbm, virt_ref, eps_sem.at[1]),
    )
    for copy in eps:
        copy.start()

    def packed(codes):
        got = 0
        for c in reversed(codes):
            got = got * CODE + c + 1
        return got

    most = max(len(r) for r in partners)
    folk = [
        pick([packed(r[at:at + KIDS]) for r in partners], me) for at in range(0, most, KIDS)
    ]
    n_folk = pick([len(r) for r in partners], me)
    near = pick(n_near, me)

    def signal(sem, amount, limit):
        code = None
        for k in range(amount):
            code = folk[k // KIDS] if k % KIDS == 0 else lax.div(code, CODE)

            @pl.when(k < limit)
            def _():
                t = lax.rem(code, CODE) - 1
                pl.semaphore_signal(sem, inc=1, device_id=device(t), device_id_type=MESH)

    if deep > rows:
        held[:, rows:, :] = jnp.zeros((n_slots + 1, deep - rows, cols), BF16)
    signal(barrier, most, n_folk)

    row = lax.broadcasted_iota(jnp.int32, (cols, cols), 0)
    col = lax.broadcasted_iota(jnp.int32, (cols, cols), 1)
    hit = row == lax.rem(col, width) * occ + col // width
    order[...] = jnp.where(hit, 1.0, 0.0).astype(BF16)
    own.wait()
    held[own_slot, 0:rows, :] = lax.dot_general(
        raw[...], order[...], NN, preferred_element_type=F32
    ).astype(BF16)
    pl.semaphore_wait(barrier, n_folk)

    own_kids = pick([packed(r[o]) for r, o in zip(routes, owns)], me)

    def piece(slot, part):
        return held.at[slot, pl.ds(cuts[part][0], cuts[part][1])]

    def copies(slot, part, code, act):
        q = jnp.where(slot == n_slots, p, lax.rem(slot, n_aux))
        for k in range(KIDS):
            this = lax.rem(code, CODE)
            code = lax.div(code, CODE)

            @pl.when(this > 0)
            def _():
                t = this - 1
                to = lax.rem(t, 2) * n_aux + q
                copy = pltpu.make_async_remote_copy(
                    src_ref=piece(slot, part), dst_ref=piece(to, part),
                    send_sem=send_sem.at[slot, part, k], recv_sem=recv_sem.at[to, part],
                    device_id=device(lax.div(t, 2)), device_id_type=MESH,
                )
                act(copy)

    for part in range(2):
        copies(own_slot, part, own_kids, lambda copy: copy.start())
    close = max(n_near)
    signal(news_sem.at[0], close, near)
    kids = [pick([packed(r[s]) for r in routes], me) for s in range(n_slots + 1)]
    spread_at = [pick([r[k] for r in news], me) for k in range(rounds - 1)]
    todo = [pick([r[i] for r in steps], me) for i in range(2 * n_slots)]
    for copy in eps:
        copy.wait()

    lane = lax.broadcasted_iota(jnp.int32, (1, LANES), 1)
    part = lane // width
    down = lax.broadcasted_iota(jnp.int32, (width, 1), 0)
    lane_in = lax.rem(lane, width)
    n_tiles = jnp.where(diag, 2, 1)

    def eps_down(which):
        got = jnp.zeros((width, 1), F32)
        for k in range(width):
            got = jnp.where(down == k, virt_ref[which * width + k], got)
        return got

    def eps_across(which):
        got = jnp.zeros((1, LANES), F32)
        for k in range(width):
            got = jnp.where(lane_in == k, virt_ref[which * width + k], got)
        return got

    occ_lane = []
    for cj in range(supers):
        got = jnp.zeros((1, LANES), F32)
        for t in range(groups):
            got = jnp.where(part == t, occ_ref[cj * groups + t], got)
        occ_lane.append(got)

    def prepare(t, c):
        block_l = jnp.where(t == 0, side_a, side_b)
        block_r = jnp.where(jnp.logical_and(diag, t == 0), side_a, side_b)
        base = -(eps_down(block_l) + eps_across(block_r))
        ints[t] = jnp.zeros((cols, cols), F32)
        for i in range(occ):
            for cj in range(i // groups, supers):
                below = base + (occ_lane[cj] + occ_ref[i])
                over[t, i * width:(i + 1) * width, cj * LANES:(cj + 1) * LANES] = (
                    (1.0 if cj == i // groups else 2.0) / below
                )
        return c

    lax.fori_loop(0, n_tiles, prepare, 0)

    def take(i, c):
        for r in range(1, rounds):

            @pl.when(i == spread_at[r - 1])
            def _():
                pl.semaphore_wait(news_sem.at[r - 1], near)
                signal(news_sem.at[r], close, near)

        entry = pick(todo, i)
        slot = lax.rem(lax.div(entry, 2), n_slots)
        meets = lax.div(entry, 4 * n_aux) == 1
        later = lax.rem(entry, 2)
        away = slot != own_slot
        for part in range(2):

            @pl.when(jnp.logical_and(later == part, away))
            def _():
                whole = piece(slot, part)
                pltpu.make_async_copy(whole, whole, recv_sem.at[slot, part]).wait()
                copies(slot, part, pick(kids, slot), lambda copy: copy.start())

        side = lax.div(slot, n_aux)
        mine = jnp.where(diag, side, 0)
        left = jnp.where(diag, slot, lax.rem(slot, n_aux))
        right = jnp.where(diag, slot, n_aux + lax.rem(slot, n_aux))

        @pl.when(meets)
        def _():
            ints[mine] += lax.dot_general(held[left], held[right], TN, preferred_element_type=F32)

        return c

    lax.fori_loop(0, 2 * n_slots, take, 0)

    tall = -(-occ // 4)
    sums[...] = jnp.zeros_like(sums)
    r8 = lax.broadcasted_iota(jnp.int32, (8, LANES), 0)
    l8 = lax.broadcasted_iota(jnp.int32, (8, LANES), 1)
    wide = lax.broadcasted_iota(jnp.int32, (cols, LANES), 0)
    thin = lax.broadcasted_iota(jnp.int32, (cols, LANES), 1)
    fold = jnp.where(wide // width == thin, 1.0, 0.0).astype(BF16)
    ri = lax.broadcasted_iota(jnp.int32, (tall * 8, occ * 8), 0)
    rj = lax.broadcasted_iota(jnp.int32, (tall * 8, occ * 8), 1)
    gather = jnp.logical_and(lax.rem(ri, 8) < 4, rj // 8 == ri // 8 * 4 + lax.rem(ri, 8))
    gather = jnp.where(gather, 1.0, 0.0).astype(BF16)
    ones = jnp.ones((8, LANES), BF16)
    free = tall * occ

    def split(x):
        high = x.astype(BF16)
        return high, (x - high.astype(F32)).astype(BF16)

    def tile(t, c):
        total = jnp.zeros((width, LANES), F32)
        for ci in range(supers):
            for cj in range(ci, supers):
                block = [
                    ints[t, pl.ds((cj * groups + g) * width, width), pl.ds(ci * LANES, LANES)]
                    for g in range(groups)
                ]
                turned = []
                for r in range(groups):
                    mixed = block[r]
                    for g in range(1, groups):
                        mixed = jnp.where(part == g, block[(g + r) % groups], mixed)
                    turned.append(mixed if r == 0 else pltpu.roll(mixed, r * width, 1))
                for s in range(groups):
                    i = ci * groups + s
                    direct = ints[t, pl.ds(i * width, width), pl.ds(cj * LANES, LANES)]
                    inverse = over[t, pl.ds(i * width, width), pl.ds(cj * LANES, LANES)]
                    swapped = turned[(0 - s) % groups]
                    for g in range(1, groups):
                        swapped = jnp.where(part == g, turned[(g - s) % groups], swapped)
                    if ci == cj:
                        term = direct * (2.0 * direct - swapped) * inverse
                    else:
                        term = (direct * (direct - swapped) + swapped * swapped) * inverse
                    total = total + term
                    short = term[0:8]
                    for m in range(8, width, 8):
                        short = short + term[m:m + 8]
                    sums[i * 8:i * 8 + 8, cj * LANES:(cj + 1) * LANES] = short

        rows_of = [
            lax.dot_general(gather, x, NN, preferred_element_type=F32) for x in split(sums[...])
        ]
        pairs_of = [
            lax.dot_general(x, fold, NN, preferred_element_type=F32)
            for x in split(rows_of[0] + rows_of[1])
        ]
        by_ij = pairs_of[0] + pairs_of[1]
        packed_ij = by_ij[0:8]
        for g in range(1, tall):
            packed_ij = packed_ij + pltpu.roll(by_ij[g * 8:g * 8 + 8], g * occ, 1)
        spread = jnp.concatenate([jnp.zeros((LANES - width, LANES), F32), total], 0)
        by_row = [
            lax.dot_general(ones, x, NT, preferred_element_type=F32) for x in split(spread)
        ]
        by_row = by_row[0] + by_row[1]
        by_col = [
            lax.dot_general(ones[:, :width], x, NN, preferred_element_type=F32) for x in split(total)
        ]
        by_col = by_col[0] + by_col[1]
        folded = by_col
        for g in range(1, groups):
            folded = folded + pltpu.roll(by_col, g * width, 1)
        packed_ij = packed_ij * jnp.where(diag, 0.5, 1.0)
        both = (by_row + folded) * 0.5
        first = jnp.where(diag, jnp.where(t == 0, both, 0.0), by_row)
        second = jnp.where(diag, jnp.where(t == 1, both, 0.0), folded)
        near_turn = free - (LANES - width)
        far_turn = near_turn - width // 2
        shares = jnp.where(r8 == 3, pltpu.roll(second, far_turn % LANES, 1), 0.0)
        shares = jnp.where(r8 == 2, pltpu.roll(second, near_turn % LANES, 1), shares)
        shares = jnp.where(r8 == 1, pltpu.roll(first, far_turn % LANES, 1), shares)
        shares = jnp.where(r8 == 0, pltpu.roll(first, near_turn % LANES, 1), shares)
        shares = jnp.where(l8 < free + width // 2, shares, 0.0)
        out = jnp.where(l8 < free, packed_ij, shares)[0:4]

        @pl.when(t == 0)
        def _():
            message[...] = out

        @pl.when(t == 1)
        def _():
            message[...] += out

        return c

    lax.fori_loop(0, n_tiles, tile, 0)
    pl.semaphore_wait(news_sem.at[rounds - 1], near)

    def tell(k, c):
        t = jnp.where(v * 2 < n_virt, n - 1 - k, k)

        @pl.when(t != me)
        def _():
            pltpu.make_async_remote_copy(
                src_ref=message, dst_ref=slots.at[me],
                send_sem=msg_send, recv_sem=msg_recv,
                device_id=device(t), device_id_type=MESH,
            ).start()

        return c

    lax.fori_loop(0, n, tell, 0)
    slots[me] = message[...]
    for part_at in range(2):
        copies(own_slot, part_at, own_kids, lambda copy: copy.wait_send())

    def flush(s, c):
        @pl.when(s != own_slot)
        def _():
            for part_at in range(2):
                copies(s, part_at, pick(kids, s), lambda copy: copy.wait_send())

        return c

    lax.fori_loop(0, n_slots, flush, 0)
    everyone = slots.at[pl.ds(0, n - 1)]
    pltpu.make_async_copy(everyone, everyone, msg_send).wait()
    pltpu.make_async_copy(everyone, everyone, msg_recv).wait()

    keep = l8[0:4] < free
    upper = r8[0:4] < 2
    acc = None
    for k in range(n):
        a, b, _ = tiles[k]
        row0 = jnp.where(v == a, 1.0, 0.0)
        row1 = jnp.where(v == b, 1.0, 0.0)
        term = slots[k] * jnp.where(keep, 1.0, jnp.where(upper, row0, row1))
        acc = term if acc is None else acc + term
    done_ref[...] = acc


def table_unpack(occ, width, done_ref, share_ref, pair_ref):
    tall = -(-occ // 4)
    free = tall * occ
    done = done_ref[...]
    share = done[0:2] + done[2:4]
    share_ref[...] = jnp.concatenate(
        [share[0, free:free + width // 2], share[1, free:free + width // 2]], 0
    )
    blocks = [done] + [pltpu.roll(done, LANES - g * occ, 1) for g in range(1, tall)]
    square = jnp.concatenate(blocks + [jnp.zeros((LANES - 4 * tall, LANES), F32)], 0)
    square = jnp.where(lax.broadcasted_iota(jnp.int32, (LANES, LANES), 1) < occ, square, 0.0)
    pair = square + square.T
    pair_ref[...] = pair[0:occ, 0:occ]


def table_call(n_virt, n_aux, occ, plan, three_index, eps_occ, eps_virt):
    rows, cols = three_index.shape
    width = cols // occ
    deep = -(-rows // 16) * 16
    n = n_virt * n_aux
    n_slots = 2 * n_aux
    vmem = pl.BlockSpec(memory_space=pltpu.VMEM)
    hbm = pl.BlockSpec(memory_space=pltpu.HBM)
    done = pl.pallas_call(
        functools.partial(table_kernel, n_virt, n_aux, occ, plan),
        out_shape=pltpu.VMEM((4, LANES), F32),
        in_specs=[hbm, hbm, hbm],
        out_specs=vmem,
        scratch_shapes=[
            pltpu.VMEM((rows, cols), BF16),
            pltpu.VMEM((n_slots + 1, deep, cols), BF16),
            pltpu.VMEM((cols, cols), BF16),
            pltpu.VMEM((2, cols, cols), F32),
            pltpu.VMEM((2, cols, cols), F32),
            pltpu.VMEM((occ * 8, cols), F32),
            pltpu.VMEM((4, LANES), F32),
            pltpu.VMEM((n, 4, LANES), F32),
            pltpu.SMEM(eps_occ.shape, F32),
            pltpu.SMEM(eps_virt.shape, F32),
            pltpu.SemaphoreType.DMA,
            pltpu.SemaphoreType.DMA((2,)),
            pltpu.SemaphoreType.DMA((n_slots + 1, 2, KIDS)),
            pltpu.SemaphoreType.DMA((n_slots, 2)),
            pltpu.SemaphoreType.DMA,
            pltpu.SemaphoreType.DMA,
            pltpu.SemaphoreType.REGULAR((len(plan[5][0]) + 1,)),
        ],
        compiler_params=pltpu.CompilerParams(collective_id=0, has_side_effects=True),
    )(three_index, eps_occ, eps_virt)
    return pl.pallas_call(
        functools.partial(table_unpack, occ, width),
        out_shape=(
            jax.ShapeDtypeStruct((width,), F32),
            jax.ShapeDtypeStruct((occ, occ), F32),
        ),
        in_specs=[vmem],
        out_specs=(vmem, vmem),
    )(pltpu.with_memory_space_constraint(done, pltpu.VMEM))


def unpack(occ, width, done_ref, share_ref, pair_ref):
    tall = -(-occ // 8)
    free = tall * width
    done = done_ref[...]
    share = done[0:1] + done[1:2]
    share_ref[...] = share[0, free:free + width]
    blocks = [done] + [pltpu.roll(done, LANES - g * width, 1) for g in range(1, tall)]
    square = jnp.concatenate(blocks + [jnp.zeros((LANES - 8 * tall, LANES), F32)], 0)
    square = jnp.where(lax.broadcasted_iota(jnp.int32, (LANES, LANES), 1) < occ, square, 0.0)
    pair = square + square.T
    pair_ref[...] = pair[0:occ, 0:occ]


def on_device(n_virt, n_aux, three_index, eps_occ, eps_virt):
    occ = eps_occ.shape[0]
    rows, cols = three_index.shape
    width = cols // occ
    pitch = -(-rows // 16) * 16
    n = n_virt * n_aux
    vmem = pl.BlockSpec(memory_space=pltpu.VMEM)
    smem = pl.BlockSpec(memory_space=pltpu.SMEM)
    plan = PLANS.get((n_virt, n_aux))
    if plan is not None:
        return table_call(n_virt, n_aux, occ, plan, three_index, eps_occ, eps_virt)
    done = pl.pallas_call(
        functools.partial(kernel, n_virt, n_aux, occ),
        out_shape=jax.ShapeDtypeStruct((8, LANES), F32),
        in_specs=[vmem, smem, smem],
        out_specs=vmem,
        scratch_shapes=[
            pltpu.VMEM((2, n_aux, rows, cols), BF16),
            pltpu.VMEM((cols, n_aux * pitch), BF16),
            pltpu.VMEM((n_aux * pitch, cols), BF16),
            pltpu.VMEM((cols, cols), BF16),
            pltpu.VMEM((cols, cols), BF16),
            pltpu.VMEM((cols, cols), F32),
            pltpu.VMEM((occ * 8, cols), F32),
            pltpu.VMEM((8, LANES), F32),
            pltpu.VMEM((8, LANES), F32),
            pltpu.VMEM((n, 8, LANES), F32),
            pltpu.SemaphoreType.DMA,
            pltpu.SemaphoreType.DMA((3, n_aux)),
            pltpu.SemaphoreType.DMA((2, n_aux)),
            pltpu.SemaphoreType.DMA,
            pltpu.SemaphoreType.DMA,
        ],
        compiler_params=pltpu.CompilerParams(collective_id=0, has_side_effects=True),
    )(three_index, eps_occ, eps_virt)
    return pl.pallas_call(
        functools.partial(unpack, occ, width),
        out_shape=(
            jax.ShapeDtypeStruct((width,), F32),
            jax.ShapeDtypeStruct((occ, occ), F32),
        ),
        in_specs=[vmem],
        out_specs=(vmem, vmem),
    )(done)


def solution(mesh):
    n_virt, n_aux = mesh.shape["virt"], mesh.shape["aux"]
    assert n_virt == 2 * n_aux and n_aux % 2 == 0
    in_specs = (P("aux", "virt"), P(), P())
    out_specs = (P("virt"), P())
    return jax.shard_map(
        functools.partial(on_device, n_virt, n_aux), mesh=mesh,
        in_specs=in_specs, out_specs=out_specs, check_vma=False,
    )
```

```python
import functools

import jax
import jax.numpy as jnp
from jax import lax
from jax.experimental import pallas as pl
from jax.experimental.pallas import tpu as pltpu
from jax.sharding import PartitionSpec as P

MESH = pl.DeviceIdType.MESH
F32 = jnp.float32
BF16 = jnp.bfloat16
EXACT = lax.Precision.HIGHEST
LANES = 128
NT = (((1,), (1,)), ((), ()))
NN = (((1,), (0,)), ((), ()))


def distances(n_aux):
    return list(range(1, n_aux + 1, 2)) + list(range(2, n_aux + 1, 2))


def pick(table, at):
    got = table[0] + jnp.int32(0)
    for k in range(1, len(table)):
        got = jnp.where(at == k, table[k] + jnp.int32(0), got)
    return got


def label_of(virt, n_virt):
    return lax.rem(virt, 2) * (n_virt // 2) + virt // 2


def virt_of(label, n_virt):
    half = n_virt // 2
    return lax.rem(label, half) * 2 + label // half


def kernel(
    n_virt, n_aux, occ,
    x_ref, occ_ref, virt_ref,
    done_ref,
    held, lhs, rhs, order, order_t, ints, sums, parts, message, slots,
    own_sem, send_sem, recv_sem, msg_send, msg_recv,
):
    rows, cols = x_ref.shape
    pitch = -(-rows // 16) * 16
    width = cols // occ
    groups = LANES // width
    supers = occ // groups
    n = n_virt * n_aux
    v = lax.axis_index("virt")
    p = lax.axis_index("aux")
    me = v * n_aux + p
    table = distances(n_aux)
    label = label_of(v, n_virt)
    other = virt_of(lax.rem(label + pick(table, p), n_virt), n_virt)
    lower = label < n_virt // 2
    solo = jnp.logical_and(p == n_aux - 1, jnp.logical_not(lower))
    extra = jnp.logical_and(p == n_aux // 2 - 1, lower)

    barrier = pltpu.get_barrier_semaphore()

    def greet(k, c):
        t = lax.rem(me + k, n)
        pl.semaphore_signal(
            barrier, inc=1,
            device_id={"virt": t // n_aux, "aux": lax.rem(t, n_aux)},
            device_id_type=MESH,
        )
        return c

    lax.fori_loop(1, n, greet, 0)
    own = pltpu.make_async_copy(x_ref, held.at[0, p], own_sem)
    own.start()
    pl.semaphore_wait(barrier, n - 1)

    pairs = n_aux // 2

    def place(k):
        return lax.rem(p // 2 + k // 2, pairs) * 2 + lax.rem(p + k, 2)

    def share_own(k):
        return pltpu.make_async_remote_copy(
            src_ref=x_ref, dst_ref=held.at[0, p],
            send_sem=send_sem.at[0, k], recv_sem=recv_sem.at[0, p],
            device_id={"virt": v, "aux": place(k)}, device_id_type=MESH,
        )

    def hand_on(k):
        q = place(k)
        return pltpu.make_async_remote_copy(
            src_ref=held.at[0, q], dst_ref=held.at[0, q],
            send_sem=send_sem.at[2, k], recv_sem=recv_sem.at[0, q],
            device_id={"virt": v, "aux": place(1)}, device_id_type=MESH,
        )

    def share_other(k):
        q = place(k)
        target = lax.rem(label + n_virt - pick(table, q), n_virt)
        copy = pltpu.make_async_remote_copy(
            src_ref=x_ref, dst_ref=held.at[1, p],
            send_sem=send_sem.at[1, k], recv_sem=recv_sem.at[1, p],
            device_id={"virt": virt_of(target, n_virt), "aux": q}, device_id_type=MESH,
        )
        wanted = jnp.logical_or(q < n_aux - 1, target < n_virt // 2)
        return copy, wanted

    for k in list(range(2, n_aux, 2)) + [1]:
        share_own(k).start()
    for k in range(n_aux):
        copy, wanted = share_other(k)
        pl.when(wanted)(copy.start)

    def arrived(side, q):
        pltpu.make_async_copy(
            held.at[side, q], held.at[side, q], recv_sem.at[side, q]
        ).wait()

    row = lax.broadcasted_iota(jnp.int32, (cols, cols), 0)
    col = lax.broadcasted_iota(jnp.int32, (cols, cols), 1)
    hit = col == lax.rem(row, width) * occ + row // width
    order[...] = jnp.where(hit, 1.0, 0.0).astype(BF16)
    hit = row == lax.rem(col, width) * occ + col // width
    order_t[...] = jnp.where(hit, 1.0, 0.0).astype(BF16)
    lhs[...] = jnp.zeros_like(lhs)
    rhs[...] = jnp.zeros_like(rhs)

    def turn(k):
        lhs[:, k * pitch:k * pitch + rows] = lax.dot_general(
            order[...], held[0, place(k)], NT, preferred_element_type=F32
        ).astype(BF16)

    own.wait()
    turn(0)
    for k in range(2, n_aux, 2):
        arrived(0, place(k))
        hand_on(k).start()
        turn(k)
    for k in range(1, n_aux, 2):
        arrived(0, place(k))
        turn(k)

    lane = lax.broadcasted_iota(jnp.int32, (1, LANES), 1)
    part = lane // width
    down = lax.broadcasted_iota(jnp.int32, (width, 1), 0)
    lane_in = lax.rem(lane, width)

    def eps_down(which):
        got = jnp.zeros((width, 1), F32)
        for k in range(width):
            got = jnp.where(down == k, virt_ref[which * width + k], got)
        return got

    def eps_across(which):
        got = jnp.zeros((1, LANES), F32)
        for k in range(width):
            got = jnp.where(lane_in == k, virt_ref[which * width + k], got)
        return got

    occ_lane = []
    for cj in range(supers):
        got = jnp.zeros((1, LANES), F32)
        for t in range(groups):
            got = jnp.where(part == t, occ_ref[cj * groups + t], got)
        occ_lane.append(got)

    tall = -(-occ // 8)
    sums[...] = jnp.zeros_like(sums)
    n_tiles = jnp.where(extra, 2, 1)
    r8 = lax.broadcasted_iota(jnp.int32, (8, LANES), 0)
    l8 = lax.broadcasted_iota(jnp.int32, (8, LANES), 1)
    free = tall * width

    def tile(t, c):
        diag = jnp.logical_or(solo, jnp.logical_and(extra, t == 0))
        source = jnp.where(diag, 0, 1)

        for k in range(n_aux):

            @pl.when(source == 1)
            def _():
                arrived(1, place(k))

            rhs[k * pitch:k * pitch + rows, :] = lax.dot_general(
                held[source, place(k)], order_t[...], NN, preferred_element_type=F32
            ).astype(BF16)
        ints[...] = lax.dot_general(lhs[...], rhs[...], NN, preferred_element_type=F32)

        base = -(eps_down(v) + eps_across(jnp.where(diag, v, other)))
        total = jnp.zeros((width, LANES), F32)
        for ci in range(supers):
            for cj in range(ci, supers):
                turned = []
                for g in range(groups):
                    block = ints[pl.ds((cj * groups + g) * width, width), pl.ds(ci * LANES, LANES)]
                    turned.append([block if r == 0 else pltpu.roll(block, r * width, 1) for r in range(groups)])
                for s in range(groups):
                    i = ci * groups + s
                    direct = ints[pl.ds(i * width, width), pl.ds(cj * LANES, LANES)]
                    swapped = turned[0][(0 - s) % groups]
                    for g in range(1, groups):
                        swapped = jnp.where(part == g, turned[g][(g - s) % groups], swapped)
                    below = base + (occ_lane[cj] + occ_ref[i])
                    if ci == cj:
                        term = direct * (2.0 * direct - swapped) / below
                    else:
                        term = 2.0 * (direct * (direct - swapped) + swapped * swapped) / below
                    total = total + term
                    short = term[0:8]
                    for m in range(8, width, 8):
                        short = short + term[m:m + 8]
                    sums[i * 8:i * 8 + 8, cj * LANES:(cj + 1) * LANES] = short

        wide = lax.broadcasted_iota(jnp.int32, (cols, LANES), 0)
        thin = lax.broadcasted_iota(jnp.int32, (cols, LANES), 1)
        fold = jnp.where(wide // width == thin, 1.0, 0.0)
        by_j = lax.dot_general(sums[...], fold, NN, precision=EXACT, preferred_element_type=F32)
        ri = lax.broadcasted_iota(jnp.int32, (tall * 8, occ * 8), 0)
        rj = lax.broadcasted_iota(jnp.int32, (tall * 8, occ * 8), 1)
        by_ij = lax.dot_general(
            jnp.where(rj // 8 == ri, 1.0, 0.0), by_j, NN,
            precision=EXACT, preferred_element_type=F32,
        )
        packed = by_ij[0:8]
        for g in range(1, tall):
            packed = packed + pltpu.roll(by_ij[g * 8:g * 8 + 8], g * width, 1)
        pads = [jnp.zeros((free, LANES), F32), total]
        if free + width < LANES:
            pads.append(jnp.zeros((LANES - free - width, LANES), F32))
        spread = jnp.concatenate(pads, 0)
        by_row = lax.dot_general(
            jnp.ones((8, LANES), F32), spread, NT, precision=EXACT, preferred_element_type=F32)
        by_col = lax.dot_general(
            jnp.ones((8, width), F32), total, NN, precision=EXACT, preferred_element_type=F32)
        folded = by_col
        for g in range(1, groups):
            folded = folded + pltpu.roll(by_col, g * width, 1)
        packed = packed * jnp.where(diag, 0.5, 1.0)
        first = jnp.where(diag, (by_row + folded) * 0.5, by_row)
        second = jnp.where(diag, 0.0, folded)
        out = jnp.where(l8 < free, packed, jnp.where(r8 == 0, first, jnp.where(r8 == 1, second, 0.0)))

        @pl.when(t == 0)
        def _():
            message[...] = out

        @pl.when(t == 1)
        def _():
            message[...] += out

        return c

    lax.fori_loop(0, n_tiles, tile, 0)

    def tell(k, c):
        t = lax.rem(me + k, n)
        pltpu.make_async_remote_copy(
            src_ref=message, dst_ref=slots.at[me],
            send_sem=msg_send, recv_sem=msg_recv,
            device_id={"virt": t // n_aux, "aux": lax.rem(t, n_aux)},
            device_id_type=MESH,
        ).start()
        return c

    lax.fori_loop(1, n, tell, 0)
    slots[me] = message[...]
    for k in list(range(2, n_aux, 2)) + [1]:
        share_own(k).wait_send()
    for k in range(2, n_aux, 2):
        hand_on(k).wait_send()
    for k in range(n_aux):
        copy, wanted = share_other(k)
        pl.when(wanted)(copy.wait_send)
    everyone = slots.at[pl.ds(0, n - 1)]
    pltpu.make_async_copy(everyone, everyone, msg_send).wait()
    pltpu.make_async_copy(everyone, everyone, msg_recv).wait()

    keep = jnp.logical_or(l8 < free, r8 < 0)

    def add(k, acc):
        sv = k // n_aux
        so = virt_of(lax.rem(label_of(sv, n_virt) + pick(table, lax.rem(k, n_aux)), n_virt), n_virt)
        row0 = jnp.where(sv == v, 1.0, 0.0)
        row1 = jnp.where(so == v, 1.0, 0.0)
        weight = jnp.where(keep, 1.0, jnp.where(r8 == 0, row0, row1))
        return acc + slots[k] * weight

    done = lax.fori_loop(0, n, add, jnp.zeros((8, LANES), F32))
    done_ref[...] = done


TILES = (
    (0, 2, 1),
    (0, 2, 0),
    (0, 1, 0),
    (1, 2, 0),
    (1, 3, 1),
    (0, 3, 0),
    (1, 3, 0),
    (2, 3, 0),
    (0, 4, 0),
    (0, 5, 0),
    (2, 4, 0),
    (2, 5, 0),
    (1, 4, 0),
    (3, 4, 0),
    (1, 5, 0),
    (3, 5, 0),
    (0, 6, 0),
    (0, 7, 0),
    (2, 6, 0),
    (2, 7, 0),
    (1, 6, 0),
    (1, 7, 0),
    (3, 6, 0),
    (3, 7, 0),
    (6, 7, 0),
    (6, 4, 0),
    (7, 4, 0),
    (6, 4, 1),
    (6, 5, 0),
    (7, 5, 1),
    (4, 5, 0),
    (7, 5, 0),
)
ROUTES = (
    ((2, 10, 18), (4, 10, 32), (2,), (16,), (3,), (3,), (), (3,), ()),
    ((4,), (0,), (10, 18), (10,), (), (7,), (1,), (), ()),
    ((), (), (0,), (2,), (), (), (6,), (6,), ()),
    ((5,), (), (), (), (14,), (14, 20), (14, 3), (1, 14), (4, 18)),
    ((12, 24), (12, 24), (24,), (), (11,), (15,), (), (26,), ()),
    ((), (), (), (), (15,), (9,), (9,), (), (5, 8)),
    ((6,), (6, 28), (5, 8, 28), (5, 8, 28), (), (), (15,), (15, 9, 11), ()),
    ((), (), (), (), (13,), (13,), (), (), (12, 40)),
    ((), (), (), (), (21, 27), (), (), (27,), (1, 22)),
    ((16, 32), (16,), (16, 34), (0, 32), (23,), (), (), (), (1, 38)),
    ((), (), (22, 38), (38,), (), (), (17, 25, 51), (), ()),
    ((20, 36, 7), (), (7,), (7, 20), (), (19,), (19,), (19, 29), ()),
    ((28, 42), (42,), (40,), (), (), (27,), (27,), (), (26,)),
    ((9, 46), (11, 44), (11,), (), (25,), (17, 21), (), (25,), ()),
    ((), (), (), (), (), (31, 61, 23), (23, 31), (31,), (26, 30)),
    ((), (), (13, 44), (13, 44), (29,), (), (), (), ()),
    ((34,), (18, 34), (), (34,), (), (37,), (), (41,), (17, 51)),
    ((), (), (32,), (), (), (43,), (), (), (25, 51, 60)),
    ((38,), (22,), (), (), (33,), (45,), (33, 45), (33, 45), (21, 60, 55)),
    ((), (36,), (36,), (36,), (), (), (), (), (17, 53)),
    ((), (), (42,), (42, 24), (45, 56), (), (), (), (19, 59, 31, 57)),
    ((40,), (40,), (), (), (35, 47), (), (), (), (29, 57)),
    ((), (46,), (46,), (46,), (), (), (41,), (), (29, 63)),
    ((44, 30), (30,), (), (), (), (), (39, 43), (39, 43), (23, 61)),
    ((50, 54), (54,), (), (50,), (), (35, 39), (), (), ()),
    ((41,), (33, 48, 56), (48, 56), (56,), (55,), (53,), (), (), ()),
    ((), (), (), (), (), (55,), (), (55, 60, 51), (50, 54)),
    ((37,), (), (37,), (37, 48), (53, 60), (), (), (21,), ()),
    ((), (41,), (), (), (), (59,), (), (), (43, 49, 58)),
    ((62,), (49, 62), (49, 35), (35, 49), (63,), (), (57,), (57,), ()),
    ((), (), (53,), (), (), (63,), (), (63,), (62,)),
    ((39, 52), (47, 52), (47, 52, 58), (47, 52, 58), (61,), (), (61, 59), (59,), ()),
)
STEPS = (
    (0, 17, 2, 19, 4, 10, 21, 8, 27, 25, 14, 6, 31, 23, 12, 29),
    (2, 3, 0, 1, 4, 10, 8, 5, 6, 27, 7, 25, 14, 12, 31, 29),
    (4, 5, 6, 7, 12, 10, 29, 14, 0, 2, 31, 11, 8, 1, 19, 25),
    (14, 15, 4, 12, 5, 29, 6, 8, 0, 23, 9, 17, 10, 2, 11, 19),
    (0, 17, 2, 19, 4, 10, 21, 27, 8, 6, 25, 23, 14, 12, 29, 31),
    (10, 0, 11, 1, 2, 19, 8, 12, 4, 25, 13, 21, 14, 6, 15, 23),
    (4, 5, 6, 7, 14, 0, 31, 1, 12, 2, 29, 3, 10, 27, 8, 25),
    (14, 15, 6, 12, 23, 13, 10, 4, 11, 21, 8, 0, 9, 17, 2, 19),
    (0, 8, 14, 1, 25, 15, 12, 4, 10, 5, 2, 29, 6, 11, 19, 23),
    (0, 1, 6, 8, 7, 4, 14, 25, 5, 2, 31, 12, 3, 10, 29, 27),
    (4, 5, 6, 7, 0, 12, 1, 29, 8, 25, 14, 10, 31, 2, 3, 27),
    (6, 7, 4, 5, 0, 1, 14, 31, 12, 2, 8, 10, 3, 29, 27, 25),
    (0, 1, 10, 2, 3, 27, 4, 8, 5, 12, 14, 25, 6, 29, 15, 23),
    (2, 3, 0, 1, 4, 5, 10, 8, 27, 14, 25, 12, 6, 15, 29, 23),
    (4, 12, 10, 5, 29, 11, 0, 6, 14, 8, 7, 1, 2, 31, 19, 25),
    (6, 7, 4, 5, 12, 10, 8, 29, 2, 11, 0, 14, 19, 9, 17, 31),
    (10, 11, 2, 14, 0, 15, 1, 19, 12, 6, 13, 23, 8, 25, 4, 21),
    (8, 2, 14, 10, 0, 9, 17, 3, 15, 27, 6, 12, 4, 23, 13, 21),
    (14, 4, 15, 2, 5, 12, 3, 6, 29, 10, 0, 8, 27, 23, 9, 17),
    (4, 2, 5, 3, 6, 14, 15, 23, 12, 0, 10, 29, 1, 8, 27, 25),
    (6, 8, 9, 10, 7, 0, 17, 11, 14, 2, 19, 4, 12, 31, 5, 29),
    (8, 9, 14, 6, 0, 15, 17, 12, 23, 2, 13, 3, 10, 27, 4, 21),
    (2, 6, 3, 7, 14, 0, 31, 4, 12, 1, 5, 8, 29, 25, 10, 27),
    (14, 15, 2, 6, 12, 0, 3, 13, 8, 23, 10, 1, 25, 27, 4, 21),
    (0, 1, 2, 3, 6, 10, 8, 4, 7, 27, 25, 14, 5, 31, 12, 29),
    (2, 3, 0, 1, 10, 8, 4, 6, 25, 5, 27, 7, 14, 31, 12, 29),
    (6, 14, 7, 4, 31, 5, 10, 2, 12, 8, 3, 9, 0, 27, 17, 29),
    (6, 23, 4, 21, 0, 17, 14, 2, 12, 19, 31, 8, 10, 25, 29, 27),
    (2, 10, 3, 27, 8, 4, 9, 12, 6, 0, 14, 13, 21, 17, 15, 23),
    (2, 19, 0, 17, 6, 8, 23, 10, 4, 21, 27, 25, 12, 14, 29, 31),
    (14, 4, 12, 15, 13, 2, 6, 21, 23, 10, 8, 3, 27, 0, 9, 17),
    (6, 7, 4, 5, 2, 12, 3, 14, 29, 0, 31, 1, 8, 25, 10, 27),
)
PARTNERS = (
    (1, 2, 4, 8, 3, 5, 9, 16),
    (0, 3, 5, 9, 2),
    (3, 0, 6, 10, 1, 5),
    (2, 1, 7, 11, 0, 6, 9, 10),
    (5, 6, 0, 12, 7, 13),
    (4, 7, 1, 13, 0, 2, 6),
    (7, 4, 2, 14, 3, 5, 15),
    (6, 5, 3, 15, 4, 20),
    (9, 10, 12, 0, 16, 11, 13, 19),
    (8, 11, 13, 1, 17, 0, 3, 16, 19, 20),
    (11, 8, 14, 2, 18, 3, 12, 13, 19, 25, 27),
    (10, 9, 15, 3, 19, 8, 14, 18, 23),
    (13, 14, 8, 4, 20, 10, 17, 21),
    (12, 15, 9, 5, 21, 4, 8, 10, 14, 22, 23),
    (15, 12, 10, 6, 22, 11, 13, 21, 30),
    (14, 13, 11, 7, 23, 6, 20, 22),
    (17, 18, 20, 8, 24, 0, 9, 25),
    (16, 19, 21, 9, 25, 12, 24, 29, 30),
    (19, 16, 22, 10, 26, 11, 27, 30),
    (18, 17, 23, 11, 27, 8, 9, 10, 24, 26, 31),
    (21, 22, 16, 12, 28, 7, 9, 15, 25, 29),
    (20, 23, 17, 13, 29, 12, 14, 28),
    (23, 20, 18, 14, 30, 13, 15, 31),
    (22, 21, 19, 15, 31, 11, 13, 30),
    (25, 26, 28, 16, 17, 19, 27, 29),
    (24, 27, 29, 17, 10, 16, 20, 26, 28),
    (27, 24, 30, 18, 19, 25, 31),
    (26, 25, 31, 19, 10, 18, 24, 30),
    (29, 30, 24, 20, 21, 25),
    (28, 31, 25, 21, 17, 20, 24),
    (31, 28, 26, 22, 14, 17, 18, 23, 27),
    (30, 29, 27, 23, 19, 22, 26),
)
NEAR = (4, 4, 4, 4, 4, 4, 4, 4, 5, 5, 5, 5, 5, 5, 5, 5, 5, 5, 5, 5, 5, 5, 5, 5, 4, 4, 4, 4, 4, 4, 4, 4)
NEWS = (
    (8, 12, 15),
    (5, 11, 15),
    (7, 12, 15),
    (3, 10, 15),
    (7, 13, 15),
    (4, 10, 15),
    (8, 12, 15),
    (1, 8, 13),
    (3, 6, 12),
    (4, 6, 11),
    (6, 8, 11),
    (7, 10, 15),
    (3, 7, 13),
    (6, 8, 14),
    (3, 8, 15),
    (4, 9, 15),
    (2, 6, 13),
    (0, 4, 11),
    (4, 13, 15),
    (4, 8, 13),
    (0, 5, 10),
    (2, 6, 12),
    (3, 8, 15),
    (3, 12, 15),
    (7, 12, 15),
    (7, 13, 14),
    (3, 7, 14),
    (6, 11, 15),
    (3, 6, 14),
    (7, 13, 15),
    (1, 6, 11),
    (7, 12, 14),
)
PLANS = {(8, 4): (TILES, ROUTES, STEPS, PARTNERS, NEAR, NEWS)}


TN = (((0,), (0,)), ((), ()))
KIDS = 4
CODE = 128


def table_kernel(
    n_virt, n_aux, occ, plan,
    x_ref, occ_hbm, virt_hbm,
    done_ref,
    raw, held, order, ints, over, sums, message, slots, weigh, occ_ref, virt_ref,
    own_sem, eps_sem, send_sem, recv_sem, msg_send, msg_recv, news_sem,
):
    rows, cols = x_ref.shape
    deep = held.shape[1]
    width = cols // occ
    groups = LANES // width
    supers = occ // groups
    n = n_virt * n_aux
    v = lax.axis_index("virt")
    p = lax.axis_index("aux")
    me = v * n_aux + p
    tiles, routes, steps, partners, n_near, news = plan
    rounds = len(news[0]) + 1
    half = -(-rows // 32) * 16
    cuts = ((0, half), (half, -(-rows // 8) * 8 - half))
    n_slots = 2 * n_aux

    def device(t):
        return {"virt": lax.div(t, n_aux), "aux": lax.rem(t, n_aux)}

    barrier = pltpu.get_barrier_semaphore()

    side_a = pick([t[0] for t in tiles], me)
    side_b = pick([t[1] for t in tiles], me)
    diag = pick([t[2] for t in tiles], me) == 1
    own_slot = jnp.where(side_a == v, p, jnp.where(side_b == v, n_aux + p, n_slots))
    owns = []
    for d, (a, b, _) in enumerate(tiles):
        q = d % n_aux
        owns.append(q if a == d // n_aux else n_aux + q if b == d // n_aux else n_slots)
    own = pltpu.make_async_copy(x_ref, raw, own_sem)
    own.start()
    eps = (
        pltpu.make_async_copy(occ_hbm, occ_ref, eps_sem.at[0]),
        pltpu.make_async_copy(virt_hbm, virt_ref, eps_sem.at[1]),
    )
    for copy in eps:
        copy.start()

    def packed(codes):
        got = 0
        for c in reversed(codes):
            got = got * CODE + c + 1
        return got

    most = max(len(r) for r in partners)
    folk = [
        pick([packed(r[at:at + KIDS]) for r in partners], me) for at in range(0, most, KIDS)
    ]
    n_folk = pick([len(r) for r in partners], me)
    near = pick(n_near, me)

    def signal(sem, amount, limit):
        code = None
        for k in range(amount):
            code = folk[k // KIDS] if k % KIDS == 0 else lax.div(code, CODE)

            @pl.when(k < limit)
            def _():
                t = lax.rem(code, CODE) - 1
                pl.semaphore_signal(sem, inc=1, device_id=device(t), device_id_type=MESH)

    if deep > rows:
        held[:, rows:, :] = jnp.zeros((n_slots + 1, deep - rows, cols), BF16)
    signal(barrier, most, n_folk)

    row = lax.broadcasted_iota(jnp.int32, (cols, cols), 0)
    col = lax.broadcasted_iota(jnp.int32, (cols, cols), 1)
    hit = row == lax.rem(col, width) * occ + col // width
    order[...] = jnp.where(hit, 1.0, 0.0).astype(BF16)
    own.wait()
    held[own_slot, 0:rows, :] = lax.dot_general(
        raw[...], order[...], NN, preferred_element_type=F32
    ).astype(BF16)
    pl.semaphore_wait(barrier, n_folk)

    own_kids = pick([packed(r[o]) for r, o in zip(routes, owns)], me)

    def piece(slot, part):
        return held.at[slot, pl.ds(cuts[part][0], cuts[part][1])]

    def decode(slot, code):
        q = jnp.where(slot == n_slots, p, lax.rem(slot, n_aux))
        found = []
        for k in range(KIDS):
            this = lax.rem(code, CODE)
            code = lax.div(code, CODE)
            t = jnp.maximum(this - 1, 0)
            found.append((this > 0, lax.div(t, 2), lax.rem(t, 2) * n_aux + q))
        return found

    def copies(slot, part, found, act):
        for there, t, to in found:

            @pl.when(there)
            def _():
                act(pltpu.make_async_remote_copy(
                    src_ref=piece(slot, part), dst_ref=piece(to, part),
                    send_sem=send_sem.at[slot], recv_sem=recv_sem.at[to, part],
                    device_id=device(t), device_id_type=MESH,
                ))

    own_found = decode(own_slot, own_kids)
    for part in range(2):
        copies(own_slot, part, own_found, lambda copy: copy.start())
    close = max(n_near)
    signal(news_sem.at[0], close, near)
    kids = [pick([packed(r[s]) for r in routes], me) for s in range(n_slots + 1)]
    spread_at = [pick([r[k] for r in news], me) for k in range(rounds - 1)]
    todo = [pick([r[i] for r in steps], me) for i in range(2 * n_slots)]
    for copy in eps:
        copy.wait()

    lane = lax.broadcasted_iota(jnp.int32, (1, LANES), 1)
    part = lane // width
    down = lax.broadcasted_iota(jnp.int32, (width, 1), 0)
    lane_in = lax.rem(lane, width)
    n_tiles = jnp.where(diag, 2, 1)

    def eps_down(which):
        got = jnp.zeros((width, 1), F32)
        for k in range(width):
            got = jnp.where(down == k, virt_ref[which * width + k], got)
        return got

    def eps_across(which):
        got = jnp.zeros((1, LANES), F32)
        for k in range(width):
            got = jnp.where(lane_in == k, virt_ref[which * width + k], got)
        return got

    occ_lane = []
    for cj in range(supers):
        got = jnp.zeros((1, LANES), F32)
        for t in range(groups):
            got = jnp.where(part == t, occ_ref[cj * groups + t], got)
        occ_lane.append(got)

    def prepare(t, c):
        block_l = jnp.where(t == 0, side_a, side_b)
        block_r = jnp.where(jnp.logical_and(diag, t == 0), side_a, side_b)
        base = -(eps_down(block_l) + eps_across(block_r))
        ints[t] = jnp.zeros((cols, cols), F32)
        for i in range(occ):
            for cj in range(i // groups, supers):
                below = base + (occ_lane[cj] + occ_ref[i])
                over[t, i * width:(i + 1) * width, cj * LANES:(cj + 1) * LANES] = (
                    (1.0 if cj == i // groups else 2.0) / below
                )
        return c

    lax.fori_loop(0, n_tiles, prepare, 0)

    keep = lax.broadcasted_iota(jnp.int32, (4, LANES), 1) < -(-occ // 4) * occ
    upper = lax.broadcasted_iota(jnp.int32, (4, LANES), 0) < 2
    for k in range(n):
        row0 = jnp.where(v == tiles[k][0], 1.0, 0.0)
        row1 = jnp.where(v == tiles[k][1], 1.0, 0.0)
        weigh[k] = jnp.where(keep, 1.0, jnp.where(upper, row0, row1))

    def take(i, c):
        for r in range(1, rounds):

            @pl.when(i == spread_at[r - 1])
            def _():
                pl.semaphore_wait(news_sem.at[r - 1], near)
                signal(news_sem.at[r], close, near)

        entry = pick(todo, i)
        slot = lax.rem(lax.div(entry, 2), n_slots)
        meets = lax.div(entry, 4 * n_aux) == 1
        later = lax.rem(entry, 2)
        away = slot != own_slot
        found = decode(slot, pick(kids, slot))
        for part in range(2):

            @pl.when(jnp.logical_and(later == part, away))
            def _():
                whole = piece(slot, part)
                pltpu.make_async_copy(whole, whole, recv_sem.at[slot, part]).wait()
                copies(slot, part, found, lambda copy: copy.start())

        side = lax.div(slot, n_aux)
        mine = jnp.where(diag, side, 0)
        left = jnp.where(diag, slot, lax.rem(slot, n_aux))
        right = jnp.where(diag, slot, n_aux + lax.rem(slot, n_aux))

        @pl.when(meets)
        def _():
            ints[mine] += lax.dot_general(held[left], held[right], TN, preferred_element_type=F32)

        return c

    lax.fori_loop(0, 2 * n_slots, take, 0)

    tall = -(-occ // 4)
    sums[...] = jnp.zeros_like(sums)
    r8 = lax.broadcasted_iota(jnp.int32, (8, LANES), 0)
    l8 = lax.broadcasted_iota(jnp.int32, (8, LANES), 1)
    wide = lax.broadcasted_iota(jnp.int32, (cols, LANES), 0)
    thin = lax.broadcasted_iota(jnp.int32, (cols, LANES), 1)
    fold = jnp.where(wide // width == thin, 1.0, 0.0).astype(BF16)
    ri = lax.broadcasted_iota(jnp.int32, (tall * 8, occ * 8), 0)
    rj = lax.broadcasted_iota(jnp.int32, (tall * 8, occ * 8), 1)
    gather = jnp.logical_and(lax.rem(ri, 8) < 4, rj // 8 == ri // 8 * 4 + lax.rem(ri, 8))
    gather = jnp.where(gather, 1.0, 0.0).astype(BF16)
    ones = jnp.ones((8, LANES), BF16)
    free = tall * occ

    def split(x):
        high = x.astype(BF16)
        return high, (x - high.astype(F32)).astype(BF16)

    def tile(t, c):
        total = jnp.zeros((width, LANES), F32)
        for ci in range(supers):
            for cj in range(ci, supers):
                block = [
                    ints[t, pl.ds((cj * groups + g) * width, width), pl.ds(ci * LANES, LANES)]
                    for g in range(groups)
                ]
                turned = []
                for r in range(groups):
                    mixed = block[r]
                    for g in range(1, groups):
                        mixed = jnp.where(part == g, block[(g + r) % groups], mixed)
                    turned.append(mixed if r == 0 else pltpu.roll(mixed, r * width, 1))
                for s in range(groups):
                    i = ci * groups + s
                    direct = ints[t, pl.ds(i * width, width), pl.ds(cj * LANES, LANES)]
                    inverse = over[t, pl.ds(i * width, width), pl.ds(cj * LANES, LANES)]
                    swapped = turned[(0 - s) % groups]
                    for g in range(1, groups):
                        swapped = jnp.where(part == g, turned[(g - s) % groups], swapped)
                    if ci == cj:
                        term = direct * (2.0 * direct - swapped) * inverse
                    else:
                        term = (direct * (direct - swapped) + swapped * swapped) * inverse
                    total = total + term
                    short = term[0:8]
                    for m in range(8, width, 8):
                        short = short + term[m:m + 8]
                    sums[i * 8:i * 8 + 8, cj * LANES:(cj + 1) * LANES] = short

        rows_of = [
            lax.dot_general(gather, x, NN, preferred_element_type=F32) for x in split(sums[...])
        ]
        pairs_of = [
            lax.dot_general(x, fold, NN, preferred_element_type=F32)
            for x in split(rows_of[0] + rows_of[1])
        ]
        by_ij = pairs_of[0] + pairs_of[1]
        packed_ij = by_ij[0:8]
        for g in range(1, tall):
            packed_ij = packed_ij + pltpu.roll(by_ij[g * 8:g * 8 + 8], g * occ, 1)
        spread = jnp.concatenate([jnp.zeros((LANES - width, LANES), F32), total], 0)
        by_row = [
            lax.dot_general(ones, x, NT, preferred_element_type=F32) for x in split(spread)
        ]
        by_row = by_row[0] + by_row[1]
        by_col = [
            lax.dot_general(ones[:, :width], x, NN, preferred_element_type=F32) for x in split(total)
        ]
        by_col = by_col[0] + by_col[1]
        folded = by_col
        for g in range(1, groups):
            folded = folded + pltpu.roll(by_col, g * width, 1)
        packed_ij = packed_ij * jnp.where(diag, 0.5, 1.0)
        both = (by_row + folded) * 0.5
        first = jnp.where(diag, jnp.where(t == 0, both, 0.0), by_row)
        second = jnp.where(diag, jnp.where(t == 1, both, 0.0), folded)
        near_turn = free - (LANES - width)
        far_turn = near_turn - width // 2
        shares = jnp.where(r8 == 3, pltpu.roll(second, far_turn % LANES, 1), 0.0)
        shares = jnp.where(r8 == 2, pltpu.roll(second, near_turn % LANES, 1), shares)
        shares = jnp.where(r8 == 1, pltpu.roll(first, far_turn % LANES, 1), shares)
        shares = jnp.where(r8 == 0, pltpu.roll(first, near_turn % LANES, 1), shares)
        shares = jnp.where(l8 < free + width // 2, shares, 0.0)
        out = jnp.where(l8 < free, packed_ij, shares)[0:4]

        @pl.when(t == 0)
        def _():
            message[...] = out

        @pl.when(t == 1)
        def _():
            message[...] += out

        return c

    lax.fori_loop(0, n_tiles, tile, 0)
    pl.semaphore_wait(news_sem.at[rounds - 1], near)

    for t in range(n):

        @pl.when(me != t)
        def _():
            pltpu.make_async_remote_copy(
                src_ref=message, dst_ref=slots.at[me],
                send_sem=msg_send, recv_sem=msg_recv,
                device_id={"virt": t // n_aux, "aux": t % n_aux}, device_id_type=MESH,
            ).start()

    slots[me] = message[...]
    sent = sum(cut[1] for cut in cuts)

    def flush(s, c):
        many = sum(jnp.where(there, 1, 0) for there, _, _ in decode(s, pick(kids, s)))
        for m in range(1, KIDS + 1):

            @pl.when(many == m)
            def _():
                gone = held.at[pl.ds(0, m), pl.ds(0, sent)]
                pltpu.make_async_copy(gone, gone, send_sem.at[s]).wait()

        return c

    lax.fori_loop(0, n_slots + 1, flush, 0)
    everyone = slots.at[pl.ds(0, n - 1)]
    pltpu.make_async_copy(everyone, everyone, msg_send).wait()
    pltpu.make_async_copy(everyone, everyone, msg_recv).wait()

    accs = [None] * 4
    for k in range(n):
        term = slots[k] * weigh[k]
        accs[k % 4] = term if accs[k % 4] is None else accs[k % 4] + term
    done_ref[...] = (accs[0] + accs[1]) + (accs[2] + accs[3])


def table_unpack(occ, width, done_ref, share_ref, pair_ref):
    tall = -(-occ // 4)
    free = tall * occ
    done = done_ref[...]
    share = done[0:2] + done[2:4]
    share_ref[...] = jnp.concatenate(
        [share[0, free:free + width // 2], share[1, free:free + width // 2]], 0
    )
    blocks = [done] + [pltpu.roll(done, LANES - g * occ, 1) for g in range(1, tall)]
    square = jnp.concatenate(blocks + [jnp.zeros((LANES - 4 * tall, LANES), F32)], 0)
    square = jnp.where(lax.broadcasted_iota(jnp.int32, (LANES, LANES), 1) < occ, square, 0.0)
    pair = square + square.T
    pair_ref[...] = pair[0:occ, 0:occ]


def table_call(n_virt, n_aux, occ, plan, three_index, eps_occ, eps_virt):
    rows, cols = three_index.shape
    width = cols // occ
    deep = -(-rows // 16) * 16
    n = n_virt * n_aux
    n_slots = 2 * n_aux
    vmem = pl.BlockSpec(memory_space=pltpu.VMEM)
    hbm = pl.BlockSpec(memory_space=pltpu.HBM)
    done = pl.pallas_call(
        functools.partial(table_kernel, n_virt, n_aux, occ, plan),
        out_shape=pltpu.VMEM((4, LANES), F32),
        in_specs=[hbm, hbm, hbm],
        out_specs=vmem,
        scratch_shapes=[
            pltpu.VMEM((rows, cols), BF16),
            pltpu.VMEM((n_slots + 1, deep, cols), BF16),
            pltpu.VMEM((cols, cols), BF16),
            pltpu.VMEM((2, cols, cols), F32),
            pltpu.VMEM((2, cols, cols), F32),
            pltpu.VMEM((occ * 8, cols), F32),
            pltpu.VMEM((4, LANES), F32),
            pltpu.VMEM((n, 4, LANES), F32),
            pltpu.VMEM((n, 4, LANES), F32),
            pltpu.SMEM(eps_occ.shape, F32),
            pltpu.SMEM(eps_virt.shape, F32),
            pltpu.SemaphoreType.DMA,
            pltpu.SemaphoreType.DMA((2,)),
            pltpu.SemaphoreType.DMA((n_slots + 1,)),
            pltpu.SemaphoreType.DMA((n_slots, 2)),
            pltpu.SemaphoreType.DMA,
            pltpu.SemaphoreType.DMA,
            pltpu.SemaphoreType.REGULAR((len(plan[5][0]) + 1,)),
        ],
        compiler_params=pltpu.CompilerParams(collective_id=0, has_side_effects=True),
    )(three_index, eps_occ, eps_virt)
    return pl.pallas_call(
        functools.partial(table_unpack, occ, width),
        out_shape=(
            jax.ShapeDtypeStruct((width,), F32),
            jax.ShapeDtypeStruct((occ, occ), F32),
        ),
        in_specs=[vmem],
        out_specs=(vmem, vmem),
    )(pltpu.with_memory_space_constraint(done, pltpu.VMEM))


def unpack(occ, width, done_ref, share_ref, pair_ref):
    tall = -(-occ // 8)
    free = tall * width
    done = done_ref[...]
    share = done[0:1] + done[1:2]
    share_ref[...] = share[0, free:free + width]
    blocks = [done] + [pltpu.roll(done, LANES - g * width, 1) for g in range(1, tall)]
    square = jnp.concatenate(blocks + [jnp.zeros((LANES - 8 * tall, LANES), F32)], 0)
    square = jnp.where(lax.broadcasted_iota(jnp.int32, (LANES, LANES), 1) < occ, square, 0.0)
    pair = square + square.T
    pair_ref[...] = pair[0:occ, 0:occ]


def on_device(n_virt, n_aux, three_index, eps_occ, eps_virt):
    occ = eps_occ.shape[0]
    rows, cols = three_index.shape
    width = cols // occ
    pitch = -(-rows // 16) * 16
    n = n_virt * n_aux
    vmem = pl.BlockSpec(memory_space=pltpu.VMEM)
    smem = pl.BlockSpec(memory_space=pltpu.SMEM)
    plan = PLANS.get((n_virt, n_aux))
    if plan is not None:
        return table_call(n_virt, n_aux, occ, plan, three_index, eps_occ, eps_virt)
    done = pl.pallas_call(
        functools.partial(kernel, n_virt, n_aux, occ),
        out_shape=jax.ShapeDtypeStruct((8, LANES), F32),
        in_specs=[vmem, smem, smem],
        out_specs=vmem,
        scratch_shapes=[
            pltpu.VMEM((2, n_aux, rows, cols), BF16),
            pltpu.VMEM((cols, n_aux * pitch), BF16),
            pltpu.VMEM((n_aux * pitch, cols), BF16),
            pltpu.VMEM((cols, cols), BF16),
            pltpu.VMEM((cols, cols), BF16),
            pltpu.VMEM((cols, cols), F32),
            pltpu.VMEM((occ * 8, cols), F32),
            pltpu.VMEM((8, LANES), F32),
            pltpu.VMEM((8, LANES), F32),
            pltpu.VMEM((n, 8, LANES), F32),
            pltpu.SemaphoreType.DMA,
            pltpu.SemaphoreType.DMA((3, n_aux)),
            pltpu.SemaphoreType.DMA((2, n_aux)),
            pltpu.SemaphoreType.DMA,
            pltpu.SemaphoreType.DMA,
        ],
        compiler_params=pltpu.CompilerParams(collective_id=0, has_side_effects=True),
    )(three_index, eps_occ, eps_virt)
    return pl.pallas_call(
        functools.partial(unpack, occ, width),
        out_shape=(
            jax.ShapeDtypeStruct((width,), F32),
            jax.ShapeDtypeStruct((occ, occ), F32),
        ),
        in_specs=[vmem],
        out_specs=(vmem, vmem),
    )(done)


def solution(mesh):
    n_virt, n_aux = mesh.shape["virt"], mesh.shape["aux"]
    assert n_virt == 2 * n_aux and n_aux % 2 == 0
    in_specs = (P("aux", "virt"), P(), P())
    out_specs = (P("virt"), P())
    return jax.shard_map(
        functools.partial(on_device, n_virt, n_aux), mesh=mesh,
        in_specs=in_specs, out_specs=out_specs, check_vma=False,
    )
```

```python
import functools

import jax
import jax.numpy as jnp
from jax import lax
from jax.experimental import pallas as pl
from jax.experimental.pallas import tpu as pltpu
from jax.sharding import PartitionSpec as P

MESH = pl.DeviceIdType.MESH
F32 = jnp.float32
BF16 = jnp.bfloat16
EXACT = lax.Precision.HIGHEST
LANES = 128
NT = (((1,), (1,)), ((), ()))
NN = (((1,), (0,)), ((), ()))


def distances(n_aux):
    return list(range(1, n_aux + 1, 2)) + list(range(2, n_aux + 1, 2))


def pick(table, at):
    got = table[0] + jnp.int32(0)
    for k in range(1, len(table)):
        got = jnp.where(at == k, table[k] + jnp.int32(0), got)
    return got


def label_of(virt, n_virt):
    return lax.rem(virt, 2) * (n_virt // 2) + virt // 2


def virt_of(label, n_virt):
    half = n_virt // 2
    return lax.rem(label, half) * 2 + label // half


def kernel(
    n_virt, n_aux, occ,
    x_ref, occ_ref, virt_ref,
    done_ref,
    held, lhs, rhs, order, order_t, ints, sums, parts, message, slots,
    own_sem, send_sem, recv_sem, msg_send, msg_recv,
):
    rows, cols = x_ref.shape
    pitch = -(-rows // 16) * 16
    width = cols // occ
    groups = LANES // width
    supers = occ // groups
    n = n_virt * n_aux
    v = lax.axis_index("virt")
    p = lax.axis_index("aux")
    me = v * n_aux + p
    table = distances(n_aux)
    label = label_of(v, n_virt)
    other = virt_of(lax.rem(label + pick(table, p), n_virt), n_virt)
    lower = label < n_virt // 2
    solo = jnp.logical_and(p == n_aux - 1, jnp.logical_not(lower))
    extra = jnp.logical_and(p == n_aux // 2 - 1, lower)

    barrier = pltpu.get_barrier_semaphore()

    def greet(k, c):
        t = lax.rem(me + k, n)
        pl.semaphore_signal(
            barrier, inc=1,
            device_id={"virt": t // n_aux, "aux": lax.rem(t, n_aux)},
            device_id_type=MESH,
        )
        return c

    lax.fori_loop(1, n, greet, 0)
    own = pltpu.make_async_copy(x_ref, held.at[0, p], own_sem)
    own.start()
    pl.semaphore_wait(barrier, n - 1)

    pairs = n_aux // 2

    def place(k):
        return lax.rem(p // 2 + k // 2, pairs) * 2 + lax.rem(p + k, 2)

    def share_own(k):
        return pltpu.make_async_remote_copy(
            src_ref=x_ref, dst_ref=held.at[0, p],
            send_sem=send_sem.at[0, k], recv_sem=recv_sem.at[0, p],
            device_id={"virt": v, "aux": place(k)}, device_id_type=MESH,
        )

    def hand_on(k):
        q = place(k)
        return pltpu.make_async_remote_copy(
            src_ref=held.at[0, q], dst_ref=held.at[0, q],
            send_sem=send_sem.at[2, k], recv_sem=recv_sem.at[0, q],
            device_id={"virt": v, "aux": place(1)}, device_id_type=MESH,
        )

    def share_other(k):
        q = place(k)
        target = lax.rem(label + n_virt - pick(table, q), n_virt)
        copy = pltpu.make_async_remote_copy(
            src_ref=x_ref, dst_ref=held.at[1, p],
            send_sem=send_sem.at[1, k], recv_sem=recv_sem.at[1, p],
            device_id={"virt": virt_of(target, n_virt), "aux": q}, device_id_type=MESH,
        )
        wanted = jnp.logical_or(q < n_aux - 1, target < n_virt // 2)
        return copy, wanted

    for k in list(range(2, n_aux, 2)) + [1]:
        share_own(k).start()
    for k in range(n_aux):
        copy, wanted = share_other(k)
        pl.when(wanted)(copy.start)

    def arrived(side, q):
        pltpu.make_async_copy(
            held.at[side, q], held.at[side, q], recv_sem.at[side, q]
        ).wait()

    row = lax.broadcasted_iota(jnp.int32, (cols, cols), 0)
    col = lax.broadcasted_iota(jnp.int32, (cols, cols), 1)
    hit = col == lax.rem(row, width) * occ + row // width
    order[...] = jnp.where(hit, 1.0, 0.0).astype(BF16)
    hit = row == lax.rem(col, width) * occ + col // width
    order_t[...] = jnp.where(hit, 1.0, 0.0).astype(BF16)
    lhs[...] = jnp.zeros_like(lhs)
    rhs[...] = jnp.zeros_like(rhs)

    def turn(k):
        lhs[:, k * pitch:k * pitch + rows] = lax.dot_general(
            order[...], held[0, place(k)], NT, preferred_element_type=F32
        ).astype(BF16)

    own.wait()
    turn(0)
    for k in range(2, n_aux, 2):
        arrived(0, place(k))
        hand_on(k).start()
        turn(k)
    for k in range(1, n_aux, 2):
        arrived(0, place(k))
        turn(k)

    lane = lax.broadcasted_iota(jnp.int32, (1, LANES), 1)
    part = lane // width
    down = lax.broadcasted_iota(jnp.int32, (width, 1), 0)
    lane_in = lax.rem(lane, width)

    def eps_down(which):
        got = jnp.zeros((width, 1), F32)
        for k in range(width):
            got = jnp.where(down == k, virt_ref[which * width + k], got)
        return got

    def eps_across(which):
        got = jnp.zeros((1, LANES), F32)
        for k in range(width):
            got = jnp.where(lane_in == k, virt_ref[which * width + k], got)
        return got

    occ_lane = []
    for cj in range(supers):
        got = jnp.zeros((1, LANES), F32)
        for t in range(groups):
            got = jnp.where(part == t, occ_ref[cj * groups + t], got)
        occ_lane.append(got)

    tall = -(-occ // 8)
    sums[...] = jnp.zeros_like(sums)
    n_tiles = jnp.where(extra, 2, 1)
    r8 = lax.broadcasted_iota(jnp.int32, (8, LANES), 0)
    l8 = lax.broadcasted_iota(jnp.int32, (8, LANES), 1)
    free = tall * width

    def tile(t, c):
        diag = jnp.logical_or(solo, jnp.logical_and(extra, t == 0))
        source = jnp.where(diag, 0, 1)

        for k in range(n_aux):

            @pl.when(source == 1)
            def _():
                arrived(1, place(k))

            rhs[k * pitch:k * pitch + rows, :] = lax.dot_general(
                held[source, place(k)], order_t[...], NN, preferred_element_type=F32
            ).astype(BF16)
        ints[...] = lax.dot_general(lhs[...], rhs[...], NN, preferred_element_type=F32)

        base = -(eps_down(v) + eps_across(jnp.where(diag, v, other)))
        total = jnp.zeros((width, LANES), F32)
        for ci in range(supers):
            for cj in range(ci, supers):
                turned = []
                for g in range(groups):
                    block = ints[pl.ds((cj * groups + g) * width, width), pl.ds(ci * LANES, LANES)]
                    turned.append([block if r == 0 else pltpu.roll(block, r * width, 1) for r in range(groups)])
                for s in range(groups):
                    i = ci * groups + s
                    direct = ints[pl.ds(i * width, width), pl.ds(cj * LANES, LANES)]
                    swapped = turned[0][(0 - s) % groups]
                    for g in range(1, groups):
                        swapped = jnp.where(part == g, turned[g][(g - s) % groups], swapped)
                    below = base + (occ_lane[cj] + occ_ref[i])
                    if ci == cj:
                        term = direct * (2.0 * direct - swapped) / below
                    else:
                        term = 2.0 * (direct * (direct - swapped) + swapped * swapped) / below
                    total = total + term
                    short = term[0:8]
                    for m in range(8, width, 8):
                        short = short + term[m:m + 8]
                    sums[i * 8:i * 8 + 8, cj * LANES:(cj + 1) * LANES] = short

        wide = lax.broadcasted_iota(jnp.int32, (cols, LANES), 0)
        thin = lax.broadcasted_iota(jnp.int32, (cols, LANES), 1)
        fold = jnp.where(wide // width == thin, 1.0, 0.0)
        by_j = lax.dot_general(sums[...], fold, NN, precision=EXACT, preferred_element_type=F32)
        ri = lax.broadcasted_iota(jnp.int32, (tall * 8, occ * 8), 0)
        rj = lax.broadcasted_iota(jnp.int32, (tall * 8, occ * 8), 1)
        by_ij = lax.dot_general(
            jnp.where(rj // 8 == ri, 1.0, 0.0), by_j, NN,
            precision=EXACT, preferred_element_type=F32,
        )
        packed = by_ij[0:8]
        for g in range(1, tall):
            packed = packed + pltpu.roll(by_ij[g * 8:g * 8 + 8], g * width, 1)
        pads = [jnp.zeros((free, LANES), F32), total]
        if free + width < LANES:
            pads.append(jnp.zeros((LANES - free - width, LANES), F32))
        spread = jnp.concatenate(pads, 0)
        by_row = lax.dot_general(
            jnp.ones((8, LANES), F32), spread, NT, precision=EXACT, preferred_element_type=F32)
        by_col = lax.dot_general(
            jnp.ones((8, width), F32), total, NN, precision=EXACT, preferred_element_type=F32)
        folded = by_col
        for g in range(1, groups):
            folded = folded + pltpu.roll(by_col, g * width, 1)
        packed = packed * jnp.where(diag, 0.5, 1.0)
        first = jnp.where(diag, (by_row + folded) * 0.5, by_row)
        second = jnp.where(diag, 0.0, folded)
        out = jnp.where(l8 < free, packed, jnp.where(r8 == 0, first, jnp.where(r8 == 1, second, 0.0)))

        @pl.when(t == 0)
        def _():
            message[...] = out

        @pl.when(t == 1)
        def _():
            message[...] += out

        return c

    lax.fori_loop(0, n_tiles, tile, 0)

    def tell(k, c):
        t = lax.rem(me + k, n)
        pltpu.make_async_remote_copy(
            src_ref=message, dst_ref=slots.at[me],
            send_sem=msg_send, recv_sem=msg_recv,
            device_id={"virt": t // n_aux, "aux": lax.rem(t, n_aux)},
            device_id_type=MESH,
        ).start()
        return c

    lax.fori_loop(1, n, tell, 0)
    slots[me] = message[...]
    for k in list(range(2, n_aux, 2)) + [1]:
        share_own(k).wait_send()
    for k in range(2, n_aux, 2):
        hand_on(k).wait_send()
    for k in range(n_aux):
        copy, wanted = share_other(k)
        pl.when(wanted)(copy.wait_send)
    everyone = slots.at[pl.ds(0, n - 1)]
    pltpu.make_async_copy(everyone, everyone, msg_send).wait()
    pltpu.make_async_copy(everyone, everyone, msg_recv).wait()

    keep = jnp.logical_or(l8 < free, r8 < 0)

    def add(k, acc):
        sv = k // n_aux
        so = virt_of(lax.rem(label_of(sv, n_virt) + pick(table, lax.rem(k, n_aux)), n_virt), n_virt)
        row0 = jnp.where(sv == v, 1.0, 0.0)
        row1 = jnp.where(so == v, 1.0, 0.0)
        weight = jnp.where(keep, 1.0, jnp.where(r8 == 0, row0, row1))
        return acc + slots[k] * weight

    done = lax.fori_loop(0, n, add, jnp.zeros((8, LANES), F32))
    done_ref[...] = done


TILES = (
    (0, 2, 0),
    (0, 2, 1),
    (0, 1, 0),
    (1, 2, 0),
    (1, 3, 1),
    (0, 3, 0),
    (1, 3, 0),
    (2, 3, 0),
    (0, 4, 0),
    (0, 5, 0),
    (2, 4, 0),
    (2, 5, 0),
    (1, 4, 0),
    (3, 4, 0),
    (1, 5, 0),
    (3, 5, 0),
    (0, 6, 0),
    (0, 7, 0),
    (2, 6, 0),
    (2, 7, 0),
    (1, 6, 0),
    (1, 7, 0),
    (3, 6, 0),
    (3, 7, 0),
    (6, 7, 0),
    (6, 4, 0),
    (7, 4, 0),
    (6, 4, 1),
    (6, 5, 0),
    (7, 5, 1),
    (4, 5, 0),
    (7, 5, 0),
)
ROUTES = (
    ((2, 4, 10, 18), (10, 4), (2, 10, 18), (), (3,), (), (3,), (), ()),
    ((), (0, 34), (), (0, 10), (7, 14), (), (), (1,), ()),
    ((), (), (0,), (2,), (), (), (), (), ()),
    ((5,), (), (5,), (), (), (), (1, 14), (14, 3), (4, 18)),
    ((12, 24), (12, 24), (24,), (24,), (11,), (), (), (), ()),
    ((), (), (), (), (), (9, 13), (), (9,), (5, 8)),
    ((6, 28), (6, 28), (6, 8, 28), (8, 6, 28), (), (15,), (9, 15), (15,), ()),
    ((), (), (), (), (13,), (), (), (), (5, 12, 40)),
    ((), (18,), (), (), (), (27, 21), (), (27, 21), (1, 22)),
    ((16, 34), (), (16, 34), (16, 34), (23, 31), (), (), (), (1, 22, 36, 3)),
    ((36,), (), (7, 22), (7,), (), (), (17, 27), (), ()),
    ((20,), (7, 20, 14), (36, 38), (20, 36), (), (), (19,), (19,), ()),
    ((42,), (42,), (42,), (), (), (), (), (), (26, 30)),
    ((9, 46), (11, 44), (11,), (11,), (17, 25), (25,), (25,), (25,), ()),
    ((), (), (), (), (), (31, 61, 23), (31,), (23, 31), (30,)),
    ((15,), (), (13, 26, 46), (13, 26, 44), (29,), (), (), (), ()),
    ((), (), (), (), (), (), (41,), (), (27, 51)),
    ((32,), (16, 32), (32,), (32,), (), (), (), (), (17, 51, 60)),
    ((38,), (38,), (), (38,), (), (33,), (33, 45), (33, 45), (21, 55)),
    ((), (), (), (), (47, 52), (), (), (35,), (17, 55)),
    ((), (), (), (42,), (33, 56, 45), (45,), (), (), (19, 57)),
    ((40,), (40,), (40,), (), (), (39,), (35,), (), (29, 57, 59)),
    ((), (46, 30), (), (46,), (), (), (), (), (23, 61, 29)),
    ((44,), (), (44,), (), (), (), (), (39, 43, 52), (29, 63)),
    ((41, 50), (), (50, 56), (50, 56, 41), (35,), (35,), (), (), ()),
    ((54,), (41, 48, 54, 56), (), (), (55,), (53,), (), (), ()),
    ((), (), (), (), (), (55,), (), (), (54,)),
    ((37,), (37,), (37, 48), (37, 48), (53, 60, 21), (), (53, 60, 51), (53, 60, 51), ()),
    ((), (), (), (), (59, 63), (19,), (), (), (39, 58)),
    ((49, 62), (43, 49, 62), (43, 49), (49,), (), (63,), (57,), (57,), ()),
    ((), (), (), (), (), (), (63, 59), (59,), (39, 58, 62)),
    ((43,), (52, 47), (52, 47), (47, 58), (61,), (), (), (61,), ()),
)
STEPS = (
    (0, 1, 2, 3, 4, 10, 5, 8, 6, 25, 12, 27, 29, 7, 14, 31),
    (2, 19, 0, 17, 4, 6, 8, 21, 10, 23, 25, 27, 12, 14, 29, 31),
    (4, 5, 6, 7, 14, 0, 10, 12, 31, 1, 11, 29, 2, 19, 8, 25),
    (12, 4, 13, 14, 21, 15, 10, 6, 23, 8, 0, 11, 1, 25, 2, 19),
    (0, 17, 2, 19, 4, 10, 21, 27, 8, 6, 25, 23, 14, 12, 31, 29),
    (10, 0, 11, 1, 2, 19, 8, 14, 25, 4, 15, 6, 12, 5, 29, 23),
    (4, 5, 6, 7, 14, 0, 31, 1, 12, 2, 29, 10, 3, 8, 27, 25),
    (14, 15, 4, 12, 5, 8, 29, 10, 6, 9, 11, 2, 23, 0, 19, 17),
    (10, 14, 0, 6, 11, 15, 1, 2, 23, 12, 4, 8, 5, 29, 19, 25),
    (0, 6, 8, 1, 7, 25, 4, 12, 5, 2, 10, 14, 3, 29, 27, 31),
    (4, 5, 6, 7, 12, 2, 0, 29, 3, 1, 10, 14, 27, 8, 31, 25),
    (6, 7, 4, 5, 2, 0, 12, 3, 1, 14, 8, 29, 10, 31, 25, 27),
    (0, 1, 2, 8, 3, 4, 25, 5, 10, 12, 6, 7, 14, 29, 27, 31),
    (2, 3, 0, 1, 6, 7, 8, 4, 5, 25, 10, 12, 14, 29, 27, 31),
    (14, 4, 10, 15, 5, 12, 11, 6, 23, 0, 29, 8, 1, 2, 19, 25),
    (6, 7, 4, 5, 0, 14, 10, 1, 31, 12, 11, 8, 2, 29, 19, 25),
    (2, 14, 15, 3, 0, 12, 8, 6, 13, 1, 25, 23, 10, 4, 21, 27),
    (2, 3, 0, 6, 10, 1, 7, 27, 14, 4, 12, 8, 5, 25, 31, 29),
    (6, 14, 7, 31, 2, 4, 12, 13, 3, 21, 10, 27, 0, 8, 1, 25),
    (6, 12, 7, 8, 4, 2, 14, 13, 9, 3, 10, 31, 21, 27, 0, 17),
    (10, 8, 6, 11, 9, 7, 0, 14, 17, 31, 2, 19, 12, 4, 13, 21),
    (10, 11, 6, 14, 0, 1, 12, 7, 31, 2, 19, 13, 4, 8, 21, 25),
    (2, 6, 3, 7, 14, 0, 31, 10, 4, 1, 12, 8, 27, 5, 29, 25),
    (14, 2, 6, 0, 3, 15, 23, 12, 4, 1, 13, 10, 21, 8, 27, 25),
    (0, 1, 2, 3, 6, 10, 7, 27, 4, 8, 5, 25, 14, 12, 31, 29),
    (2, 3, 0, 1, 10, 8, 6, 7, 25, 4, 27, 14, 5, 12, 31, 29),
    (4, 14, 12, 5, 2, 15, 10, 29, 0, 3, 6, 8, 9, 27, 17, 23),
    (6, 23, 4, 21, 2, 14, 12, 19, 0, 31, 29, 17, 8, 10, 25, 27),
    (2, 10, 8, 3, 9, 6, 27, 7, 12, 0, 14, 17, 4, 13, 21, 31),
    (2, 19, 0, 17, 6, 4, 8, 10, 23, 21, 25, 12, 14, 27, 29, 31),
    (12, 14, 13, 6, 15, 2, 4, 23, 10, 8, 21, 0, 11, 19, 1, 25),
    (6, 7, 4, 5, 2, 14, 3, 12, 31, 0, 29, 8, 1, 25, 10, 27),
)
PARTNERS = (
    (1, 2, 4, 8, 3, 9),
    (0, 3, 5, 9, 2),
    (3, 0, 6, 10, 5, 7),
    (2, 1, 7, 11, 6, 10),
    (5, 6, 0, 12, 13),
    (4, 7, 1, 13, 0),
    (7, 4, 2, 14, 5, 15),
    (6, 5, 3, 15, 1, 11),
    (9, 10, 12, 0, 16, 13, 17, 19),
    (8, 11, 13, 1, 17, 0, 3, 20, 28),
    (11, 8, 14, 2, 18, 27),
    (10, 9, 15, 3, 19, 8, 14, 22),
    (13, 14, 8, 4, 20),
    (12, 15, 9, 5, 21, 8, 10, 16),
    (15, 12, 10, 6, 22, 21, 23),
    (14, 13, 11, 7, 23, 9, 12, 22),
    (17, 18, 20, 8, 24),
    (16, 19, 21, 9, 25, 1, 24),
    (19, 16, 22, 10, 26, 9, 11, 27),
    (18, 17, 23, 11, 27, 21, 28, 30),
    (21, 22, 16, 12, 28, 7, 24, 25),
    (20, 23, 17, 13, 29, 12, 31),
    (23, 20, 18, 14, 30, 13, 15),
    (22, 21, 19, 15, 31, 13),
    (25, 26, 28, 16, 27, 29),
    (24, 27, 29, 17, 16),
    (27, 24, 30, 18, 19, 23, 25, 31),
    (26, 25, 31, 19, 18),
    (29, 30, 24, 20, 21, 25),
    (28, 31, 25, 21, 30),
    (31, 28, 26, 22, 14, 17, 27),
    (30, 29, 27, 23, 28),
)
NEAR = (4, 4, 4, 4, 4, 4, 4, 4, 5, 5, 5, 5, 5, 5, 5, 5, 5, 5, 5, 5, 5, 5, 5, 5, 4, 4, 4, 4, 4, 4, 4, 4)
AWAITED = (6, 6, 5, 6, 4, 6, 5, 6, 7, 8, 7, 7, 7, 9, 7, 7, 7, 7, 6, 7, 6, 8, 7, 7, 6, 7, 4, 8, 7, 5, 6, 6)
NEWS = (
    (8, 12, 14),
    (5, 9, 15),
    (6, 12, 14),
    (3, 8, 12),
    (7, 12, 15),
    (4, 10, 15),
    (8, 12, 15),
    (1, 7, 13),
    (1, 7, 15),
    (1, 7, 11),
    (5, 10, 12),
    (6, 9, 14),
    (2, 5, 11),
    (6, 10, 14),
    (2, 7, 11),
    (5, 9, 12),
    (0, 2, 10),
    (0, 3, 7),
    (3, 9, 14),
    (1, 8, 14),
    (0, 4, 9),
    (1, 5, 10),
    (2, 6, 12),
    (1, 7, 14),
    (6, 12, 15),
    (6, 11, 15),
    (0, 6, 12),
    (8, 12, 15),
    (3, 7, 11),
    (5, 10, 15),
    (1, 5, 11),
    (6, 10, 13),
)
PLANS = {(8, 4): (TILES, ROUTES, STEPS, PARTNERS, NEAR, NEWS, AWAITED)}


TN = (((0,), (0,)), ((), ()))
KIDS = 4
CODE = 128


def table_kernel(
    n_virt, n_aux, occ, plan,
    x_ref, occ_hbm, virt_hbm,
    done_ref,
    raw, held, order, ints, over, sums, message, slots, weigh, occ_ref, virt_ref,
    own_sem, eps_sem, send_sem, recv_sem, msg_send, msg_recv, news_sem,
):
    rows, cols = x_ref.shape
    deep = held.shape[1]
    width = cols // occ
    groups = LANES // width
    supers = occ // groups
    n = n_virt * n_aux
    v = lax.axis_index("virt")
    p = lax.axis_index("aux")
    me = v * n_aux + p
    tiles, routes, steps, partners, n_near, news, awaited = plan
    rounds = len(news[0]) + 1
    half = -(-rows // 32) * 16
    cuts = ((0, half), (half, -(-rows // 8) * 8 - half))
    n_slots = 2 * n_aux

    def device(t):
        return {"virt": lax.div(t, n_aux), "aux": lax.rem(t, n_aux)}

    barrier = pltpu.get_barrier_semaphore()

    side_a = pick([t[0] for t in tiles], me)
    side_b = pick([t[1] for t in tiles], me)
    diag = pick([t[2] for t in tiles], me) == 1
    own_slot = jnp.where(side_a == v, p, jnp.where(side_b == v, n_aux + p, n_slots))
    owns = []
    for d, (a, b, _) in enumerate(tiles):
        q = d % n_aux
        owns.append(q if a == d // n_aux else n_aux + q if b == d // n_aux else n_slots)
    own = pltpu.make_async_copy(x_ref, raw, own_sem)
    own.start()
    eps = (
        pltpu.make_async_copy(occ_hbm, occ_ref, eps_sem.at[0]),
        pltpu.make_async_copy(virt_hbm, virt_ref, eps_sem.at[1]),
    )
    for copy in eps:
        copy.start()

    def packed(codes):
        got = 0
        for c in reversed(codes):
            got = got * CODE + c + 1
        return got

    most = max(len(r) for r in partners)
    folk = [
        pick([packed(r[at:at + KIDS]) for r in partners], me) for at in range(0, most, KIDS)
    ]
    n_folk = pick([len(r) for r in partners], me)
    near = pick(n_near, me)

    def signal(sem, amount, limit):
        code = None
        for k in range(amount):
            code = folk[k // KIDS] if k % KIDS == 0 else lax.div(code, CODE)

            @pl.when(k < limit)
            def _():
                t = lax.rem(code, CODE) - 1
                pl.semaphore_signal(sem, inc=1, device_id=device(t), device_id_type=MESH)

    if deep > rows:
        held[:, rows:, :] = jnp.zeros((n_slots + 1, deep - rows, cols), BF16)
    signal(barrier, most, n_folk)

    row = lax.broadcasted_iota(jnp.int32, (cols, cols), 0)
    col = lax.broadcasted_iota(jnp.int32, (cols, cols), 1)
    hit = row == lax.rem(col, width) * occ + col // width
    order[...] = jnp.where(hit, 1.0, 0.0).astype(BF16)
    own.wait()
    held[own_slot, 0:rows, :] = lax.dot_general(
        raw[...], order[...], NN, preferred_element_type=F32
    ).astype(BF16)
    pl.semaphore_wait(barrier, pick(awaited, me))

    own_kids = pick([packed(r[o]) for r, o in zip(routes, owns)], me)

    def piece(slot, part):
        return held.at[slot, pl.ds(cuts[part][0], cuts[part][1])]

    def decode(slot, code):
        q = jnp.where(slot == n_slots, p, lax.rem(slot, n_aux))
        found = []
        for k in range(KIDS):
            this = lax.rem(code, CODE)
            code = lax.div(code, CODE)
            t = jnp.maximum(this - 1, 0)
            found.append((this > 0, lax.div(t, 2), lax.rem(t, 2) * n_aux + q))
        return found

    def copies(slot, part, found, act):
        for there, t, to in found:

            @pl.when(there)
            def _():
                act(pltpu.make_async_remote_copy(
                    src_ref=piece(slot, part), dst_ref=piece(to, part),
                    send_sem=send_sem.at[slot], recv_sem=recv_sem.at[to, part],
                    device_id=device(t), device_id_type=MESH,
                ))

    own_found = decode(own_slot, own_kids)
    for part in range(2):
        copies(own_slot, part, own_found, lambda copy: copy.start())
    close = max(n_near)
    signal(news_sem.at[0], close, near)
    kids = [pick([packed(r[s]) for r in routes], me) for s in range(n_slots + 1)]
    spread_at = [pick([r[k] for r in news], me) for k in range(rounds - 1)]
    todo = [pick([r[i] for r in steps], me) for i in range(2 * n_slots)]
    for copy in eps:
        copy.wait()

    lane = lax.broadcasted_iota(jnp.int32, (1, LANES), 1)
    part = lane // width
    down = lax.broadcasted_iota(jnp.int32, (width, 1), 0)
    lane_in = lax.rem(lane, width)
    n_tiles = jnp.where(diag, 2, 1)

    def eps_down(which):
        got = jnp.zeros((width, 1), F32)
        for k in range(width):
            got = jnp.where(down == k, virt_ref[which * width + k], got)
        return got

    def eps_across(which):
        got = jnp.zeros((1, LANES), F32)
        for k in range(width):
            got = jnp.where(lane_in == k, virt_ref[which * width + k], got)
        return got

    occ_lane = []
    for cj in range(supers):
        got = jnp.zeros((1, LANES), F32)
        for t in range(groups):
            got = jnp.where(part == t, occ_ref[cj * groups + t], got)
        occ_lane.append(got)

    def prepare(t, c):
        block_l = jnp.where(t == 0, side_a, side_b)
        block_r = jnp.where(jnp.logical_and(diag, t == 0), side_a, side_b)
        base = -(eps_down(block_l) + eps_across(block_r))
        ints[t] = jnp.zeros((cols, cols), F32)
        for i in range(occ):
            for cj in range(i // groups, supers):
                below = base + (occ_lane[cj] + occ_ref[i])
                over[t, i * width:(i + 1) * width, cj * LANES:(cj + 1) * LANES] = (
                    (1.0 if cj == i // groups else 2.0) / below
                )
        return c

    lax.fori_loop(0, n_tiles, prepare, 0)

    keep = lax.broadcasted_iota(jnp.int32, (4, LANES), 1) < -(-occ // 4) * occ
    upper = lax.broadcasted_iota(jnp.int32, (4, LANES), 0) < 2
    for k in range(n):
        row0 = jnp.where(v == tiles[k][0], 1.0, 0.0)
        row1 = jnp.where(v == tiles[k][1], 1.0, 0.0)
        weigh[k] = jnp.where(keep, 1.0, jnp.where(upper, row0, row1))

    def take(i, c):
        for r in range(1, rounds):

            @pl.when(i == spread_at[r - 1])
            def _():
                pl.semaphore_wait(news_sem.at[r - 1], near)
                signal(news_sem.at[r], close, near)

        entry = pick(todo, i)
        slot = lax.rem(lax.div(entry, 2), n_slots)
        meets = lax.div(entry, 4 * n_aux) == 1
        later = lax.rem(entry, 2)
        away = slot != own_slot
        found = decode(slot, pick(kids, slot))
        for part in range(2):

            @pl.when(jnp.logical_and(later == part, away))
            def _():
                whole = piece(slot, part)
                pltpu.make_async_copy(whole, whole, recv_sem.at[slot, part]).wait()
                copies(slot, part, found, lambda copy: copy.start())

        side = lax.div(slot, n_aux)
        mine = jnp.where(diag, side, 0)
        left = jnp.where(diag, slot, lax.rem(slot, n_aux))
        right = jnp.where(diag, slot, n_aux + lax.rem(slot, n_aux))

        @pl.when(meets)
        def _():
            ints[mine] += lax.dot_general(held[left], held[right], TN, preferred_element_type=F32)

        return c

    lax.fori_loop(0, 2 * n_slots, take, 0)

    tall = -(-occ // 4)
    sums[...] = jnp.zeros_like(sums)
    r8 = lax.broadcasted_iota(jnp.int32, (8, LANES), 0)
    l8 = lax.broadcasted_iota(jnp.int32, (8, LANES), 1)
    wide = lax.broadcasted_iota(jnp.int32, (cols, LANES), 0)
    thin = lax.broadcasted_iota(jnp.int32, (cols, LANES), 1)
    fold = jnp.where(wide // width == thin, 1.0, 0.0).astype(BF16)
    ri = lax.broadcasted_iota(jnp.int32, (tall * 8, occ * 8), 0)
    rj = lax.broadcasted_iota(jnp.int32, (tall * 8, occ * 8), 1)
    gather = jnp.logical_and(lax.rem(ri, 8) < 4, rj // 8 == ri // 8 * 4 + lax.rem(ri, 8))
    gather = jnp.where(gather, 1.0, 0.0).astype(BF16)
    ones = jnp.ones((8, LANES), BF16)
    free = tall * occ

    def split(x):
        high = x.astype(BF16)
        return high, (x - high.astype(F32)).astype(BF16)

    def tile(t, c):
        total = jnp.zeros((width, LANES), F32)
        for ci in range(supers):
            for cj in range(ci, supers):
                block = [
                    ints[t, pl.ds((cj * groups + g) * width, width), pl.ds(ci * LANES, LANES)]
                    for g in range(groups)
                ]
                turned = []
                for r in range(groups):
                    mixed = block[r]
                    for g in range(1, groups):
                        mixed = jnp.where(part == g, block[(g + r) % groups], mixed)
                    turned.append(mixed if r == 0 else pltpu.roll(mixed, r * width, 1))
                for s in range(groups):
                    i = ci * groups + s
                    direct = ints[t, pl.ds(i * width, width), pl.ds(cj * LANES, LANES)]
                    inverse = over[t, pl.ds(i * width, width), pl.ds(cj * LANES, LANES)]
                    swapped = turned[(0 - s) % groups]
                    for g in range(1, groups):
                        swapped = jnp.where(part == g, turned[(g - s) % groups], swapped)
                    if ci == cj:
                        term = direct * (2.0 * direct - swapped) * inverse
                    else:
                        term = (direct * (direct - swapped) + swapped * swapped) * inverse
                    total = total + term
                    short = term[0:8]
                    for m in range(8, width, 8):
                        short = short + term[m:m + 8]
                    sums[i * 8:i * 8 + 8, cj * LANES:(cj + 1) * LANES] = short

        rows_of = [
            lax.dot_general(gather, x, NN, preferred_element_type=F32) for x in split(sums[...])
        ]
        pairs_of = [
            lax.dot_general(x, fold, NN, preferred_element_type=F32)
            for x in split(rows_of[0] + rows_of[1])
        ]
        by_ij = pairs_of[0] + pairs_of[1]
        packed_ij = by_ij[0:8]
        for g in range(1, tall):
            packed_ij = packed_ij + pltpu.roll(by_ij[g * 8:g * 8 + 8], g * occ, 1)
        spread = jnp.concatenate([jnp.zeros((LANES - width, LANES), F32), total], 0)
        by_row = [
            lax.dot_general(ones, x, NT, preferred_element_type=F32) for x in split(spread)
        ]
        by_row = by_row[0] + by_row[1]
        by_col = [
            lax.dot_general(ones[:, :width], x, NN, preferred_element_type=F32) for x in split(total)
        ]
        by_col = by_col[0] + by_col[1]
        folded = by_col
        for g in range(1, groups):
            folded = folded + pltpu.roll(by_col, g * width, 1)
        packed_ij = packed_ij * jnp.where(diag, 0.5, 1.0)
        both = (by_row + folded) * 0.5
        first = jnp.where(diag, jnp.where(t == 0, both, 0.0), by_row)
        second = jnp.where(diag, jnp.where(t == 1, both, 0.0), folded)
        near_turn = free - (LANES - width)
        far_turn = near_turn - width // 2
        shares = jnp.where(r8 == 3, pltpu.roll(second, far_turn % LANES, 1), 0.0)
        shares = jnp.where(r8 == 2, pltpu.roll(second, near_turn % LANES, 1), shares)
        shares = jnp.where(r8 == 1, pltpu.roll(first, far_turn % LANES, 1), shares)
        shares = jnp.where(r8 == 0, pltpu.roll(first, near_turn % LANES, 1), shares)
        shares = jnp.where(l8 < free + width // 2, shares, 0.0)
        out = jnp.where(l8 < free, packed_ij, shares)[0:4]

        @pl.when(t == 0)
        def _():
            message[...] = out

        @pl.when(t == 1)
        def _():
            message[...] += out

        return c

    lax.fori_loop(0, n_tiles, tile, 0)
    pl.semaphore_wait(news_sem.at[rounds - 1], near)

    for t in range(n):

        @pl.when(me != t)
        def _():
            pltpu.make_async_remote_copy(
                src_ref=message, dst_ref=slots.at[me],
                send_sem=msg_send, recv_sem=msg_recv,
                device_id={"virt": t // n_aux, "aux": t % n_aux}, device_id_type=MESH,
            ).start()

    slots[me] = message[...]
    sent = sum(cut[1] for cut in cuts)

    def flush(s, c):
        many = sum(jnp.where(there, 1, 0) for there, _, _ in decode(s, pick(kids, s)))
        for m in range(1, KIDS + 1):

            @pl.when(many == m)
            def _():
                gone = held.at[pl.ds(0, m), pl.ds(0, sent)]
                pltpu.make_async_copy(gone, gone, send_sem.at[s]).wait()

        return c

    lax.fori_loop(0, n_slots + 1, flush, 0)
    everyone = slots.at[pl.ds(0, n - 1)]
    pltpu.make_async_copy(everyone, everyone, msg_send).wait()
    pltpu.make_async_copy(everyone, everyone, msg_recv).wait()

    accs = [None] * 4
    for k in range(n):
        term = slots[k] * weigh[k]
        accs[k % 4] = term if accs[k % 4] is None else accs[k % 4] + term
    done_ref[...] = (accs[0] + accs[1]) + (accs[2] + accs[3])


def table_unpack(occ, width, done_ref, share_ref, pair_ref):
    tall = -(-occ // 4)
    free = tall * occ
    done = done_ref[...]
    share = done[0:2] + done[2:4]
    share_ref[...] = jnp.concatenate(
        [share[0, free:free + width // 2], share[1, free:free + width // 2]], 0
    )
    blocks = [done] + [pltpu.roll(done, LANES - g * occ, 1) for g in range(1, tall)]
    square = jnp.concatenate(blocks + [jnp.zeros((LANES - 4 * tall, LANES), F32)], 0)
    square = jnp.where(lax.broadcasted_iota(jnp.int32, (LANES, LANES), 1) < occ, square, 0.0)
    pair = square + square.T
    pair_ref[...] = pair[0:occ, 0:occ]


def table_call(n_virt, n_aux, occ, plan, three_index, eps_occ, eps_virt):
    rows, cols = three_index.shape
    width = cols // occ
    deep = -(-rows // 16) * 16
    n = n_virt * n_aux
    n_slots = 2 * n_aux
    vmem = pl.BlockSpec(memory_space=pltpu.VMEM)
    hbm = pl.BlockSpec(memory_space=pltpu.HBM)
    done = pl.pallas_call(
        functools.partial(table_kernel, n_virt, n_aux, occ, plan),
        out_shape=pltpu.VMEM((4, LANES), F32),
        in_specs=[hbm, hbm, hbm],
        out_specs=vmem,
        scratch_shapes=[
            pltpu.VMEM((rows, cols), BF16),
            pltpu.VMEM((n_slots + 1, deep, cols), BF16),
            pltpu.VMEM((cols, cols), BF16),
            pltpu.VMEM((2, cols, cols), F32),
            pltpu.VMEM((2, cols, cols), F32),
            pltpu.VMEM((occ * 8, cols), F32),
            pltpu.VMEM((4, LANES), F32),
            pltpu.VMEM((n, 4, LANES), F32),
            pltpu.VMEM((n, 4, LANES), F32),
            pltpu.SMEM(eps_occ.shape, F32),
            pltpu.SMEM(eps_virt.shape, F32),
            pltpu.SemaphoreType.DMA,
            pltpu.SemaphoreType.DMA((2,)),
            pltpu.SemaphoreType.DMA((n_slots + 1,)),
            pltpu.SemaphoreType.DMA((n_slots, 2)),
            pltpu.SemaphoreType.DMA,
            pltpu.SemaphoreType.DMA,
            pltpu.SemaphoreType.REGULAR((len(plan[5][0]) + 1,)),
        ],
        compiler_params=pltpu.CompilerParams(collective_id=0, has_side_effects=True),
    )(three_index, eps_occ, eps_virt)
    return pl.pallas_call(
        functools.partial(table_unpack, occ, width),
        out_shape=(
            jax.ShapeDtypeStruct((width,), F32),
            jax.ShapeDtypeStruct((occ, occ), F32),
        ),
        in_specs=[vmem],
        out_specs=(vmem, vmem),
    )(pltpu.with_memory_space_constraint(done, pltpu.VMEM))


def unpack(occ, width, done_ref, share_ref, pair_ref):
    tall = -(-occ // 8)
    free = tall * width
    done = done_ref[...]
    share = done[0:1] + done[1:2]
    share_ref[...] = share[0, free:free + width]
    blocks = [done] + [pltpu.roll(done, LANES - g * width, 1) for g in range(1, tall)]
    square = jnp.concatenate(blocks + [jnp.zeros((LANES - 8 * tall, LANES), F32)], 0)
    square = jnp.where(lax.broadcasted_iota(jnp.int32, (LANES, LANES), 1) < occ, square, 0.0)
    pair = square + square.T
    pair_ref[...] = pair[0:occ, 0:occ]


def on_device(n_virt, n_aux, three_index, eps_occ, eps_virt):
    occ = eps_occ.shape[0]
    rows, cols = three_index.shape
    width = cols // occ
    pitch = -(-rows // 16) * 16
    n = n_virt * n_aux
    vmem = pl.BlockSpec(memory_space=pltpu.VMEM)
    smem = pl.BlockSpec(memory_space=pltpu.SMEM)
    plan = PLANS.get((n_virt, n_aux))
    if plan is not None:
        return table_call(n_virt, n_aux, occ, plan, three_index, eps_occ, eps_virt)
    done = pl.pallas_call(
        functools.partial(kernel, n_virt, n_aux, occ),
        out_shape=jax.ShapeDtypeStruct((8, LANES), F32),
        in_specs=[vmem, smem, smem],
        out_specs=vmem,
        scratch_shapes=[
            pltpu.VMEM((2, n_aux, rows, cols), BF16),
            pltpu.VMEM((cols, n_aux * pitch), BF16),
            pltpu.VMEM((n_aux * pitch, cols), BF16),
            pltpu.VMEM((cols, cols), BF16),
            pltpu.VMEM((cols, cols), BF16),
            pltpu.VMEM((cols, cols), F32),
            pltpu.VMEM((occ * 8, cols), F32),
            pltpu.VMEM((8, LANES), F32),
            pltpu.VMEM((8, LANES), F32),
            pltpu.VMEM((n, 8, LANES), F32),
            pltpu.SemaphoreType.DMA,
            pltpu.SemaphoreType.DMA((3, n_aux)),
            pltpu.SemaphoreType.DMA((2, n_aux)),
            pltpu.SemaphoreType.DMA,
            pltpu.SemaphoreType.DMA,
        ],
        compiler_params=pltpu.CompilerParams(collective_id=0, has_side_effects=True),
    )(three_index, eps_occ, eps_virt)
    return pl.pallas_call(
        functools.partial(unpack, occ, width),
        out_shape=(
            jax.ShapeDtypeStruct((width,), F32),
            jax.ShapeDtypeStruct((occ, occ), F32),
        ),
        in_specs=[vmem],
        out_specs=(vmem, vmem),
    )(done)


def solution(mesh):
    n_virt, n_aux = mesh.shape["virt"], mesh.shape["aux"]
    assert n_virt == 2 * n_aux and n_aux % 2 == 0
    in_specs = (P("aux", "virt"), P(), P())
    out_specs = (P("virt"), P())
    return jax.shard_map(
        functools.partial(on_device, n_virt, n_aux), mesh=mesh,
        in_specs=in_specs, out_specs=out_specs, check_vma=False,
    )
```

```python
import functools

import jax
import jax.numpy as jnp
from jax import lax
from jax.experimental import pallas as pl
from jax.experimental.pallas import tpu as pltpu
from jax.sharding import PartitionSpec as P

MESH = pl.DeviceIdType.MESH
F32 = jnp.float32
BF16 = jnp.bfloat16
EXACT = lax.Precision.HIGHEST
LANES = 128
NT = (((1,), (1,)), ((), ()))
NN = (((1,), (0,)), ((), ()))


def distances(n_aux):
    return list(range(1, n_aux + 1, 2)) + list(range(2, n_aux + 1, 2))


def pick(table, at):
    got = table[0] + jnp.int32(0)
    for k in range(1, len(table)):
        got = jnp.where(at == k, table[k] + jnp.int32(0), got)
    return got


def label_of(virt, n_virt):
    return lax.rem(virt, 2) * (n_virt // 2) + virt // 2


def virt_of(label, n_virt):
    half = n_virt // 2
    return lax.rem(label, half) * 2 + label // half


def kernel(
    n_virt, n_aux, occ,
    x_ref, occ_ref, virt_ref,
    done_ref,
    held, lhs, rhs, order, order_t, ints, sums, parts, message, slots,
    own_sem, send_sem, recv_sem, msg_send, msg_recv,
):
    rows, cols = x_ref.shape
    pitch = -(-rows // 16) * 16
    width = cols // occ
    groups = LANES // width
    supers = occ // groups
    n = n_virt * n_aux
    v = lax.axis_index("virt")
    p = lax.axis_index("aux")
    me = v * n_aux + p
    table = distances(n_aux)
    label = label_of(v, n_virt)
    other = virt_of(lax.rem(label + pick(table, p), n_virt), n_virt)
    lower = label < n_virt // 2
    solo = jnp.logical_and(p == n_aux - 1, jnp.logical_not(lower))
    extra = jnp.logical_and(p == n_aux // 2 - 1, lower)

    barrier = pltpu.get_barrier_semaphore()

    def greet(k, c):
        t = lax.rem(me + k, n)
        pl.semaphore_signal(
            barrier, inc=1,
            device_id={"virt": t // n_aux, "aux": lax.rem(t, n_aux)},
            device_id_type=MESH,
        )
        return c

    lax.fori_loop(1, n, greet, 0)
    own = pltpu.make_async_copy(x_ref, held.at[0, p], own_sem)
    own.start()
    pl.semaphore_wait(barrier, n - 1)

    pairs = n_aux // 2

    def place(k):
        return lax.rem(p // 2 + k // 2, pairs) * 2 + lax.rem(p + k, 2)

    def share_own(k):
        return pltpu.make_async_remote_copy(
            src_ref=x_ref, dst_ref=held.at[0, p],
            send_sem=send_sem.at[0, k], recv_sem=recv_sem.at[0, p],
            device_id={"virt": v, "aux": place(k)}, device_id_type=MESH,
        )

    def hand_on(k):
        q = place(k)
        return pltpu.make_async_remote_copy(
            src_ref=held.at[0, q], dst_ref=held.at[0, q],
            send_sem=send_sem.at[2, k], recv_sem=recv_sem.at[0, q],
            device_id={"virt": v, "aux": place(1)}, device_id_type=MESH,
        )

    def share_other(k):
        q = place(k)
        target = lax.rem(label + n_virt - pick(table, q), n_virt)
        copy = pltpu.make_async_remote_copy(
            src_ref=x_ref, dst_ref=held.at[1, p],
            send_sem=send_sem.at[1, k], recv_sem=recv_sem.at[1, p],
            device_id={"virt": virt_of(target, n_virt), "aux": q}, device_id_type=MESH,
        )
        wanted = jnp.logical_or(q < n_aux - 1, target < n_virt // 2)
        return copy, wanted

    for k in list(range(2, n_aux, 2)) + [1]:
        share_own(k).start()
    for k in range(n_aux):
        copy, wanted = share_other(k)
        pl.when(wanted)(copy.start)

    def arrived(side, q):
        pltpu.make_async_copy(
            held.at[side, q], held.at[side, q], recv_sem.at[side, q]
        ).wait()

    row = lax.broadcasted_iota(jnp.int32, (cols, cols), 0)
    col = lax.broadcasted_iota(jnp.int32, (cols, cols), 1)
    hit = col == lax.rem(row, width) * occ + row // width
    order[...] = jnp.where(hit, 1.0, 0.0).astype(BF16)
    hit = row == lax.rem(col, width) * occ + col // width
    order_t[...] = jnp.where(hit, 1.0, 0.0).astype(BF16)
    lhs[...] = jnp.zeros_like(lhs)
    rhs[...] = jnp.zeros_like(rhs)

    def turn(k):
        lhs[:, k * pitch:k * pitch + rows] = lax.dot_general(
            order[...], held[0, place(k)], NT, preferred_element_type=F32
        ).astype(BF16)

    own.wait()
    turn(0)
    for k in range(2, n_aux, 2):
        arrived(0, place(k))
        hand_on(k).start()
        turn(k)
    for k in range(1, n_aux, 2):
        arrived(0, place(k))
        turn(k)

    lane = lax.broadcasted_iota(jnp.int32, (1, LANES), 1)
    part = lane // width
    down = lax.broadcasted_iota(jnp.int32, (width, 1), 0)
    lane_in = lax.rem(lane, width)

    def eps_down(which):
        got = jnp.zeros((width, 1), F32)
        for k in range(width):
            got = jnp.where(down == k, virt_ref[which * width + k], got)
        return got

    def eps_across(which):
        got = jnp.zeros((1, LANES), F32)
        for k in range(width):
            got = jnp.where(lane_in == k, virt_ref[which * width + k], got)
        return got

    occ_lane = []
    for cj in range(supers):
        got = jnp.zeros((1, LANES), F32)
        for t in range(groups):
            got = jnp.where(part == t, occ_ref[cj * groups + t], got)
        occ_lane.append(got)

    tall = -(-occ // 8)
    sums[...] = jnp.zeros_like(sums)
    n_tiles = jnp.where(extra, 2, 1)
    r8 = lax.broadcasted_iota(jnp.int32, (8, LANES), 0)
    l8 = lax.broadcasted_iota(jnp.int32, (8, LANES), 1)
    free = tall * width

    def tile(t, c):
        diag = jnp.logical_or(solo, jnp.logical_and(extra, t == 0))
        source = jnp.where(diag, 0, 1)

        for k in range(n_aux):

            @pl.when(source == 1)
            def _():
                arrived(1, place(k))

            rhs[k * pitch:k * pitch + rows, :] = lax.dot_general(
                held[source, place(k)], order_t[...], NN, preferred_element_type=F32
            ).astype(BF16)
        ints[...] = lax.dot_general(lhs[...], rhs[...], NN, preferred_element_type=F32)

        base = -(eps_down(v) + eps_across(jnp.where(diag, v, other)))
        total = jnp.zeros((width, LANES), F32)
        for ci in range(supers):
            for cj in range(ci, supers):
                turned = []
                for g in range(groups):
                    block = ints[pl.ds((cj * groups + g) * width, width), pl.ds(ci * LANES, LANES)]
                    turned.append([block if r == 0 else pltpu.roll(block, r * width, 1) for r in range(groups)])
                for s in range(groups):
                    i = ci * groups + s
                    direct = ints[pl.ds(i * width, width), pl.ds(cj * LANES, LANES)]
                    swapped = turned[0][(0 - s) % groups]
                    for g in range(1, groups):
                        swapped = jnp.where(part == g, turned[g][(g - s) % groups], swapped)
                    below = base + (occ_lane[cj] + occ_ref[i])
                    if ci == cj:
                        term = direct * (2.0 * direct - swapped) / below
                    else:
                        term = 2.0 * (direct * (direct - swapped) + swapped * swapped) / below
                    total = total + term
                    short = term[0:8]
                    for m in range(8, width, 8):
                        short = short + term[m:m + 8]
                    sums[i * 8:i * 8 + 8, cj * LANES:(cj + 1) * LANES] = short

        wide = lax.broadcasted_iota(jnp.int32, (cols, LANES), 0)
        thin = lax.broadcasted_iota(jnp.int32, (cols, LANES), 1)
        fold = jnp.where(wide // width == thin, 1.0, 0.0)
        by_j = lax.dot_general(sums[...], fold, NN, precision=EXACT, preferred_element_type=F32)
        ri = lax.broadcasted_iota(jnp.int32, (tall * 8, occ * 8), 0)
        rj = lax.broadcasted_iota(jnp.int32, (tall * 8, occ * 8), 1)
        by_ij = lax.dot_general(
            jnp.where(rj // 8 == ri, 1.0, 0.0), by_j, NN,
            precision=EXACT, preferred_element_type=F32,
        )
        packed = by_ij[0:8]
        for g in range(1, tall):
            packed = packed + pltpu.roll(by_ij[g * 8:g * 8 + 8], g * width, 1)
        pads = [jnp.zeros((free, LANES), F32), total]
        if free + width < LANES:
            pads.append(jnp.zeros((LANES - free - width, LANES), F32))
        spread = jnp.concatenate(pads, 0)
        by_row = lax.dot_general(
            jnp.ones((8, LANES), F32), spread, NT, precision=EXACT, preferred_element_type=F32)
        by_col = lax.dot_general(
            jnp.ones((8, width), F32), total, NN, precision=EXACT, preferred_element_type=F32)
        folded = by_col
        for g in range(1, groups):
            folded = folded + pltpu.roll(by_col, g * width, 1)
        packed = packed * jnp.where(diag, 0.5, 1.0)
        first = jnp.where(diag, (by_row + folded) * 0.5, by_row)
        second = jnp.where(diag, 0.0, folded)
        out = jnp.where(l8 < free, packed, jnp.where(r8 == 0, first, jnp.where(r8 == 1, second, 0.0)))

        @pl.when(t == 0)
        def _():
            message[...] = out

        @pl.when(t == 1)
        def _():
            message[...] += out

        return c

    lax.fori_loop(0, n_tiles, tile, 0)

    def tell(k, c):
        t = lax.rem(me + k, n)
        pltpu.make_async_remote_copy(
            src_ref=message, dst_ref=slots.at[me],
            send_sem=msg_send, recv_sem=msg_recv,
            device_id={"virt": t // n_aux, "aux": lax.rem(t, n_aux)},
            device_id_type=MESH,
        ).start()
        return c

    lax.fori_loop(1, n, tell, 0)
    slots[me] = message[...]
    for k in list(range(2, n_aux, 2)) + [1]:
        share_own(k).wait_send()
    for k in range(2, n_aux, 2):
        hand_on(k).wait_send()
    for k in range(n_aux):
        copy, wanted = share_other(k)
        pl.when(wanted)(copy.wait_send)
    everyone = slots.at[pl.ds(0, n - 1)]
    pltpu.make_async_copy(everyone, everyone, msg_send).wait()
    pltpu.make_async_copy(everyone, everyone, msg_recv).wait()

    keep = jnp.logical_or(l8 < free, r8 < 0)

    def add(k, acc):
        sv = k // n_aux
        so = virt_of(lax.rem(label_of(sv, n_virt) + pick(table, lax.rem(k, n_aux)), n_virt), n_virt)
        row0 = jnp.where(sv == v, 1.0, 0.0)
        row1 = jnp.where(so == v, 1.0, 0.0)
        weight = jnp.where(keep, 1.0, jnp.where(r8 == 0, row0, row1))
        return acc + slots[k] * weight

    done = lax.fori_loop(0, n, add, jnp.zeros((8, LANES), F32))
    done_ref[...] = done


TILES = (
    (0, 2, 0),
    (0, 2, 1),
    (0, 1, 0),
    (1, 2, 0),
    (1, 3, 1),
    (0, 3, 0),
    (1, 3, 0),
    (2, 3, 0),
    (0, 4, 0),
    (0, 5, 0),
    (2, 4, 0),
    (2, 5, 0),
    (1, 4, 0),
    (3, 4, 0),
    (1, 5, 0),
    (3, 5, 0),
    (0, 6, 0),
    (0, 7, 0),
    (2, 6, 0),
    (2, 7, 0),
    (1, 6, 0),
    (1, 7, 0),
    (3, 6, 0),
    (3, 7, 0),
    (6, 7, 0),
    (6, 4, 0),
    (7, 4, 0),
    (6, 4, 1),
    (6, 5, 0),
    (7, 5, 1),
    (4, 5, 0),
    (7, 5, 0),
)
ROUTES = (
    ((2, 4, 10, 18), (10, 4), (2, 10, 18), (), (3,), (), (3,), (), ()),
    ((), (0, 34), (), (0, 10), (7, 14), (), (), (1,), ()),
    ((), (), (0,), (2,), (), (), (), (), ()),
    ((5,), (), (5,), (), (), (), (1, 14), (14, 3), (4, 18)),
    ((12, 24), (12, 24), (24,), (24,), (11,), (), (), (), ()),
    ((), (), (), (), (), (9, 13), (), (9,), (5, 8)),
    ((6, 28), (6, 28), (6, 8, 28), (8, 6, 28), (), (15,), (9, 15), (15,), ()),
    ((), (), (), (), (13,), (), (), (), (5, 12, 40)),
    ((), (18,), (), (), (), (27, 21), (), (27, 21), (1, 22)),
    ((16, 34), (), (16, 34), (16, 34), (23, 31), (), (), (), (1, 22, 36, 3)),
    ((36,), (), (7, 22), (7,), (), (), (17, 27), (), ()),
    ((20,), (7, 20, 14), (36, 38), (20, 36), (), (), (19,), (19,), ()),
    ((42,), (42,), (42,), (), (), (), (), (), (26, 30)),
    ((9, 46), (11, 44), (11,), (11,), (17, 25), (25,), (25,), (25,), ()),
    ((), (), (), (), (), (31, 61, 23), (31,), (23, 31), (30,)),
    ((15,), (), (13, 26, 46), (13, 26, 44), (29,), (), (), (), ()),
    ((), (), (), (), (), (), (41,), (), (27, 51)),
    ((32,), (16, 32), (32,), (32,), (), (), (), (), (17, 51, 60)),
    ((38,), (38,), (), (38,), (), (33,), (33, 45), (33, 45), (21, 55)),
    ((), (), (), (), (47, 52), (), (), (35,), (17, 55)),
    ((), (), (), (42,), (33, 56, 45), (45,), (), (), (19, 57)),
    ((40,), (40,), (40,), (), (), (39,), (35,), (), (29, 57, 59)),
    ((), (46, 30), (), (46,), (), (), (), (), (23, 61, 29)),
    ((44,), (), (44,), (), (), (), (), (39, 43, 52), (29, 63)),
    ((41, 50), (), (50, 56), (50, 56, 41), (35,), (35,), (), (), ()),
    ((54,), (41, 48, 54, 56), (), (), (55,), (53,), (), (), ()),
    ((), (), (), (), (), (55,), (), (), (54,)),
    ((37,), (37,), (37, 48), (37, 48), (53, 60, 21), (), (53, 60, 51), (53, 60, 51), ()),
    ((), (), (), (), (59, 63), (19,), (), (), (39, 58)),
    ((49, 62), (43, 49, 62), (43, 49), (49,), (), (63,), (57,), (57,), ()),
    ((), (), (), (), (), (), (63, 59), (59,), (39, 58, 62)),
    ((43,), (52, 47), (52, 47), (47, 58), (61,), (), (), (61,), ()),
)
STEPS = (
    (0, 1, 2, 3, 4, 10, 5, 8, 6, 25, 12, 27, 29, 7, 14, 31),
    (2, 19, 0, 17, 4, 6, 8, 21, 10, 23, 25, 27, 12, 14, 29, 31),
    (4, 5, 6, 7, 14, 0, 10, 12, 31, 1, 11, 29, 2, 19, 8, 25),
    (12, 4, 13, 14, 21, 15, 10, 6, 23, 8, 0, 11, 1, 25, 2, 19),
    (0, 17, 2, 19, 4, 10, 21, 27, 8, 6, 25, 23, 14, 12, 31, 29),
    (10, 0, 11, 1, 2, 19, 8, 14, 25, 4, 15, 6, 12, 5, 29, 23),
    (4, 5, 6, 7, 14, 0, 31, 1, 12, 2, 29, 10, 3, 8, 27, 25),
    (14, 15, 4, 12, 5, 8, 29, 10, 6, 9, 11, 2, 23, 0, 19, 17),
    (10, 14, 0, 6, 11, 15, 1, 2, 23, 12, 4, 8, 5, 29, 19, 25),
    (0, 6, 8, 1, 7, 25, 4, 12, 5, 2, 10, 14, 3, 29, 27, 31),
    (4, 5, 6, 7, 12, 2, 0, 29, 3, 1, 10, 14, 27, 8, 31, 25),
    (6, 7, 4, 5, 2, 0, 12, 3, 1, 14, 8, 29, 10, 31, 25, 27),
    (0, 1, 2, 8, 3, 4, 25, 5, 10, 12, 6, 7, 14, 29, 27, 31),
    (2, 3, 0, 1, 6, 7, 8, 4, 5, 25, 10, 12, 14, 29, 27, 31),
    (14, 4, 10, 15, 5, 12, 11, 6, 23, 0, 29, 8, 1, 2, 19, 25),
    (6, 7, 4, 5, 0, 14, 10, 1, 31, 12, 11, 8, 2, 29, 19, 25),
    (2, 14, 15, 3, 0, 12, 8, 6, 13, 1, 25, 23, 10, 4, 21, 27),
    (2, 3, 0, 6, 10, 1, 7, 27, 14, 4, 12, 8, 5, 25, 31, 29),
    (6, 14, 7, 31, 2, 4, 12, 13, 3, 21, 10, 27, 0, 8, 1, 25),
    (6, 12, 7, 8, 4, 2, 14, 13, 9, 3, 10, 31, 21, 27, 0, 17),
    (10, 8, 6, 11, 9, 7, 0, 14, 17, 31, 2, 19, 12, 4, 13, 21),
    (10, 11, 6, 14, 0, 1, 12, 7, 31, 2, 19, 13, 4, 8, 21, 25),
    (2, 6, 3, 7, 14, 0, 31, 10, 4, 1, 12, 8, 27, 5, 29, 25),
    (14, 2, 6, 0, 3, 15, 23, 12, 4, 1, 13, 10, 21, 8, 27, 25),
    (0, 1, 2, 3, 6, 10, 7, 27, 4, 8, 5, 25, 14, 12, 31, 29),
    (2, 3, 0, 1, 10, 8, 6, 7, 25, 4, 27, 14, 5, 12, 31, 29),
    (4, 14, 12, 5, 2, 15, 10, 29, 0, 3, 6, 8, 9, 27, 17, 23),
    (6, 23, 4, 21, 2, 14, 12, 19, 0, 31, 29, 17, 8, 10, 25, 27),
    (2, 10, 8, 3, 9, 6, 27, 7, 12, 0, 14, 17, 4, 13, 21, 31),
    (2, 19, 0, 17, 6, 4, 8, 10, 23, 21, 25, 12, 14, 27, 29, 31),
    (12, 14, 13, 6, 15, 2, 4, 23, 10, 8, 21, 0, 11, 19, 1, 25),
    (6, 7, 4, 5, 2, 14, 3, 12, 31, 0, 29, 8, 1, 25, 10, 27),
)
PARTNERS = (
    (1, 2, 4, 8, 3, 9),
    (0, 3, 5, 9, 2),
    (3, 0, 6, 10, 5, 7),
    (2, 1, 7, 11, 6, 10),
    (5, 6, 0, 12, 13),
    (4, 7, 1, 13, 0),
    (7, 4, 2, 14, 5, 15),
    (6, 5, 3, 15, 1, 11),
    (9, 10, 12, 0, 16, 13, 17, 19),
    (8, 11, 13, 1, 17, 0, 3, 20, 28),
    (11, 8, 14, 2, 18, 27),
    (10, 9, 15, 3, 19, 8, 14, 22),
    (13, 14, 8, 4, 20),
    (12, 15, 9, 5, 21, 8, 10, 16),
    (15, 12, 10, 6, 22, 21, 23),
    (14, 13, 11, 7, 23, 9, 12, 22),
    (17, 18, 20, 8, 24),
    (16, 19, 21, 9, 25, 1, 24),
    (19, 16, 22, 10, 26, 9, 11, 27),
    (18, 17, 23, 11, 27, 21, 28, 30),
    (21, 22, 16, 12, 28, 7, 24, 25),
    (20, 23, 17, 13, 29, 12, 31),
    (23, 20, 18, 14, 30, 13, 15),
    (22, 21, 19, 15, 31, 13),
    (25, 26, 28, 16, 27, 29),
    (24, 27, 29, 17, 16),
    (27, 24, 30, 18, 19, 23, 25, 31),
    (26, 25, 31, 19, 18),
    (29, 30, 24, 20, 21, 25),
    (28, 31, 25, 21, 30),
    (31, 28, 26, 22, 14, 17, 27),
    (30, 29, 27, 23, 28),
)
NEAR = (4, 4, 4, 4, 4, 4, 4, 4, 5, 5, 5, 5, 5, 5, 5, 5, 5, 5, 5, 5, 5, 5, 5, 5, 4, 4, 4, 4, 4, 4, 4, 4)
AWAITED = (6, 6, 5, 6, 4, 6, 5, 6, 7, 8, 7, 7, 7, 9, 7, 7, 7, 7, 6, 7, 6, 8, 7, 7, 6, 7, 4, 8, 7, 5, 6, 6)
NEWS = (
    (8, 12, 14),
    (5, 9, 15),
    (6, 12, 14),
    (3, 8, 12),
    (7, 12, 15),
    (4, 10, 15),
    (8, 12, 15),
    (1, 7, 13),
    (1, 7, 15),
    (1, 7, 11),
    (5, 10, 12),
    (6, 9, 14),
    (2, 5, 11),
    (6, 10, 14),
    (2, 7, 11),
    (5, 9, 12),
    (0, 2, 10),
    (0, 3, 7),
    (3, 9, 14),
    (1, 8, 14),
    (0, 4, 9),
    (1, 5, 10),
    (2, 6, 12),
    (1, 7, 14),
    (6, 12, 15),
    (6, 11, 15),
    (0, 6, 12),
    (8, 12, 15),
    (3, 7, 11),
    (5, 10, 15),
    (1, 5, 11),
    (6, 10, 13),
)
PLANS = {(8, 4): (TILES, ROUTES, STEPS, PARTNERS, NEAR, NEWS, AWAITED)}


TN = (((0,), (0,)), ((), ()))
KIDS = 4
CODE = 128


def table_kernel(
    n_virt, n_aux, occ, plan,
    x_ref, occ_hbm, virt_hbm,
    done_ref,
    raw, held, order, ints, over, sums, message, slots, weigh, occ_ref, virt_ref,
    own_sem, eps_sem, send_sem, recv_sem, msg_send, msg_recv, news_sem,
):
    rows, cols = x_ref.shape
    deep = held.shape[1]
    width = cols // occ
    groups = LANES // width
    supers = occ // groups
    n = n_virt * n_aux
    v = lax.axis_index("virt")
    p = lax.axis_index("aux")
    me = v * n_aux + p
    tiles, routes, steps, partners, n_near, news, awaited = plan
    rounds = len(news[0]) + 1
    half = -(-rows // 32) * 16
    cuts = ((0, half), (half, -(-rows // 8) * 8 - half))
    n_slots = 2 * n_aux

    def device(t):
        return {"virt": lax.div(t, n_aux), "aux": lax.rem(t, n_aux)}

    barrier = pltpu.get_barrier_semaphore()

    own = pltpu.make_async_copy(x_ref, raw, own_sem)
    own.start()
    if deep > rows:
        held[:, rows:, :] = jnp.zeros((n_slots + 1, deep - rows, cols), BF16)

    def packed(codes):
        got = 0
        for c in reversed(codes):
            got = got * CODE + c + 1
        return got

    most = max(len(r) for r in partners)
    folk = [
        pick([packed(r[at:at + KIDS]) for r in partners], me) for at in range(0, most, KIDS)
    ]
    n_folk = pick([len(r) for r in partners], me)
    near = pick(n_near, me)

    def signal(sem, amount, limit):
        code = None
        for k in range(amount):
            code = folk[k // KIDS] if k % KIDS == 0 else lax.div(code, CODE)

            @pl.when(k < limit)
            def _():
                t = lax.rem(code, CODE) - 1
                pl.semaphore_signal(sem, inc=1, device_id=device(t), device_id_type=MESH)

    signal(barrier, most, n_folk)
    eps = (
        pltpu.make_async_copy(occ_hbm, occ_ref, eps_sem.at[0]),
        pltpu.make_async_copy(virt_hbm, virt_ref, eps_sem.at[1]),
    )
    for copy in eps:
        copy.start()
    side_a = pick([t[0] for t in tiles], me)
    side_b = pick([t[1] for t in tiles], me)
    diag = pick([t[2] for t in tiles], me) == 1
    own_slot = jnp.where(side_a == v, p, jnp.where(side_b == v, n_aux + p, n_slots))
    owns = []
    for d, (a, b, _) in enumerate(tiles):
        q = d % n_aux
        owns.append(q if a == d // n_aux else n_aux + q if b == d // n_aux else n_slots)

    row = lax.broadcasted_iota(jnp.int32, (cols, cols), 0)
    col = lax.broadcasted_iota(jnp.int32, (cols, cols), 1)
    hit = row == lax.rem(col, width) * occ + col // width
    order[...] = jnp.where(hit, 1.0, 0.0).astype(BF16)
    own.wait()
    held[own_slot, 0:rows, :] = lax.dot_general(
        raw[...], order[...], NN, preferred_element_type=F32
    ).astype(BF16)
    pl.semaphore_wait(barrier, pick(awaited, me))

    own_kids = pick([packed(r[o]) for r, o in zip(routes, owns)], me)

    def piece(slot, part):
        return held.at[slot, pl.ds(cuts[part][0], cuts[part][1])]

    def decode(slot, code):
        q = jnp.where(slot == n_slots, p, lax.rem(slot, n_aux))
        found = []
        for k in range(KIDS):
            this = lax.rem(code, CODE)
            code = lax.div(code, CODE)
            t = jnp.maximum(this - 1, 0)
            found.append((this > 0, lax.div(t, 2), lax.rem(t, 2) * n_aux + q))
        return found

    def copies(slot, part, found, act):
        for there, t, to in found:

            @pl.when(there)
            def _():
                act(pltpu.make_async_remote_copy(
                    src_ref=piece(slot, part), dst_ref=piece(to, part),
                    send_sem=send_sem.at[slot], recv_sem=recv_sem.at[to, part],
                    device_id=device(t), device_id_type=MESH,
                ))

    own_found = decode(own_slot, own_kids)
    for part in range(2):
        copies(own_slot, part, own_found, lambda copy: copy.start())
    close = max(n_near)
    signal(news_sem.at[0], close, near)
    kids = [pick([packed(r[s]) for r in routes], me) for s in range(n_slots + 1)]
    spread_at = [pick([r[k] for r in news], me) for k in range(rounds - 1)]
    todo = [pick([r[i] for r in steps], me) for i in range(2 * n_slots)]
    for copy in eps:
        copy.wait()

    lane = lax.broadcasted_iota(jnp.int32, (1, LANES), 1)
    part = lane // width
    down = lax.broadcasted_iota(jnp.int32, (width, 1), 0)
    lane_in = lax.rem(lane, width)
    n_tiles = jnp.where(diag, 2, 1)

    def eps_down(which):
        got = jnp.zeros((width, 1), F32)
        for k in range(width):
            got = jnp.where(down == k, virt_ref[which * width + k], got)
        return got

    def eps_across(which):
        got = jnp.zeros((1, LANES), F32)
        for k in range(width):
            got = jnp.where(lane_in == k, virt_ref[which * width + k], got)
        return got

    occ_lane = []
    for cj in range(supers):
        got = jnp.zeros((1, LANES), F32)
        for t in range(groups):
            got = jnp.where(part == t, occ_ref[cj * groups + t], got)
        occ_lane.append(got)

    def prepare(t, c):
        block_l = jnp.where(t == 0, side_a, side_b)
        block_r = jnp.where(jnp.logical_and(diag, t == 0), side_a, side_b)
        base = -(eps_down(block_l) + eps_across(block_r))
        ints[t] = jnp.zeros((cols, cols), F32)
        for i in range(occ):
            for cj in range(i // groups, supers):
                below = base + (occ_lane[cj] + occ_ref[i])
                over[t, i * width:(i + 1) * width, cj * LANES:(cj + 1) * LANES] = (
                    (1.0 if cj == i // groups else 2.0) / below
                )
        return c

    lax.fori_loop(0, n_tiles, prepare, 0)

    keep = lax.broadcasted_iota(jnp.int32, (4, LANES), 1) < -(-occ // 4) * occ
    upper = lax.broadcasted_iota(jnp.int32, (4, LANES), 0) < 2
    for k in range(n):
        row0 = jnp.where(v == tiles[k][0], 1.0, 0.0)
        row1 = jnp.where(v == tiles[k][1], 1.0, 0.0)
        weigh[k] = jnp.where(keep, 1.0, jnp.where(upper, row0, row1))

    def take(i, c):
        for r in range(1, rounds):

            @pl.when(i == spread_at[r - 1])
            def _():
                pl.semaphore_wait(news_sem.at[r - 1], near)
                signal(news_sem.at[r], close, near)

        entry = pick(todo, i)
        slot = lax.rem(lax.div(entry, 2), n_slots)
        meets = lax.div(entry, 4 * n_aux) == 1
        later = lax.rem(entry, 2)
        away = slot != own_slot
        found = decode(slot, pick(kids, slot))
        for part in range(2):

            @pl.when(jnp.logical_and(later == part, away))
            def _():
                whole = piece(slot, part)
                pltpu.make_async_copy(whole, whole, recv_sem.at[slot, part]).wait()
                copies(slot, part, found, lambda copy: copy.start())

        side = lax.div(slot, n_aux)
        mine = jnp.where(diag, side, 0)
        left = jnp.where(diag, slot, lax.rem(slot, n_aux))
        right = jnp.where(diag, slot, n_aux + lax.rem(slot, n_aux))

        @pl.when(meets)
        def _():
            ints[mine] += lax.dot_general(held[left], held[right], TN, preferred_element_type=F32)

        return c

    lax.fori_loop(0, 2 * n_slots, take, 0)

    tall = -(-occ // 4)
    sums[...] = jnp.zeros_like(sums)
    r8 = lax.broadcasted_iota(jnp.int32, (8, LANES), 0)
    l8 = lax.broadcasted_iota(jnp.int32, (8, LANES), 1)
    wide = lax.broadcasted_iota(jnp.int32, (cols, LANES), 0)
    thin = lax.broadcasted_iota(jnp.int32, (cols, LANES), 1)
    fold = jnp.where(wide // width == thin, 1.0, 0.0).astype(BF16)
    ri = lax.broadcasted_iota(jnp.int32, (tall * 8, occ * 8), 0)
    rj = lax.broadcasted_iota(jnp.int32, (tall * 8, occ * 8), 1)
    gather = jnp.logical_and(lax.rem(ri, 8) < 4, rj // 8 == ri // 8 * 4 + lax.rem(ri, 8))
    gather = jnp.where(gather, 1.0, 0.0).astype(BF16)
    ones = jnp.ones((8, LANES), BF16)
    free = tall * occ

    def split(x):
        high = x.astype(BF16)
        return high, (x - high.astype(F32)).astype(BF16)

    def tile(t, c):
        total = jnp.zeros((width, LANES), F32)
        for ci in range(supers):
            for cj in range(ci, supers):
                block = [
                    ints[t, pl.ds((cj * groups + g) * width, width), pl.ds(ci * LANES, LANES)]
                    for g in range(groups)
                ]
                turned = []
                for r in range(groups):
                    mixed = block[r]
                    for g in range(1, groups):
                        mixed = jnp.where(part == g, block[(g + r) % groups], mixed)
                    turned.append(mixed if r == 0 else pltpu.roll(mixed, r * width, 1))
                for s in range(groups):
                    i = ci * groups + s
                    direct = ints[t, pl.ds(i * width, width), pl.ds(cj * LANES, LANES)]
                    inverse = over[t, pl.ds(i * width, width), pl.ds(cj * LANES, LANES)]
                    swapped = turned[(0 - s) % groups]
                    for g in range(1, groups):
                        swapped = jnp.where(part == g, turned[(g - s) % groups], swapped)
                    if ci == cj:
                        term = direct * (2.0 * direct - swapped) * inverse
                    else:
                        term = (direct * (direct - swapped) + swapped * swapped) * inverse
                    total = total + term
                    short = term[0:8]
                    for m in range(8, width, 8):
                        short = short + term[m:m + 8]
                    sums[i * 8:i * 8 + 8, cj * LANES:(cj + 1) * LANES] = short

        rows_of = [
            lax.dot_general(gather, x, NN, preferred_element_type=F32) for x in split(sums[...])
        ]
        pairs_of = [
            lax.dot_general(x, fold, NN, preferred_element_type=F32)
            for x in split(rows_of[0] + rows_of[1])
        ]
        by_ij = pairs_of[0] + pairs_of[1]
        packed_ij = by_ij[0:8]
        for g in range(1, tall):
            packed_ij = packed_ij + pltpu.roll(by_ij[g * 8:g * 8 + 8], g * occ, 1)
        spread = jnp.concatenate([jnp.zeros((LANES - width, LANES), F32), total], 0)
        by_row = [
            lax.dot_general(ones, x, NT, preferred_element_type=F32) for x in split(spread)
        ]
        by_row = by_row[0] + by_row[1]
        by_col = [
            lax.dot_general(ones[:, :width], x, NN, preferred_element_type=F32) for x in split(total)
        ]
        by_col = by_col[0] + by_col[1]
        folded = by_col
        for g in range(1, groups):
            folded = folded + pltpu.roll(by_col, g * width, 1)
        packed_ij = packed_ij * jnp.where(diag, 0.5, 1.0)
        both = (by_row + folded) * 0.5
        first = jnp.where(diag, jnp.where(t == 0, both, 0.0), by_row)
        second = jnp.where(diag, jnp.where(t == 1, both, 0.0), folded)
        near_turn = free - (LANES - width)
        far_turn = near_turn - width // 2
        shares = jnp.where(r8 == 3, pltpu.roll(second, far_turn % LANES, 1), 0.0)
        shares = jnp.where(r8 == 2, pltpu.roll(second, near_turn % LANES, 1), shares)
        shares = jnp.where(r8 == 1, pltpu.roll(first, far_turn % LANES, 1), shares)
        shares = jnp.where(r8 == 0, pltpu.roll(first, near_turn % LANES, 1), shares)
        shares = jnp.where(l8 < free + width // 2, shares, 0.0)
        out = jnp.where(l8 < free, packed_ij, shares)[0:4]

        @pl.when(t == 0)
        def _():
            message[...] = out

        @pl.when(t == 1)
        def _():
            message[...] += out

        return c

    lax.fori_loop(0, n_tiles, tile, 0)
    pl.semaphore_wait(news_sem.at[rounds - 1], near)

    for t in range(n):

        @pl.when(me != t)
        def _():
            pltpu.make_async_remote_copy(
                src_ref=message, dst_ref=slots.at[me],
                send_sem=msg_send, recv_sem=msg_recv,
                device_id={"virt": t // n_aux, "aux": t % n_aux}, device_id_type=MESH,
            ).start()

    slots[me] = message[...]
    sent = sum(cut[1] for cut in cuts)

    def flush(s, c):
        many = sum(jnp.where(there, 1, 0) for there, _, _ in decode(s, pick(kids, s)))
        for m in range(1, KIDS + 1):

            @pl.when(many == m)
            def _():
                gone = held.at[pl.ds(0, m), pl.ds(0, sent)]
                pltpu.make_async_copy(gone, gone, send_sem.at[s]).wait()

        return c

    lax.fori_loop(0, n_slots + 1, flush, 0)
    everyone = slots.at[pl.ds(0, n - 1)]
    pltpu.make_async_copy(everyone, everyone, msg_send).wait()
    pltpu.make_async_copy(everyone, everyone, msg_recv).wait()

    accs = [None] * 4
    for k in range(n):
        term = slots[k] * weigh[k]
        accs[k % 4] = term if accs[k % 4] is None else accs[k % 4] + term
    done_ref[...] = (accs[0] + accs[1]) + (accs[2] + accs[3])


def table_unpack(occ, width, done_ref, share_ref, pair_ref):
    tall = -(-occ // 4)
    free = tall * occ
    done = done_ref[...]
    share = done[0:2] + done[2:4]
    share_ref[...] = jnp.concatenate(
        [share[0, free:free + width // 2], share[1, free:free + width // 2]], 0
    )
    blocks = [done] + [pltpu.roll(done, LANES - g * occ, 1) for g in range(1, tall)]
    square = jnp.concatenate(blocks + [jnp.zeros((LANES - 4 * tall, LANES), F32)], 0)
    square = jnp.where(lax.broadcasted_iota(jnp.int32, (LANES, LANES), 1) < occ, square, 0.0)
    pair = square + square.T
    pair_ref[...] = pair[0:occ, 0:occ]


def table_call(n_virt, n_aux, occ, plan, three_index, eps_occ, eps_virt):
    rows, cols = three_index.shape
    width = cols // occ
    deep = -(-rows // 16) * 16
    n = n_virt * n_aux
    n_slots = 2 * n_aux
    vmem = pl.BlockSpec(memory_space=pltpu.VMEM)
    hbm = pl.BlockSpec(memory_space=pltpu.HBM)
    done = pl.pallas_call(
        functools.partial(table_kernel, n_virt, n_aux, occ, plan),
        out_shape=pltpu.VMEM((4, LANES), F32),
        in_specs=[hbm, hbm, hbm],
        out_specs=vmem,
        scratch_shapes=[
            pltpu.VMEM((rows, cols), BF16),
            pltpu.VMEM((n_slots + 1, deep, cols), BF16),
            pltpu.VMEM((cols, cols), BF16),
            pltpu.VMEM((2, cols, cols), F32),
            pltpu.VMEM((2, cols, cols), F32),
            pltpu.VMEM((occ * 8, cols), F32),
            pltpu.VMEM((4, LANES), F32),
            pltpu.VMEM((n, 4, LANES), F32),
            pltpu.VMEM((n, 4, LANES), F32),
            pltpu.SMEM(eps_occ.shape, F32),
            pltpu.SMEM(eps_virt.shape, F32),
            pltpu.SemaphoreType.DMA,
            pltpu.SemaphoreType.DMA((2,)),
            pltpu.SemaphoreType.DMA((n_slots + 1,)),
            pltpu.SemaphoreType.DMA((n_slots, 2)),
            pltpu.SemaphoreType.DMA,
            pltpu.SemaphoreType.DMA,
            pltpu.SemaphoreType.REGULAR((len(plan[5][0]) + 1,)),
        ],
        compiler_params=pltpu.CompilerParams(collective_id=0, has_side_effects=True),
    )(three_index, eps_occ, eps_virt)
    return pl.pallas_call(
        functools.partial(table_unpack, occ, width),
        out_shape=(
            jax.ShapeDtypeStruct((width,), F32),
            jax.ShapeDtypeStruct((occ, occ), F32),
        ),
        in_specs=[vmem],
        out_specs=(vmem, vmem),
    )(pltpu.with_memory_space_constraint(done, pltpu.VMEM))


def unpack(occ, width, done_ref, share_ref, pair_ref):
    tall = -(-occ // 8)
    free = tall * width
    done = done_ref[...]
    share = done[0:1] + done[1:2]
    share_ref[...] = share[0, free:free + width]
    blocks = [done] + [pltpu.roll(done, LANES - g * width, 1) for g in range(1, tall)]
    square = jnp.concatenate(blocks + [jnp.zeros((LANES - 8 * tall, LANES), F32)], 0)
    square = jnp.where(lax.broadcasted_iota(jnp.int32, (LANES, LANES), 1) < occ, square, 0.0)
    pair = square + square.T
    pair_ref[...] = pair[0:occ, 0:occ]


def on_device(n_virt, n_aux, three_index, eps_occ, eps_virt):
    occ = eps_occ.shape[0]
    rows, cols = three_index.shape
    width = cols // occ
    pitch = -(-rows // 16) * 16
    n = n_virt * n_aux
    vmem = pl.BlockSpec(memory_space=pltpu.VMEM)
    smem = pl.BlockSpec(memory_space=pltpu.SMEM)
    plan = PLANS.get((n_virt, n_aux))
    if plan is not None:
        return table_call(n_virt, n_aux, occ, plan, three_index, eps_occ, eps_virt)
    done = pl.pallas_call(
        functools.partial(kernel, n_virt, n_aux, occ),
        out_shape=jax.ShapeDtypeStruct((8, LANES), F32),
        in_specs=[vmem, smem, smem],
        out_specs=vmem,
        scratch_shapes=[
            pltpu.VMEM((2, n_aux, rows, cols), BF16),
            pltpu.VMEM((cols, n_aux * pitch), BF16),
            pltpu.VMEM((n_aux * pitch, cols), BF16),
            pltpu.VMEM((cols, cols), BF16),
            pltpu.VMEM((cols, cols), BF16),
            pltpu.VMEM((cols, cols), F32),
            pltpu.VMEM((occ * 8, cols), F32),
            pltpu.VMEM((8, LANES), F32),
            pltpu.VMEM((8, LANES), F32),
            pltpu.VMEM((n, 8, LANES), F32),
            pltpu.SemaphoreType.DMA,
            pltpu.SemaphoreType.DMA((3, n_aux)),
            pltpu.SemaphoreType.DMA((2, n_aux)),
            pltpu.SemaphoreType.DMA,
            pltpu.SemaphoreType.DMA,
        ],
        compiler_params=pltpu.CompilerParams(collective_id=0, has_side_effects=True),
    )(three_index, eps_occ, eps_virt)
    return pl.pallas_call(
        functools.partial(unpack, occ, width),
        out_shape=(
            jax.ShapeDtypeStruct((width,), F32),
            jax.ShapeDtypeStruct((occ, occ), F32),
        ),
        in_specs=[vmem],
        out_specs=(vmem, vmem),
    )(done)


def solution(mesh):
    n_virt, n_aux = mesh.shape["virt"], mesh.shape["aux"]
    assert n_virt == 2 * n_aux and n_aux % 2 == 0
    in_specs = (P("aux", "virt"), P(), P())
    out_specs = (P("virt"), P())
    return jax.shard_map(
        functools.partial(on_device, n_virt, n_aux), mesh=mesh,
        in_specs=in_specs, out_specs=out_specs, check_vma=False,
    )
```
